8 devices in a mesh: data: 1 (over z), node: 2 (over y), expert: 4 (over x, core).
Axes of the slice: x: 2, y: 2, z: 1, core: 2. Of those that a mesh axis runs over, the one named last changes fastest.
Arguments:
- tokens: bfloat16 [2048, 2048], P(('data', 'node', 'expert'))
- expert_ids: int32 [2048, 8], P(('data', 'node', 'expert'))
- gate_weights: float32 [2048, 8], P(('data', 'node', 'expert'))
- slot_ids: int32 [2048, 8], P(('data', 'node', 'expert'))
- w_gate: bfloat16 [128, 2048, 768], P(('node', 'expert'))
- w_up: bfloat16 [128, 2048, 768], P(('node', 'expert'))
- w_down: bfloat16 [128, 768, 2048], P(('node', 'expert'))
Outputs:
- output: bfloat16 [2048, 2048], P(('data', 'node', 'expert'))
All inputs are finite; a program needn't handle non-finite values.
Results may differ from the reference program's by a relative error of at most 0.00154.
Values are sent between devices in bfloat16 or wider.
A program may use at most 1 GiB of HBM per device.

```python
import jax
import jax.numpy as jnp
from jax import lax

EXPERTS = 128
D = 2048
FF = 768
TOP = 8
TOKENS_DEV = 256
GROUP = 8
CAP = 32

TOKENS = GROUP * TOKENS_DEV


def device_slots(flat_ids):
    choice_count = flat_ids.shape[0]
    sort_order = jnp.argsort(flat_ids, stable=True)
    sorted_ids = flat_ids[sort_order]
    counts = jnp.zeros((EXPERTS,), jnp.int32).at[flat_ids].add(1)
    starts = jnp.cumsum(counts) - counts
    rank_sorted = jnp.arange(choice_count, dtype=jnp.int32) - starts[sorted_ids]
    rank_all = jnp.zeros((choice_count,), jnp.int32).at[sort_order].set(rank_sorted)
    return jnp.where(rank_all < CAP, rank_all, -1)


def draw_routing(key):
    sub_keys = jax.random.split(key, 5)
    hot_first = jax.random.randint(sub_keys[0], (), 0, EXPERTS)
    pick_hot = jax.random.randint(sub_keys[1], (TOKENS,), 0, 4)
    hot_base = jax.random.randint(sub_keys[2], (TOKENS,), 0, max(EXPERTS // 4, 1))
    any_base = jax.random.randint(sub_keys[3], (TOKENS,), 0, EXPERTS)
    base_ids = jnp.where(pick_hot == 0, hot_base, any_base)
    local_row = jnp.arange(TOKENS, dtype=jnp.int32) % TOKENS_DEV
    base_ids = jnp.where(local_row < CAP, 0, base_ids)
    step_max = (EXPERTS - 1) // max(TOP - 1, 1)
    step_sizes = jax.random.randint(sub_keys[4], (TOKENS, TOP), 1, step_max + 1)
    step_sizes = step_sizes.at[:, 0].set(0)
    offsets = jnp.cumsum(step_sizes, axis=1)
    expert_ids = ((base_ids[:, None] + hot_first + offsets) % EXPERTS).astype(jnp.int32)
    slot_ids = jax.vmap(device_slots)(expert_ids.reshape(GROUP, TOKENS_DEV * TOP))
    return expert_ids, slot_ids.reshape(TOKENS, TOP).astype(jnp.int32)


def setup_inputs(seed: int = 0, part: int = 0) -> dict:
    part_key = jax.random.fold_in(jax.random.key(seed), part)
    key_tokens, key_route, key_gates = jax.random.split(part_key, 3)
    key_gate_w, key_up_w, key_down_w = jax.random.split(jax.random.key(seed + 1), 3)
    tokens = jax.random.normal(key_tokens, (TOKENS, D), jnp.float32).astype(jnp.bfloat16)
    expert_ids, slot_ids = draw_routing(key_route)
    gate_weights = (0.5 + jax.random.uniform(key_gates, (TOKENS, TOP), jnp.float32)) * TOP ** -0.5
    w_gate = (jax.random.normal(key_gate_w, (EXPERTS, D, FF), jnp.float32) * D ** -0.5).astype(jnp.bfloat16)
    w_up = (jax.random.normal(key_up_w, (EXPERTS, D, FF), jnp.float32) * D ** -0.5).astype(jnp.bfloat16)
    w_down = (jax.random.normal(key_down_w, (EXPERTS, FF, D), jnp.float32) * FF ** -0.5).astype(jnp.bfloat16)
    return {"tokens": tokens, "expert_ids": expert_ids, "gate_weights": gate_weights, "slot_ids": slot_ids, "w_gate": w_gate, "w_up": w_up, "w_down": w_down}


def expert_block(expert_rows, gate_mat, up_mat, down_mat):
    proj_gate = jnp.dot(expert_rows, gate_mat, preferred_element_type=jnp.float32)
    proj_up = jnp.dot(expert_rows, up_mat, preferred_element_type=jnp.float32)
    hidden = (jax.nn.silu(proj_gate) * proj_up).astype(jnp.bfloat16)
    return jnp.dot(hidden, down_mat, preferred_element_type=jnp.float32).astype(jnp.bfloat16)


def reference(tokens, expert_ids, gate_weights, slot_ids, w_gate, w_up, w_down):
    buffer_rows = GROUP * CAP
    source_dev = (jnp.arange(TOKENS, dtype=jnp.int32) // TOKENS_DEV)[:, None]
    kept = slot_ids >= 0
    flat_pos = jnp.where(kept, expert_ids * buffer_rows + source_dev * CAP + slot_ids, EXPERTS * buffer_rows).reshape(-1)
    tok_index = jnp.broadcast_to(jnp.arange(TOKENS, dtype=jnp.int32)[:, None], (TOKENS, TOP)).reshape(-1)
    src_table = jnp.full((EXPERTS * buffer_rows,), TOKENS, jnp.int32).at[flat_pos].set(tok_index, mode="drop")
    gate_table = jnp.zeros((EXPERTS * buffer_rows,), jnp.float32).at[flat_pos].set(gate_weights.reshape(-1), mode="drop")

    def one_expert(out_sum, operands):
        src_rows, row_gates, gate_mat, up_mat, down_mat = operands
        expert_rows = jnp.take(tokens, src_rows, axis=0, mode="fill", fill_value=0)
        expert_out = expert_block(expert_rows, gate_mat, up_mat, down_mat)
        out_sum = out_sum.at[src_rows].add(row_gates[:, None] * expert_out.astype(jnp.float32), mode="drop")
        return out_sum, None

    out_sum, _ = lax.scan(one_expert, jnp.zeros((TOKENS, D), jnp.float32), (src_table.reshape(EXPERTS, buffer_rows), gate_table.reshape(EXPERTS, buffer_rows), w_gate, w_up, w_down))
    return out_sum.astype(jnp.bfloat16)
```

```python
import functools

import jax
import jax.numpy as jnp
from jax import lax
from jax.experimental import pallas as pl
from jax.experimental.pallas import tpu as pltpu
from jax.sharding import PartitionSpec as P

CAP_FACTOR = 2
MESH = pl.DeviceIdType.MESH
F32 = jnp.float32
BF16 = jnp.bfloat16

ROWS = 256
WIDTH = 2048
FF = 768
LOCAL = 16
CAP = 32
GROUP = 8
SLOTS = LOCAL * CAP
KC = 512
NK = WIDTH // KC
NB = 4
CC = 256
NC = WIDTH // CC
NBD = 8
LAG = 2

OWN = 0
PBUF = 64
DRECV = 80
RA1 = 144
RB1 = 160
RA2 = 176
RB2 = 184
NBLK = 192


def capacity(rows, top_k, experts):
    return ((CAP_FACTOR * rows * top_k + 8 * experts - 1) // (8 * experts)) * 8


def layer_kernel(
    r_ref, tok_ref, wg_ref, wu_ref, wd_ref, out_ref,
    rall, rt, xall, pmat, gbuf, big, wbuf, hbuf, dbuf, ybuf,
    lsem, rs_sem, rr_sem, xs_sem, xr_sem, w_sem, d_sem,
    ds_sem, dr_sem, is_sem, ir_sem, ready,
):
    data = lax.axis_index("data")
    y = lax.axis_index("node")
    ex = lax.axis_index("expert")
    x = ex // 2
    q = ex % 2
    g = y * 4 + ex
    flip = 1 - 2 * q
    gx = y * 4 + (1 - x) * 2 + q
    gy = (1 - y) * 4 + x * 2 + q
    gd = (1 - y) * 4 + (1 - x) * 2 + q
    gp = g + flip
    partner = (data, y, ex + flip)
    xn = (data, y, (1 - x) * 2 + q)
    yn = (data, 1 - y, ex)

    barrier = pltpu.get_barrier_semaphore()
    for d in range(1, GROUP):
        t = (g + d) % GROUP
        pl.semaphore_signal(barrier, inc=1, device_id=(data, t // 4, t % 4), device_id_type=MESH)

    def own_load(k):
        return pltpu.make_async_copy(
            tok_ref.at[:, pl.ds(k * KC, KC)],
            xall.at[pl.ds(pl.multiple_of((k * GROUP + g) * ROWS, ROWS), ROWS), :],
            lsem.at[k],
        )

    for k in range(NK):
        own_load(k).start()

    def w_load(i):
        k, e, slot = i // LOCAL, i % LOCAL, i % NB
        rows = pl.ds(pl.multiple_of(k * KC, KC), KC)
        return [
            pltpu.make_async_copy(ref.at[e, rows, :], wbuf.at[slot, j], w_sem.at[slot, j])
            for j, ref in enumerate((wg_ref, wu_ref))
        ]

    def d_load(i):
        c, e, slot = i // LOCAL, i % LOCAL, i % NBD
        cols = pl.ds(pl.multiple_of(c * CC, CC), CC)
        return pltpu.make_async_copy(wd_ref.at[e, :, cols], dbuf.at[slot], d_sem.at[slot])

    for i in range(NB):
        for cp in w_load(i):
            cp.start()
    for i in range(NBD):
        d_load(i).start()

    rall[pl.ds(pl.multiple_of(g * 16, 16), 16), :] = r_ref[...]
    pl.semaphore_wait(barrier, GROUP - 1)

    def r_copy(d, owner, dst):
        return pltpu.make_async_remote_copy(
            src_ref=r_ref,
            dst_ref=rall.at[pl.ds(pl.multiple_of(owner * 16, 16), 16), :],
            send_sem=rs_sem.at[d - 1],
            recv_sem=rr_sem.at[d - 1],
            device_id=(data, dst // 4, dst % 4),
            device_id_type=MESH,
        )

    for d in range(1, GROUP):
        r_copy(d, g, (g + d) % GROUP).start()

    def x_copy(i, k, s, dev, lo=0, n=ROWS):
        ref = xall.at[pl.ds(pl.multiple_of((k * GROUP + s) * ROWS + lo, 128), n), :]
        return pltpu.make_async_remote_copy(
            src_ref=ref, dst_ref=ref, send_sem=xs_sem.at[i, k], recv_sem=xr_sem.at[i, k],
            device_id=dev, device_id_type=MESH,
        )

    HALF = ROWS // 2

    def send(i, k):
        return x_copy(i, k, *(
            (g, partner),
            (g, xn),
            (g, yn),
            (gx, yn, 0, HALF),
            (gx, partner),
            (gy, xn, HALF, HALF),
            (gy, partner),
            (gd, partner),
        )[i])

    def arrival(i, k):
        return x_copy(i, k, *(
            (gp, partner),
            (gx, xn),
            (gy, yn),
            (gd, yn, 0, HALF),
            (gx + flip, partner),
            (gd, xn, HALF, HALF),
            (gy + flip, partner),
            (gd + flip, partner),
        )[i])

    def own(k):
        own_load(k).wait()
        for i in (1, 2, 0):
            send(i, k).start()

    def forward(k):
        arrival(1, k).wait_recv()
        send(3, k).start()
        send(4, k).start()
        arrival(2, k).wait_recv()
        send(5, k).start()
        send(6, k).start()

    def finish(k):
        arrival(3, k).wait_recv()
        arrival(5, k).wait_recv()
        send(7, k).start()
        for i in (0, 4, 6, 7):
            arrival(i, k).wait_recv()

    own(0)

    for d in range(1, GROUP):
        r_copy(d, (g + GROUP - d) % GROUP, g).wait_recv()
    rt[...] = jnp.transpose(rall[...])

    base = (g * SLOTS).astype(F32)
    PB = 64

    def build_p(i, carry):
        s, b = i // (SLOTS // PB), i % (SLOTS // PB)
        want = lax.broadcasted_iota(jnp.int32, (PB, ROWS), 0).astype(F32) + (base + (b * PB).astype(F32))
        pos = rall[pl.ds(pl.multiple_of(s * 16, 16), 8), :]
        hit = jnp.zeros((PB, ROWS), F32)
        for j in range(8):
            hit = jnp.where(pos[j : j + 1, :] == want, 1.0, hit)
        pmat[pl.ds(pl.multiple_of(i * PB, PB), PB), :] = hit.astype(BF16)
        return carry

    lax.fori_loop(0, GROUP * SLOTS // PB, build_p, 0)

    forward(0)
    own(1)
    finish(0)

    def build_g(i):
        s, half = i % GROUP, i // GROUP
        t0 = pl.multiple_of(half * 128, 128)
        v = pltpu.roll(rt[pl.ds(t0, 128), :], (128 - s * 16) % 128, 1)
        want = lax.broadcasted_iota(jnp.int32, (128, SLOTS), 1).astype(F32) + base
        sel = jnp.zeros((128, SLOTS), F32)
        for j in range(8):
            sel = jnp.where(v[:, j : j + 1] == want, v[:, 8 + j : 9 + j], sel)
        g1 = (sel * (1.0 - 2.0**-8)).astype(BF16)
        rest = sel - g1.astype(F32)
        g2 = rest.astype(BF16)
        g3 = (rest - g2.astype(F32)).astype(BF16)
        for p, part in enumerate((g1, g2, g3)):
            xall[pl.ds(pl.multiple_of(s * 768 + p * 256 + t0, 128), 128), :] = part

    def gather_rows(k):
        def body(i, carry):
            s, m = i // 2, i % 2
            pm = pmat[pl.ds(pl.multiple_of(i * 256, 256), 256), :]
            xs = xall[pl.ds(pl.multiple_of((k * GROUP + s) * ROWS, ROWS), ROWS), :]
            got = jnp.dot(pm, xs, preferred_element_type=F32).astype(BF16)
            gbuf[s, pl.ds(pl.multiple_of(m * 256, 256), 256), :] = got
            return carry

        lax.fori_loop(0, 2 * GROUP, body, 0)

    def block(i, n=1):
        return pl.ds(pl.multiple_of(i * 256, 256), n * 256)

    def experts(k, lo, hi):
        def body(e, carry):
            i = k * LOCAL + e
            slot = i % NB
            for cp in w_load(i):
                cp.wait()
            lhs = gbuf[:, pl.ds(pl.multiple_of(e * CAP, CAP), CAP), :].reshape(GROUP * CAP, KC)
            for n in range(FF // 256):
                vals = []
                for j in range(2):
                    v = jnp.dot(lhs, wbuf[slot, j, :, n * 256 : (n + 1) * 256], preferred_element_type=F32)
                    at = e * 12 + j * 6 + n * 2
                    if k > 0:
                        v = v + jnp.concatenate([big[block(at), :], big[block(at + 1), :]], axis=1)
                    if k < NK - 1:
                        big[block(at), :] = v[:, :128]
                        big[block(at + 1), :] = v[:, 128:]
                    vals.append(v)
                if k == NK - 1:
                    hbuf[e, :, n * 256 : (n + 1) * 256] = (jax.nn.silu(vals[0]) * vals[1]).astype(BF16)
            if k == NK - 1:
                build_g(e)

            @pl.when(i + NB < NK * LOCAL)
            def _():
                for cp in w_load(i + NB):
                    cp.start()

            return carry

        lax.fori_loop(lo, hi, body, 0)

    for k in range(NK):
        if k == NK - 1:
            for kk in range(NK - 1):
                for i in range(8):
                    send(i, kk).wait_send()
        gather_rows(k)
        experts(k, 0, 8)
        if k < NK - 1:
            forward(k + 1)
        if k < NK - 2:
            own(k + 2)
        experts(k, 8, LOCAL)
        if k < NK - 1:
            finish(k + 1)

    for dev in (partner, xn, yn):
        pl.semaphore_signal(ready, inc=1, device_id=dev, device_id_type=MESH)

    def part(core, d, to):
        dx, dy = d % 2, d // 2
        s = ((y + dy) % 2) * 4 + ((x + dx) % 2) * 2 + core
        ys = ybuf[s]
        gs = xall[pl.ds(pl.multiple_of(s * 768, 256), 768), :]
        v = jnp.dot(gs, ys, preferred_element_type=F32)
        v = v[0:256] + (v[256:512] + v[512:768])
        big[block(to + dx * 2 + dy), :] = v[:, :128]
        big[block(to + 4 + dy * 2 + dx), :] = v[:, 128:]

    def d2d(c):
        return pltpu.make_async_remote_copy(
            src_ref=big.at[block(PBUF + (c % 2) * 8, 8), :],
            dst_ref=big.at[block(DRECV + c * 8, 8), :],
            send_sem=ds_sem.at[c], recv_sem=dr_sem.at[c],
            device_id=partner, device_id_type=MESH,
        )

    def ici(i, c):
        src, dst, n, dev = (
            (OWN + c * 8 + 2, RA1 + c * 2, 2, xn),
            (OWN + c * 8 + 6, RB1 + c * 2, 2, yn),
            (OWN + c * 8 + 1, RA2 + c, 1, yn),
            (OWN + c * 8 + 5, RB2 + c, 1, xn),
        )[i]
        return pltpu.make_async_remote_copy(
            src_ref=big.at[block(src, n), :], dst_ref=big.at[block(dst, n), :],
            send_sem=is_sem.at[i, c], recv_sem=ir_sem.at[i, c],
            device_id=dev, device_id_type=MESH,
        )

    def second_hop(c):
        ici(0, c).wait_recv()
        big[block(OWN + c * 8 + 1), :] = big[block(OWN + c * 8 + 1), :] + big[block(RA1 + c * 2 + 1), :]
        ici(2, c).start()
        ici(1, c).wait_recv()
        big[block(OWN + c * 8 + 5), :] = big[block(OWN + c * 8 + 5), :] + big[block(RB1 + c * 2 + 1), :]
        ici(3, c).start()

    def column_chunk(c, carry):
        def down(e, inner):
            i = c * LOCAL + e
            d_load(i).wait()
            v = jnp.dot(hbuf[e], dbuf[i % NBD], preferred_element_type=F32).astype(BF16)
            ybuf[:, pl.ds(pl.multiple_of(e * CAP, CAP), CAP), :] = v.reshape(GROUP, CAP, CC)

            @pl.when(i + NBD < NC * LOCAL)
            def _():
                d_load(i + NBD).start()

            return inner

        lax.fori_loop(0, LOCAL, down, 0)

        @pl.when(c >= 2)
        def _():
            d2d(c - 2).wait_send()

        def theirs(d, inner):
            part(1 - q, d, PBUF + (c % 2) * 8)
            return inner

        lax.fori_loop(0, 4, theirs, 0)

        @pl.when(c == 0)
        def _():
            pl.semaphore_wait(ready, 3)

        d2d(c).start()

        def ours(d, inner):
            part(q, d, OWN + c * 8)
            return inner

        lax.fori_loop(0, 4, ours, 0)

        @pl.when(c >= LAG)
        def _():
            second_hop(c - LAG)

        d2d(c).wait_recv()

        def add(b, inner):
            big[block(OWN + c * 8 + b), :] = big[block(OWN + c * 8 + b), :] + big[block(DRECV + c * 8 + b), :]
            return inner

        lax.fori_loop(0, 8, add, 0)
        ici(0, c).start()
        ici(1, c).start()
        return carry

    lax.fori_loop(0, NC, column_chunk, 0)

    def tail(c, carry):
        second_hop(c)
        return carry

    lax.fori_loop(NC - LAG, NC, tail, 0)

    def final(c, carry):
        ici(2, c).wait_recv()
        a = big[block(OWN + c * 8), :] + big[block(RA1 + c * 2), :] + big[block(RA2 + c), :]
        ici(3, c).wait_recv()
        b = big[block(OWN + c * 8 + 4), :] + big[block(RB1 + c * 2), :] + big[block(RB2 + c), :]
        out_ref[:, pl.ds(pl.multiple_of(c * CC, CC), 128)] = a.astype(BF16)
        out_ref[:, pl.ds(pl.multiple_of(c * CC + 128, 128), 128)] = b.astype(BF16)
        for i in range(4):
            ici(i, c).wait_send()
        return carry

    lax.fori_loop(0, NC, final, 0)

    for c in (NC - 2, NC - 1):
        d2d(c).wait_send()
    for i in range(8):
        send(i, NK - 1).wait_send()
    for d in range(1, GROUP):
        r_copy(d, g, (g + d) % GROUP).wait_send()


def solution(mesh):
    group_axes = ("node", "expert")
    group_size = mesh.shape["node"] * mesh.shape["expert"]
    tok_spec = P(("data", "node", "expert"), None)
    weight_spec = P(("node", "expert"), None, None)

    def local_layer(tokens, expert_ids, gate_weights, slot_ids, w_gate, w_up, w_down):
        rows, width = tokens.shape
        top_k = expert_ids.shape[1]
        local_experts = w_gate.shape[0]
        slot_count = capacity(rows, top_k, local_experts * group_size)
        assert (rows, width, local_experts, slot_count, group_size) == (ROWS, WIDTH, LOCAL, CAP, GROUP)
        flat_pos = jnp.where(slot_ids >= 0, expert_ids * slot_count + slot_ids, -1)
        routing = jnp.concatenate([flat_pos.astype(F32), gate_weights], axis=1).T

        vmem = pl.BlockSpec(memory_space=pltpu.VMEM)
        hbm = pl.BlockSpec(memory_space=pl.ANY)
        dma = pltpu.SemaphoreType.DMA
        return pl.pallas_call(
            layer_kernel,
            out_shape=jax.ShapeDtypeStruct((rows, width), BF16),
            in_specs=[vmem, hbm, hbm, hbm, hbm],
            out_specs=vmem,
            scratch_shapes=[
                pltpu.VMEM((GROUP * 16, ROWS), F32),
                pltpu.VMEM((ROWS, GROUP * 16), F32),
                pltpu.VMEM((NK * GROUP * ROWS, KC), BF16),
                pltpu.VMEM((GROUP * SLOTS, ROWS), BF16),
                pltpu.VMEM((GROUP, SLOTS, KC), BF16),
                pltpu.VMEM((NBLK * 256, 128), F32),
                pltpu.VMEM((NB, 2, KC, FF), BF16),
                pltpu.VMEM((LOCAL, GROUP * CAP, FF), BF16),
                pltpu.VMEM((NBD, FF, CC), BF16),
                pltpu.VMEM((GROUP, SLOTS, CC), BF16),
                dma((NK,)),
                dma((GROUP - 1,)),
                dma((GROUP - 1,)),
                dma((8, NK)),
                dma((8, NK)),
                dma((NB, 2)),
                dma((NBD,)),
                dma((NC,)),
                dma((NC,)),
                dma((4, NC)),
                dma((4, NC)),
                pltpu.SemaphoreType.REGULAR,
            ],
            compiler_params=pltpu.CompilerParams(
                collective_id=0, has_side_effects=True, vmem_limit_bytes=67043328,
            ),
            cost_estimate=pl.CostEstimate(
                flops=6 * LOCAL * GROUP * CAP * WIDTH * FF,
                bytes_accessed=6 * LOCAL * WIDTH * FF,
                transcendentals=LOCAL * GROUP * CAP * FF,
            ),
            name="moe_layer",
        )(routing, tokens, w_gate, w_up, w_down)

    return jax.shard_map(local_layer, mesh=mesh, in_specs=(tok_spec, tok_spec, tok_spec, tok_spec, weight_spec, weight_spec, weight_spec), out_specs=tok_spec, check_vma=False)
```

```python
import jax
import jax.numpy as jnp
from jax import lax
from jax.experimental import pallas as pl
from jax.experimental.pallas import tpu as pltpu
from jax.sharding import PartitionSpec as P

CAP_FACTOR = 2
MESH = pl.DeviceIdType.MESH
F32 = jnp.float32
BF16 = jnp.bfloat16

ROWS = 256
WIDTH = 2048
FF = 768
LOCAL = 16
CAP = 32
GROUP = 8
SLOTS = LOCAL * CAP
KC = 256
NK = WIDTH // KC
NB = 10
CC = 256
NC = WIDTH // CC
NBD = 8
LAG = 2

OWN = 0
PBUF = 64
DRECV = 80
RA1 = 144
RB1 = 160
RA2 = 176
RB2 = 184
NBLK = 192


def capacity(rows, top_k, experts):
    return ((CAP_FACTOR * rows * top_k + 8 * experts - 1) // (8 * experts)) * 8


def layer_kernel(
    id_ref, slot_ref, gate_ref, tok_ref, wg_ref, wu_ref, wd_ref, out_ref,
    rall, rt, xall, pmat, gmat, gbuf, big, wbuf, hbuf, dbuf,
    lsem, rs_sem, rr_sem, xs_sem, xr_sem, w_sem, d_sem,
    ds_sem, dr_sem, is_sem, ir_sem, ready,
):
    data = lax.axis_index("data")
    y = lax.axis_index("node")
    ex = lax.axis_index("expert")
    x = ex // 2
    q = ex % 2
    g = y * 4 + ex
    flip = 1 - 2 * q
    gx = y * 4 + (1 - x) * 2 + q
    gy = (1 - y) * 4 + x * 2 + q
    gd = (1 - y) * 4 + (1 - x) * 2 + q
    gp = g + flip
    partner = (data, y, ex + flip)
    xn = (data, y, (1 - x) * 2 + q)
    yn = (data, 1 - y, ex)

    barrier = pltpu.get_barrier_semaphore()
    for d in range(1, GROUP):
        t = (g + d) % GROUP
        pl.semaphore_signal(barrier, inc=1, device_id=(data, t // 4, t % 4), device_id_type=MESH)

    def own_load(k):
        return pltpu.make_async_copy(
            tok_ref.at[:, pl.ds(k * KC, KC)],
            xall.at[pl.ds(pl.multiple_of((k * GROUP + g) * ROWS, ROWS), ROWS), :],
            lsem.at[k],
        )

    for k in range(NK):
        own_load(k).start()

    def w_load(i):
        k, e, slot = i // LOCAL, i % LOCAL, i % NB
        rows = pl.ds(pl.multiple_of(k * KC, KC), KC)
        return [
            pltpu.make_async_copy(ref.at[e, rows, :], wbuf.at[slot, j], w_sem.at[slot, j])
            for j, ref in enumerate((wg_ref, wu_ref))
        ]

    def d_load(i):
        c, e, slot = i // LOCAL, i % LOCAL, i % NBD
        cols = pl.ds(pl.multiple_of(c * CC, CC), CC)
        return pltpu.make_async_copy(wd_ref.at[e, :, cols], dbuf.at[slot], d_sem.at[slot])

    for i in range(NB):
        for cp in w_load(i):
            cp.start()
    for i in range(NBD):
        d_load(i).start()

    mine = pl.multiple_of(g * 16, 16)
    flat_pos = jnp.where(slot_ref[...] >= 0, id_ref[...] * CAP + slot_ref[...], -1)
    rall[pl.ds(mine, 8), :] = flat_pos.astype(F32)
    rall[pl.ds(mine + 8, 8), :] = gate_ref[...]
    pl.semaphore_wait(barrier, GROUP - 1)

    def r_copy(d, owner, dst):
        ref = rall.at[pl.ds(pl.multiple_of(owner * 16, 16), 16), :]
        return pltpu.make_async_remote_copy(
            src_ref=ref,
            dst_ref=ref,
            send_sem=rs_sem.at[d - 1],
            recv_sem=rr_sem.at[d - 1],
            device_id=(data, dst // 4, dst % 4),
            device_id_type=MESH,
        )

    for d in range(1, GROUP):
        r_copy(d, g, (g + d) % GROUP).start()

    def x_copy(i, k, s, dev, lo=0, n=ROWS):
        ref = xall.at[pl.ds(pl.multiple_of((k * GROUP + s) * ROWS + lo, 128), n), :]
        return pltpu.make_async_remote_copy(
            src_ref=ref, dst_ref=ref, send_sem=xs_sem.at[i, k], recv_sem=xr_sem.at[i, k],
            device_id=dev, device_id_type=MESH,
        )

    HALF = ROWS // 2

    def send(i, k):
        return x_copy(i, k, *(
            (g, partner),
            (g, xn),
            (g, yn),
            (gx, yn, 0, HALF),
            (gx, partner),
            (gy, xn, HALF, HALF),
            (gy, partner),
            (gd, partner),
        )[i])

    def arrival(i, k):
        return x_copy(i, k, *(
            (gp, partner),
            (gx, xn),
            (gy, yn),
            (gd, yn, 0, HALF),
            (gx + flip, partner),
            (gd, xn, HALF, HALF),
            (gy + flip, partner),
            (gd + flip, partner),
        )[i])

    def own(k):
        own_load(k).wait()
        for i in (1, 2, 0):
            send(i, k).start()

    def forward(k):
        arrival(1, k).wait_recv()
        send(3, k).start()
        send(4, k).start()
        arrival(2, k).wait_recv()
        send(5, k).start()
        send(6, k).start()

    def finish(k):
        arrival(3, k).wait_recv()
        arrival(5, k).wait_recv()
        send(7, k).start()
        for i in (0, 4, 6, 7):
            arrival(i, k).wait_recv()

    own(0)
    own(1)

    for d in range(1, GROUP):
        r_copy(d, (g + GROUP - d) % GROUP, g).wait_recv()
    rt[...] = jnp.transpose(rall[...])

    base = (g * SLOTS).astype(F32)
    ybuf = pmat
    PB = 64
    GB = 64

    def build_p(i, carry):
        s, b = i // (SLOTS // PB), i % (SLOTS // PB)
        want = lax.broadcasted_iota(jnp.int32, (PB, ROWS), 0).astype(F32) + (base + (b * PB).astype(F32))
        pos = rall[pl.ds(pl.multiple_of(s * 16, 16), 8), :]
        hit = jnp.zeros((PB, ROWS), F32)
        for j in range(8):
            hit = jnp.where(pos[j : j + 1, :] == want, 1.0, hit)
        pmat[s, pl.ds(pl.multiple_of(b * PB, PB), PB), :] = hit.astype(BF16)
        return carry

    def build_g(i, carry):
        s, b = i % GROUP, i // GROUP
        t0 = pl.multiple_of(b * GB, GB)
        v = pltpu.roll(rt[pl.ds(t0, GB), :], (128 - s * 16) % 128, 1)
        want = lax.broadcasted_iota(jnp.int32, (GB, SLOTS), 1).astype(F32) + base
        sel = jnp.zeros((GB, SLOTS), F32)
        for j in range(8):
            sel = jnp.where(v[:, j : j + 1] == want, v[:, 8 + j : 9 + j], sel)
        g1 = (sel * (1.0 - 2.0**-8)).astype(BF16)
        rest = sel - g1.astype(F32)
        g2 = rest.astype(BF16)
        g3 = (rest - g2.astype(F32)).astype(BF16)
        for p, part in enumerate((g1, g2, g3)):
            gmat[s, pl.ds(pl.multiple_of(p * 256 + t0, GB), GB), :] = part
        return carry

    lax.fori_loop(0, GROUP * SLOTS // PB, build_p, 0)
    forward(0)
    own(2)
    gn = GROUP * ROWS // GB
    lax.fori_loop(0, gn // 2, build_g, 0)
    forward(1)
    own(3)
    lax.fori_loop(gn // 2, gn, build_g, 0)
    finish(0)

    def gather_rows(k):
        def body(i, carry):
            for s in (2 * i, 2 * i + 1):
                xs = xall[pl.ds(pl.multiple_of((k * GROUP + s) * ROWS, ROWS), ROWS), :]
                gbuf[s] = jnp.dot(pmat[s], xs, preferred_element_type=F32).astype(BF16)
            return carry

        lax.fori_loop(0, GROUP // 2, body, 0)

    def block(i, n=1):
        return pl.ds(pl.multiple_of(i * 256, 256), n * 256)

    def down(c, e):
        i = c * LOCAL + e
        d_load(i).wait()
        v = jnp.dot(hbuf[e], dbuf[i % NBD], preferred_element_type=F32).astype(BF16)
        ybuf[:, pl.ds(pl.multiple_of(e * CAP, CAP), CAP), :] = v.reshape(GROUP, CAP, CC)

        @pl.when(i + NBD < NC * LOCAL)
        def _():
            d_load(i + NBD).start()

    def experts(k):
        def body(e, carry):
            i = k * LOCAL + e
            slot = i % NB
            for cp in w_load(i):
                cp.wait()
            lhs = gbuf[:, pl.ds(pl.multiple_of(e * CAP, CAP), CAP), :].reshape(GROUP * CAP, KC)
            for n in range(FF // 256):
                vals = []
                for j in range(2):
                    v = jnp.dot(lhs, wbuf[slot, j, :, n * 256 : (n + 1) * 256], preferred_element_type=F32)
                    at = e * 12 + j * 6 + n * 2
                    if k > 0:
                        v = v + jnp.concatenate([big[block(at), :], big[block(at + 1), :]], axis=1)
                    if k < NK - 1:
                        big[block(at), :] = v[:, :128]
                        big[block(at + 1), :] = v[:, 128:]
                    vals.append(v)
                if k == NK - 1:
                    hbuf[e, :, n * 256 : (n + 1) * 256] = (jax.nn.silu(vals[0]) * vals[1]).astype(BF16)
            if k == NK - 1:
                down(0, e)

            @pl.when(i + NB < NK * LOCAL)
            def _():
                for cp in w_load(i + NB):
                    cp.start()

            return carry

        lax.fori_loop(0, LOCAL, body, 0)

    for k in range(NK):
        gather_rows(k)
        experts(k)
        if k + 2 < NK:
            forward(k + 2)
        if k + 4 < NK:
            own(k + 4)
        if k + 1 < NK:
            finish(k + 1)

    for dev in (partner, xn, yn):
        pl.semaphore_signal(ready, inc=1, device_id=dev, device_id_type=MESH)

    def part(core, d, to):
        dx, dy = d % 2, d // 2
        s = ((y + dy) % 2) * 4 + ((x + dx) % 2) * 2 + core
        ys = ybuf[s]
        v = jnp.dot(gmat[s], ys, preferred_element_type=F32)
        v = v[0:256] + (v[256:512] + v[512:768])
        big[block(to + dx * 2 + dy), :] = v[:, :128]
        big[block(to + 4 + dy * 2 + dx), :] = v[:, 128:]

    def d2d(c):
        return pltpu.make_async_remote_copy(
            src_ref=big.at[block(PBUF + (c % 2) * 8, 8), :],
            dst_ref=big.at[block(DRECV + c * 8, 8), :],
            send_sem=ds_sem.at[c], recv_sem=dr_sem.at[c],
            device_id=partner, device_id_type=MESH,
        )

    def ici(i, c):
        src, dst, n, dev = (
            (OWN + c * 8 + 2, RA1 + c * 2, 2, xn),
            (OWN + c * 8 + 6, RB1 + c * 2, 2, yn),
            (OWN + c * 8 + 1, RA2 + c, 1, yn),
            (OWN + c * 8 + 5, RB2 + c, 1, xn),
        )[i]
        return pltpu.make_async_remote_copy(
            src_ref=big.at[block(src, n), :], dst_ref=big.at[block(dst, n), :],
            send_sem=is_sem.at[i, c], recv_sem=ir_sem.at[i, c],
            device_id=dev, device_id_type=MESH,
        )

    def second_hop(c):
        ici(0, c).wait_recv()
        big[block(OWN + c * 8 + 1), :] = big[block(OWN + c * 8 + 1), :] + big[block(RA1 + c * 2 + 1), :]
        ici(2, c).start()
        ici(1, c).wait_recv()
        big[block(OWN + c * 8 + 5), :] = big[block(OWN + c * 8 + 5), :] + big[block(RB1 + c * 2 + 1), :]
        ici(3, c).start()

    def column_chunk(c, carry):
        @pl.when(c > 0)
        def _():
            def one(e, inner):
                down(c, e)
                return inner

            lax.fori_loop(0, LOCAL, one, 0)

        @pl.when(c >= 2)
        def _():
            d2d(c - 2).wait_send()

        def theirs(d, inner):
            part(1 - q, d, PBUF + (c % 2) * 8)
            return inner

        lax.fori_loop(0, 4, theirs, 0)

        @pl.when(c == 0)
        def _():
            pl.semaphore_wait(ready, 3)

        d2d(c).start()

        def ours(d, inner):
            part(q, d, OWN + c * 8)
            return inner

        lax.fori_loop(0, 4, ours, 0)

        @pl.when(c >= LAG)
        def _():
            second_hop(c - LAG)

        d2d(c).wait_recv()

        def add(b, inner):
            big[block(OWN + c * 8 + b), :] = big[block(OWN + c * 8 + b), :] + big[block(DRECV + c * 8 + b), :]
            return inner

        lax.fori_loop(0, 8, add, 0)
        ici(0, c).start()
        ici(1, c).start()
        return carry

    lax.fori_loop(0, NC, column_chunk, 0)

    def tail(c, carry):
        second_hop(c)
        return carry

    lax.fori_loop(NC - LAG, NC, tail, 0)

    def final(c, carry):
        ici(2, c).wait_recv()
        a = big[block(OWN + c * 8), :] + big[block(RA1 + c * 2), :] + big[block(RA2 + c), :]
        ici(3, c).wait_recv()
        b = big[block(OWN + c * 8 + 4), :] + big[block(RB1 + c * 2), :] + big[block(RB2 + c), :]
        out_ref[:, pl.ds(pl.multiple_of(c * CC, CC), 128)] = a.astype(BF16)
        out_ref[:, pl.ds(pl.multiple_of(c * CC + 128, 128), 128)] = b.astype(BF16)
        for i in range(4):
            ici(i, c).wait_send()
        return carry

    lax.fori_loop(0, NC, final, 0)

    for c in (NC - 2, NC - 1):
        d2d(c).wait_send()
    for k in range(NK):
        for i in range(8):
            send(i, k).wait_send()
    for d in range(1, GROUP):
        r_copy(d, g, (g + d) % GROUP).wait_send()


def solution(mesh):
    group_axes = ("node", "expert")
    group_size = mesh.shape["node"] * mesh.shape["expert"]
    tok_spec = P(("data", "node", "expert"), None)
    weight_spec = P(("node", "expert"), None, None)

    def local_layer(tokens, expert_ids, gate_weights, slot_ids, w_gate, w_up, w_down):
        rows, width = tokens.shape
        top_k = expert_ids.shape[1]
        local_experts = w_gate.shape[0]
        slot_count = capacity(rows, top_k, local_experts * group_size)
        assert (rows, width, local_experts, slot_count, group_size) == (ROWS, WIDTH, LOCAL, CAP, GROUP)
        vmem = pl.BlockSpec(memory_space=pltpu.VMEM)
        hbm = pl.BlockSpec(memory_space=pl.ANY)
        dma = pltpu.SemaphoreType.DMA
        return pl.pallas_call(
            layer_kernel,
            out_shape=jax.ShapeDtypeStruct((rows, width), BF16),
            in_specs=[vmem, vmem, vmem, hbm, hbm, hbm, hbm],
            out_specs=vmem,
            scratch_shapes=[
                pltpu.VMEM((GROUP * 16, ROWS), F32),
                pltpu.VMEM((ROWS, GROUP * 16), F32),
                pltpu.VMEM((NK * GROUP * ROWS, KC), BF16),
                pltpu.VMEM((GROUP, SLOTS, ROWS), BF16),
                pltpu.VMEM((GROUP, 3 * ROWS, SLOTS), BF16),
                pltpu.VMEM((GROUP, SLOTS, KC), BF16),
                pltpu.VMEM((NBLK * 256, 128), F32),
                pltpu.VMEM((NB, 2, KC, FF), BF16),
                pltpu.VMEM((LOCAL, GROUP * CAP, FF), BF16),
                pltpu.VMEM((NBD, FF, CC), BF16),
                dma((NK,)),
                dma((GROUP - 1,)),
                dma((GROUP - 1,)),
                dma((8, NK)),
                dma((8, NK)),
                dma((NB, 2)),
                dma((NBD,)),
                dma((NC,)),
                dma((NC,)),
                dma((4, NC)),
                dma((4, NC)),
                pltpu.SemaphoreType.REGULAR,
            ],
            compiler_params=pltpu.CompilerParams(
                collective_id=0, has_side_effects=True, vmem_limit_bytes=67043328,
            ),
            cost_estimate=pl.CostEstimate(
                flops=6 * LOCAL * GROUP * CAP * WIDTH * FF,
                bytes_accessed=6 * LOCAL * WIDTH * FF,
                transcendentals=LOCAL * GROUP * CAP * FF,
            ),
            name="moe_layer",
        )(expert_ids.T, slot_ids.T, gate_weights.T, tokens, w_gate, w_up, w_down)

    return jax.shard_map(local_layer, mesh=mesh, in_specs=(tok_spec, tok_spec, tok_spec, tok_spec, weight_spec, weight_spec, weight_spec), out_specs=tok_spec, check_vma=False)
```

```python
import jax
import jax.numpy as jnp
from jax import lax
from jax.experimental import pallas as pl
from jax.experimental.pallas import tpu as pltpu
from jax.sharding import PartitionSpec as P

CAP_FACTOR = 2
MESH = pl.DeviceIdType.MESH
F32 = jnp.float32
BF16 = jnp.bfloat16

ROWS = 256
WIDTH = 2048
FF = 768
LOCAL = 16
CAP = 32
GROUP = 8
SLOTS = LOCAL * CAP
KC = 256
NK = WIDTH // KC
U = 4
NB = 3
CC = 256
NC = WIDTH // CC
NBD = 2
LAG = 2

OWN = 0
PBUF = 64
DRECV = 80
RA1 = 144
RB1 = 160
RA2 = 176
RB2 = 184
NBLK = 192


def capacity(rows, top_k, experts):
    return ((CAP_FACTOR * rows * top_k + 8 * experts - 1) // (8 * experts)) * 8


def layer_kernel(
    id_ref, slot_ref, gate_ref, tok_ref, wg_ref, wu_ref, wd_ref, out_ref,
    rall, rt, xall, pmat, gmat, gbuf, big, wbuf, hbuf, dbuf,
    lsem, rs_sem, rr_sem, xs_sem, xr_sem, w_sem, d_sem,
    ds_sem, dr_sem, is_sem, ir_sem, ready,
):
    data = lax.axis_index("data")
    y = lax.axis_index("node")
    ex = lax.axis_index("expert")
    x = ex // 2
    q = ex % 2
    g = y * 4 + ex
    flip = 1 - 2 * q
    gx = y * 4 + (1 - x) * 2 + q
    gy = (1 - y) * 4 + x * 2 + q
    gd = (1 - y) * 4 + (1 - x) * 2 + q
    gp = g + flip
    partner = (data, y, ex + flip)
    xn = (data, y, (1 - x) * 2 + q)
    yn = (data, 1 - y, ex)

    barrier = pltpu.get_barrier_semaphore()
    for d in range(1, GROUP):
        t = (g + d) % GROUP
        pl.semaphore_signal(barrier, inc=1, device_id=(data, t // 4, t % 4), device_id_type=MESH)

    def own_load(k):
        return pltpu.make_async_copy(
            tok_ref.at[:, pl.ds(pl.multiple_of(k * KC, KC), KC)],
            xall.at[pl.ds(pl.multiple_of((k * GROUP + g) * ROWS, ROWS), ROWS), :],
            lsem.at[k],
        )

    for k in range(NK):
        own_load(k).start()

    steps = LOCAL // U

    def w_load(i):
        k, e, slot = i // steps, (i % steps) * U, i % NB
        rows = pl.ds(pl.multiple_of(k * KC, KC), KC)
        return [
            pltpu.make_async_copy(ref.at[pl.ds(e, U), rows, :], wbuf.at[slot, j], w_sem.at[slot, j])
            for j, ref in enumerate((wg_ref, wu_ref))
        ]

    def d_load(i):
        c, e, slot = i // steps, (i % steps) * U, i % NBD
        cols = pl.ds(pl.multiple_of(c * CC, CC), CC)
        return pltpu.make_async_copy(wd_ref.at[pl.ds(e, U), :, cols], dbuf.at[slot], d_sem.at[slot])

    for i in range(NB):
        for cp in w_load(i):
            cp.start()
    for i in range(NBD):
        d_load(i).start()

    mine = pl.multiple_of(g * 16, 16)
    flat_pos = jnp.where(slot_ref[...] >= 0, id_ref[...] * CAP + slot_ref[...], -1)
    rall[pl.ds(mine, 8), :] = flat_pos.astype(F32)
    rall[pl.ds(mine + 8, 8), :] = gate_ref[...]
    pl.semaphore_wait(barrier, GROUP - 1)

    def r_copy(d, owner, dst):
        ref = rall.at[pl.ds(pl.multiple_of(owner * 16, 16), 16), :]
        return pltpu.make_async_remote_copy(
            src_ref=ref,
            dst_ref=ref,
            send_sem=rs_sem.at[d - 1],
            recv_sem=rr_sem.at[d - 1],
            device_id=(data, dst // 4, dst % 4),
            device_id_type=MESH,
        )

    for d in range(1, GROUP):
        r_copy(d, g, (g + d) % GROUP).start()

    def x_copy(i, k, s, dev, lo=0, n=ROWS):
        ref = xall.at[pl.ds(pl.multiple_of((k * GROUP + s) * ROWS + lo, 128), n), :]
        return pltpu.make_async_remote_copy(
            src_ref=ref, dst_ref=ref, send_sem=xs_sem.at[i, k], recv_sem=xr_sem.at[i, k],
            device_id=dev, device_id_type=MESH,
        )

    HALF = ROWS // 2

    def send(i, k):
        return x_copy(i, k, *(
            (g, partner),
            (g, xn),
            (g, yn),
            (gx, yn, 0, HALF),
            (gx, partner),
            (gy, xn, HALF, HALF),
            (gy, partner),
            (gd, partner),
        )[i])

    def arrival(i, k):
        return x_copy(i, k, *(
            (gp, partner),
            (gx, xn),
            (gy, yn),
            (gd, yn, 0, HALF),
            (gx + flip, partner),
            (gd, xn, HALF, HALF),
            (gy + flip, partner),
            (gd + flip, partner),
        )[i])

    def own(k):
        own_load(k).wait()
        for i in (1, 2, 0):
            send(i, k).start()

    def forward(k):
        arrival(1, k).wait_recv()
        send(3, k).start()
        send(4, k).start()
        arrival(2, k).wait_recv()
        send(5, k).start()
        send(6, k).start()

    def finish(k):
        arrival(3, k).wait_recv()
        arrival(5, k).wait_recv()
        send(7, k).start()
        for i in (0, 4, 6, 7):
            arrival(i, k).wait_recv()

    own(0)
    own(1)

    for d in range(1, GROUP):
        r_copy(d, (g + GROUP - d) % GROUP, g).wait_recv()
    rt[...] = jnp.transpose(rall[...])

    base = (g * SLOTS).astype(F32)
    ybuf = pmat
    PB = 64
    GB = 64

    def build_p(i, carry):
        s, b = i // (SLOTS // PB), i % (SLOTS // PB)
        want = lax.broadcasted_iota(jnp.int32, (PB, ROWS), 0).astype(F32) + (base + (b * PB).astype(F32))
        pos = rall[pl.ds(pl.multiple_of(s * 16, 16), 8), :]
        hit = jnp.zeros((PB, ROWS), F32)
        for j in range(8):
            hit = jnp.where(pos[j : j + 1, :] == want, 1.0, hit)
        pmat[s, pl.ds(pl.multiple_of(b * PB, PB), PB), :] = hit.astype(BF16)
        return carry

    def build_g(i, carry):
        s, b = i % GROUP, i // GROUP
        t0 = pl.multiple_of(b * GB, GB)
        v = pltpu.roll(rt[pl.ds(t0, GB), :], (128 - s * 16) % 128, 1)
        want = lax.broadcasted_iota(jnp.int32, (GB, SLOTS), 1).astype(F32) + base
        sel = jnp.zeros((GB, SLOTS), F32)
        for j in range(8):
            sel = jnp.where(v[:, j : j + 1] == want, v[:, 8 + j : 9 + j], sel)
        g1 = (sel * (1.0 - 2.0**-8)).astype(BF16)
        rest = sel - g1.astype(F32)
        g2 = rest.astype(BF16)
        g3 = (rest - g2.astype(F32)).astype(BF16)
        for p, part in enumerate((g1, g2, g3)):
            gmat[s, pl.ds(pl.multiple_of(p * 256 + t0, GB), GB), :] = part
        return carry

    lax.fori_loop(0, GROUP * SLOTS // PB, build_p, 0)
    forward(0)
    own(2)
    gn = GROUP * ROWS // GB
    lax.fori_loop(0, gn // 4, build_g, 0)
    forward(1)
    own(3)
    finish(0)

    def gather_rows(k):
        def body(i, carry):
            for u in range(4):
                s = 4 * i + u
                xs = xall[pl.ds(pl.multiple_of((k * GROUP + s) * ROWS, ROWS), ROWS), :]
                gbuf[s] = jnp.dot(pmat[s], xs, preferred_element_type=F32).astype(BF16)
            return carry

        lax.fori_loop(0, GROUP // 4, body, 0)

    def block(i, n=1):
        return pl.ds(pl.multiple_of(i * 256, 256), n * 256)

    def down(c, t):
        i = c * steps + t
        slot = i % NBD
        d_load(i).wait()
        rows = pl.ds(pl.multiple_of(t * U * CAP, U * CAP), U * CAP)
        for u in range(U):
            v = jnp.dot(hbuf[t * U + u], dbuf[slot, u], preferred_element_type=F32).astype(BF16)
            ybuf.at[:, rows, :][:, u * CAP : (u + 1) * CAP, :] = v.reshape(GROUP, CAP, CC)

        @pl.when(i + NBD < NC * steps)
        def _():
            d_load(i + NBD).start()

    def experts(k, first=False, last=False):
        def body(t, carry):
            i = k * steps + t
            slot = i % NB
            for cp in w_load(i):
                cp.wait()
            lhs4 = gbuf.at[:, pl.ds(pl.multiple_of(t * U * CAP, U * CAP), U * CAP), :]
            big4 = big.at[block(t * U * 12, U * 12), :]
            for u in range(U):
                lhs = lhs4[:, u * CAP : (u + 1) * CAP, :].reshape(GROUP * CAP, KC)
                for n in range(FF // 256):
                    vals = []
                    for j in range(2):
                        v = jnp.dot(lhs, wbuf[slot, j, u, :, n * 256 : (n + 1) * 256], preferred_element_type=F32)
                        at = (u * 12 + j * 6 + n * 2) * 256
                        if not first:
                            v = v + jnp.concatenate([big4[at : at + 256, :], big4[at + 256 : at + 512, :]], axis=1)
                        if not last:
                            big4[at : at + 256, :] = v[:, :128]
                            big4[at + 256 : at + 512, :] = v[:, 128:]
                        vals.append(v)
                    if last:
                        hbuf[t * U + u, :, n * 256 : (n + 1) * 256] = (jax.nn.silu(vals[0]) * vals[1]).astype(BF16)

            @pl.when(i + NB < NK * steps)
            def _():
                for cp in w_load(i + NB):
                    cp.start()

            if last:
                down(0, t)

            return carry

        lax.fori_loop(0, steps, body, 0)

    gather_rows(0)
    experts(0, first=True)
    forward(2)
    own(4)
    finish(1)

    def middle(k, carry):
        gather_rows(k)
        experts(k)

        @pl.when(k + 2 < NK)
        def _():
            forward(k + 2)

        @pl.when(k + 4 < NK)
        def _():
            own(k + 4)

        lax.fori_loop(4 + k * 4, 8 + k * 4, build_g, 0)
        finish(k + 1)
        return carry

    lax.fori_loop(1, NK - 1, middle, 0)
    gather_rows(NK - 1)
    experts(NK - 1, last=True)

    for dev in (partner, xn, yn):
        pl.semaphore_signal(ready, inc=1, device_id=dev, device_id_type=MESH)

    def part(core, d, to):
        dx, dy = d % 2, d // 2
        s = ((y + dy) % 2) * 4 + ((x + dx) % 2) * 2 + core
        ys = ybuf[s]
        v = jnp.dot(gmat[s], ys, preferred_element_type=F32)
        v = v[0:256] + (v[256:512] + v[512:768])
        into = big.at[block(to, 8), :]
        a, b = (dx * 2 + dy) * 256, (4 + dy * 2 + dx) * 256
        into[a : a + 256, :] = v[:, :128]
        into[b : b + 256, :] = v[:, 128:]

    def d2d(c):
        return pltpu.make_async_remote_copy(
            src_ref=big.at[block(PBUF + (c % 2) * 8, 8), :],
            dst_ref=big.at[block(DRECV + c * 8, 8), :],
            send_sem=ds_sem.at[c], recv_sem=dr_sem.at[c],
            device_id=partner, device_id_type=MESH,
        )

    def ici(i, c):
        src, dst, n, dev = (
            (OWN + c * 8 + 2, RA1 + c * 2, 2, xn),
            (OWN + c * 8 + 6, RB1 + c * 2, 2, yn),
            (OWN + c * 8 + 1, RA2 + c, 1, yn),
            (OWN + c * 8 + 5, RB2 + c, 1, xn),
        )[i]
        return pltpu.make_async_remote_copy(
            src_ref=big.at[block(src, n), :], dst_ref=big.at[block(dst, n), :],
            send_sem=is_sem.at[i, c], recv_sem=ir_sem.at[i, c],
            device_id=dev, device_id_type=MESH,
        )

    def second_hop(c):
        ici(0, c).wait_recv()
        big[block(OWN + c * 8 + 1), :] = big[block(OWN + c * 8 + 1), :] + big[block(RA1 + c * 2 + 1), :]
        ici(2, c).start()
        ici(1, c).wait_recv()
        big[block(OWN + c * 8 + 5), :] = big[block(OWN + c * 8 + 5), :] + big[block(RB1 + c * 2 + 1), :]
        ici(3, c).start()

    def column_chunk(c, carry):
        @pl.when(c > 0)
        def _():
            def one(t, inner):
                down(c, t)
                return inner

            lax.fori_loop(0, steps, one, 0)

        @pl.when(c >= 2)
        def _():
            d2d(c - 2).wait_send()

        for d in range(4):
            part(1 - q, d, PBUF + (c % 2) * 8)

        @pl.when(c == 0)
        def _():
            pl.semaphore_wait(ready, 3)

        d2d(c).start()

        for d in range(4):
            part(q, d, OWN + c * 8)

        @pl.when(c >= LAG)
        def _():
            second_hop(c - LAG)

        d2d(c).wait_recv()

        def add(b, inner):
            big[block(OWN + c * 8 + b), :] = big[block(OWN + c * 8 + b), :] + big[block(DRECV + c * 8 + b), :]
            return inner

        lax.fori_loop(0, 8, add, 0)
        ici(0, c).start()
        ici(1, c).start()
        return carry

    lax.fori_loop(0, NC, column_chunk, 0)

    def tail(c, carry):
        second_hop(c)
        return carry

    lax.fori_loop(NC - LAG, NC, tail, 0)

    def final(c, carry):
        ici(2, c).wait_recv()
        a = big[block(OWN + c * 8), :] + big[block(RA1 + c * 2), :] + big[block(RA2 + c), :]
        ici(3, c).wait_recv()
        b = big[block(OWN + c * 8 + 4), :] + big[block(RB1 + c * 2), :] + big[block(RB2 + c), :]
        out_ref[:, pl.ds(pl.multiple_of(c * CC, CC), 128)] = a.astype(BF16)
        out_ref[:, pl.ds(pl.multiple_of(c * CC + 128, 128), 128)] = b.astype(BF16)
        for i in range(4):
            ici(i, c).wait_send()
        return carry

    lax.fori_loop(0, NC, final, 0)

    for c in (NC - 2, NC - 1):
        d2d(c).wait_send()
    for k in range(NK):
        for i in range(8):
            send(i, k).wait_send()
    for d in range(1, GROUP):
        r_copy(d, g, (g + d) % GROUP).wait_send()


def solution(mesh):
    group_axes = ("node", "expert")
    group_size = mesh.shape["node"] * mesh.shape["expert"]
    tok_spec = P(("data", "node", "expert"), None)
    weight_spec = P(("node", "expert"), None, None)

    def local_layer(tokens, expert_ids, gate_weights, slot_ids, w_gate, w_up, w_down):
        rows, width = tokens.shape
        top_k = expert_ids.shape[1]
        local_experts = w_gate.shape[0]
        slot_count = capacity(rows, top_k, local_experts * group_size)
        assert (rows, width, local_experts, slot_count, group_size) == (ROWS, WIDTH, LOCAL, CAP, GROUP)
        vmem = pl.BlockSpec(memory_space=pltpu.VMEM)
        hbm = pl.BlockSpec(memory_space=pl.ANY)
        dma = pltpu.SemaphoreType.DMA
        return pl.pallas_call(
            layer_kernel,
            out_shape=jax.ShapeDtypeStruct((rows, width), BF16),
            in_specs=[vmem, vmem, vmem, hbm, hbm, hbm, hbm],
            out_specs=vmem,
            scratch_shapes=[
                pltpu.VMEM((GROUP * 16, ROWS), F32),
                pltpu.VMEM((ROWS, GROUP * 16), F32),
                pltpu.VMEM((NK * GROUP * ROWS, KC), BF16),
                pltpu.VMEM((GROUP, SLOTS, ROWS), BF16),
                pltpu.VMEM((GROUP, 3 * ROWS, SLOTS), BF16),
                pltpu.VMEM((GROUP, SLOTS, KC), BF16),
                pltpu.VMEM((NBLK * 256, 128), F32),
                pltpu.VMEM((NB, 2, U, KC, FF), BF16),
                pltpu.VMEM((LOCAL, GROUP * CAP, FF), BF16),
                pltpu.VMEM((NBD, U, FF, CC), BF16),
                dma((NK,)),
                dma((GROUP - 1,)),
                dma((GROUP - 1,)),
                dma((8, NK)),
                dma((8, NK)),
                dma((NB, 2)),
                dma((NBD,)),
                dma((NC,)),
                dma((NC,)),
                dma((4, NC)),
                dma((4, NC)),
                pltpu.SemaphoreType.REGULAR,
            ],
            compiler_params=pltpu.CompilerParams(
                collective_id=0, has_side_effects=True, vmem_limit_bytes=67043328,
            ),
            cost_estimate=pl.CostEstimate(
                flops=6 * LOCAL * GROUP * CAP * WIDTH * FF,
                bytes_accessed=6 * LOCAL * WIDTH * FF,
                transcendentals=LOCAL * GROUP * CAP * FF,
            ),
            name="moe_layer",
        )(expert_ids.T, slot_ids.T, gate_weights.T, tokens, w_gate, w_up, w_down)

    return jax.shard_map(local_layer, mesh=mesh, in_specs=(tok_spec, tok_spec, tok_spec, tok_spec, weight_spec, weight_spec, weight_spec), out_specs=tok_spec, check_vma=False)
```

```python
import jax
import jax.numpy as jnp
from jax import lax
from jax.experimental import pallas as pl
from jax.experimental.pallas import tpu as pltpu
from jax.sharding import PartitionSpec as P

CAP_FACTOR = 2
MESH = pl.DeviceIdType.MESH
F32 = jnp.float32
BF16 = jnp.bfloat16

ROWS = 256
WIDTH = 2048
FF = 768
LOCAL = 16
CAP = 32
GROUP = 8
SLOTS = LOCAL * CAP
KC = 256
NK = WIDTH // KC
U = 4
NB = 3
CC = 256
NC = WIDTH // CC
NBD = 2
LAG = 2

OWN = 0
PBUF = 64
DRECV = 80
RA1 = 144
RB1 = 160
RA2 = 176
RB2 = 184
NBLK = 192


def capacity(rows, top_k, experts):
    return ((CAP_FACTOR * rows * top_k + 8 * experts - 1) // (8 * experts)) * 8


def layer_kernel(
    id_ref, slot_ref, gate_ref, tok_ref, wg_ref, wu_ref, wd_ref, out_ref,
    rall, rt, xall, pmat, gmat, gbuf, big, wbuf, hbuf, dbuf,
    lsem, rs_sem, rr_sem, xs_sem, xr_sem, w_sem, d_sem,
    ds_sem, dr_sem, is_sem, ir_sem, ready,
):
    data = lax.axis_index("data")
    y = lax.axis_index("node")
    ex = lax.axis_index("expert")
    x = ex // 2
    q = ex % 2
    g = y * 4 + ex
    flip = 1 - 2 * q
    gx = y * 4 + (1 - x) * 2 + q
    gy = (1 - y) * 4 + x * 2 + q
    gd = (1 - y) * 4 + (1 - x) * 2 + q
    gp = g + flip
    partner = (data, y, ex + flip)
    xn = (data, y, (1 - x) * 2 + q)
    yn = (data, 1 - y, ex)

    barrier = pltpu.get_barrier_semaphore()
    for d in range(1, GROUP):
        t = (g + d) % GROUP
        pl.semaphore_signal(barrier, inc=1, device_id=(data, t // 4, t % 4), device_id_type=MESH)

    def own_load(k):
        return pltpu.make_async_copy(
            tok_ref.at[:, pl.ds(pl.multiple_of(k * KC, KC), KC)],
            xall.at[pl.ds(pl.multiple_of((k * GROUP + g) * ROWS, ROWS), ROWS), :],
            lsem.at[k],
        )

    for k in range(NK):
        own_load(k).start()

    steps = LOCAL // U

    def w_load(i):
        k, e, slot = i // steps, (i % steps) * U, i % NB
        rows = pl.ds(pl.multiple_of(k * KC, KC), KC)
        return [
            pltpu.make_async_copy(ref.at[pl.ds(e, U), rows, :], wbuf.at[slot, j], w_sem.at[slot, j])
            for j, ref in enumerate((wg_ref, wu_ref))
        ]

    def d_load(i):
        c, e, slot = i // steps, (i % steps) * U, i % NBD
        cols = pl.ds(pl.multiple_of(c * CC, CC), CC)
        return pltpu.make_async_copy(wd_ref.at[pl.ds(e, U), :, cols], dbuf.at[slot], d_sem.at[slot])

    for i in range(NB):
        for cp in w_load(i):
            cp.start()
    for i in range(NBD):
        d_load(i).start()

    mine = pl.multiple_of(g * 16, 16)
    flat_pos = jnp.where(slot_ref[...] >= 0, id_ref[...] * CAP + slot_ref[...], -1)
    rall[pl.ds(mine, 8), :] = flat_pos.astype(F32)
    rall[pl.ds(mine + 8, 8), :] = gate_ref[...]
    pl.semaphore_wait(barrier, GROUP - 1)

    def r_copy(d, owner, dst):
        ref = rall.at[pl.ds(pl.multiple_of(owner * 16, 16), 16), :]
        return pltpu.make_async_remote_copy(
            src_ref=ref,
            dst_ref=ref,
            send_sem=rs_sem.at[d - 1],
            recv_sem=rr_sem.at[d - 1],
            device_id=(data, dst // 4, dst % 4),
            device_id_type=MESH,
        )

    for d in range(1, GROUP):
        r_copy(d, g, (g + d) % GROUP).start()

    def x_copy(i, k, s, dev, lo=0, n=ROWS):
        ref = xall.at[pl.ds(pl.multiple_of((k * GROUP + s) * ROWS + lo, 128), n), :]
        return pltpu.make_async_remote_copy(
            src_ref=ref, dst_ref=ref, send_sem=xs_sem.at[i, k], recv_sem=xr_sem.at[i, k],
            device_id=dev, device_id_type=MESH,
        )

    HALF = ROWS // 2

    def send(i, k):
        return x_copy(i, k, *(
            (g, partner),
            (g, xn),
            (g, yn),
            (gx, yn, 0, HALF),
            (gx, partner),
            (gy, xn, HALF, HALF),
            (gy, partner),
            (gd, partner),
        )[i])

    def arrival(i, k):
        return x_copy(i, k, *(
            (gp, partner),
            (gx, xn),
            (gy, yn),
            (gd, yn, 0, HALF),
            (gx + flip, partner),
            (gd, xn, HALF, HALF),
            (gy + flip, partner),
            (gd + flip, partner),
        )[i])

    def own(k):
        own_load(k).wait()
        for i in (1, 2, 0):
            send(i, k).start()

    def forward(k):
        arrival(1, k).wait_recv()
        send(3, k).start()
        send(4, k).start()
        arrival(2, k).wait_recv()
        send(5, k).start()
        send(6, k).start()

    def finish(k):
        arrival(3, k).wait_recv()
        arrival(5, k).wait_recv()
        send(7, k).start()
        for i in (0, 4, 6, 7):
            arrival(i, k).wait_recv()

    own(0)
    own(1)

    for d in range(1, GROUP):
        r_copy(d, (g + GROUP - d) % GROUP, g).wait_recv()
    rt[...] = jnp.transpose(rall[...])

    base = (g * SLOTS).astype(F32)
    ybuf = pmat
    PB = 64
    GB = 64

    def build_p(i, carry):
        s, b = i // (SLOTS // PB), i % (SLOTS // PB)
        want = lax.broadcasted_iota(jnp.int32, (PB, ROWS), 0).astype(F32) + (base + (b * PB).astype(F32))
        pos = rall[pl.ds(pl.multiple_of(s * 16, 16), 8), :]
        hit = jnp.zeros((PB, ROWS), F32)
        for j in range(8):
            hit = jnp.where(pos[j : j + 1, :] == want, 1.0, hit)
        pmat[s, pl.ds(pl.multiple_of(b * PB, PB), PB), :] = hit.astype(BF16)
        return carry

    def build_g(i, carry):
        s, b = i % GROUP, i // GROUP
        t0 = pl.multiple_of(b * GB, GB)
        v = pltpu.roll(rt[pl.ds(t0, GB), :], (128 - s * 16) % 128, 1)
        want = lax.broadcasted_iota(jnp.int32, (GB, SLOTS), 1).astype(F32) + base
        sel = jnp.zeros((GB, SLOTS), F32)
        for j in range(8):
            sel = jnp.where(v[:, j : j + 1] == want, v[:, 8 + j : 9 + j], sel)
        g1 = (sel * (1.0 - 2.0**-8)).astype(BF16)
        rest = sel - g1.astype(F32)
        g2 = rest.astype(BF16)
        g3 = (rest - g2.astype(F32)).astype(BF16)
        for p, part in enumerate((g1, g2, g3)):
            gmat[s, pl.ds(pl.multiple_of(p * 256 + t0, GB), GB), :] = part
        return carry

    lax.fori_loop(0, GROUP * SLOTS // PB, build_p, 0)
    forward(0)
    own(2)
    gn = GROUP * ROWS // GB
    lax.fori_loop(0, gn // 4, build_g, 0)
    forward(1)
    own(3)
    finish(0)

    def gather_rows(k):
        for s in range(GROUP):
            xs = xall[pl.ds(pl.multiple_of((k * GROUP + s) * ROWS, ROWS), ROWS), :]
            gbuf[s] = jnp.dot(pmat[s], xs, preferred_element_type=F32).astype(BF16)

    def block(i, n=1):
        return pl.ds(pl.multiple_of(i * 256, 256), n * 256)

    def down(c, t):
        i = c * steps + t
        slot = i % NBD
        d_load(i).wait()
        rows = pl.ds(pl.multiple_of(t * U * CAP, U * CAP), U * CAP)
        for u in range(U):
            v = jnp.dot(hbuf[t * U + u], dbuf[slot, u], preferred_element_type=F32).astype(BF16)
            ybuf.at[:, rows, :][:, u * CAP : (u + 1) * CAP, :] = v.reshape(GROUP, CAP, CC)

        @pl.when(i + NBD < NC * steps)
        def _():
            d_load(i + NBD).start()

    def experts(k, first=False, last=False):
        def body(t, carry):
            i = k * steps + t
            slot = i % NB
            for cp in w_load(i):
                cp.wait()
            lhs4 = gbuf.at[:, pl.ds(pl.multiple_of(t * U * CAP, U * CAP), U * CAP), :]
            big4 = big.at[block(t * U * 12, U * 12), :]
            for u in range(U):
                lhs = lhs4[:, u * CAP : (u + 1) * CAP, :].reshape(GROUP * CAP, KC)
                for n in range(FF // 256):
                    vals = []
                    for j in range(2):
                        v = jnp.dot(lhs, wbuf[slot, j, u, :, n * 256 : (n + 1) * 256], preferred_element_type=F32)
                        at = (u * 12 + j * 6 + n * 2) * 256
                        if not first:
                            v = v + jnp.concatenate([big4[at : at + 256, :], big4[at + 256 : at + 512, :]], axis=1)
                        if not last:
                            big4[at : at + 256, :] = v[:, :128]
                            big4[at + 256 : at + 512, :] = v[:, 128:]
                        vals.append(v)
                    if last:
                        hbuf[t * U + u, :, n * 256 : (n + 1) * 256] = (jax.nn.silu(vals[0]) * vals[1]).astype(BF16)

            @pl.when(i + NB < NK * steps)
            def _():
                for cp in w_load(i + NB):
                    cp.start()

            if last:
                down(0, t)
            elif not first:
                build_g(4 + k * 4 + t, 0)

            return carry

        lax.fori_loop(0, steps, body, 0)

    gather_rows(0)
    experts(0, first=True)
    forward(2)
    own(4)
    finish(1)

    def middle(k, carry):
        gather_rows(k)
        experts(k)

        @pl.when(k + 2 < NK)
        def _():
            forward(k + 2)

        @pl.when(k + 4 < NK)
        def _():
            own(k + 4)

        finish(k + 1)
        return carry

    lax.fori_loop(1, NK - 1, middle, 0)
    gather_rows(NK - 1)
    experts(NK - 1, last=True)

    for dev in (partner, xn, yn):
        pl.semaphore_signal(ready, inc=1, device_id=dev, device_id_type=MESH)

    def part(core, d, to):
        dx, dy = d % 2, d // 2
        s = ((y + dy) % 2) * 4 + ((x + dx) % 2) * 2 + core
        ys = ybuf[s]
        v = jnp.dot(gmat[s], ys, preferred_element_type=F32)
        v = v[0:256] + (v[256:512] + v[512:768])
        into = big.at[block(to, 8), :]
        a, b = (dx * 2 + dy) * 256, (4 + dy * 2 + dx) * 256
        into[a : a + 256, :] = v[:, :128]
        into[b : b + 256, :] = v[:, 128:]

    def d2d(c):
        return pltpu.make_async_remote_copy(
            src_ref=big.at[block(PBUF + (c % 2) * 8, 8), :],
            dst_ref=big.at[block(DRECV + c * 8, 8), :],
            send_sem=ds_sem.at[c], recv_sem=dr_sem.at[c],
            device_id=partner, device_id_type=MESH,
        )

    def ici(i, c):
        src, dst, n, dev = (
            (OWN + c * 8 + 2, RA1 + c * 2, 2, xn),
            (OWN + c * 8 + 6, RB1 + c * 2, 2, yn),
            (OWN + c * 8 + 1, RA2 + c, 1, yn),
            (OWN + c * 8 + 5, RB2 + c, 1, xn),
        )[i]
        return pltpu.make_async_remote_copy(
            src_ref=big.at[block(src, n), :], dst_ref=big.at[block(dst, n), :],
            send_sem=is_sem.at[i, c], recv_sem=ir_sem.at[i, c],
            device_id=dev, device_id_type=MESH,
        )

    def second_hop(c):
        ici(0, c).wait_recv()
        big[block(OWN + c * 8 + 1), :] = big[block(OWN + c * 8 + 1), :] + big[block(RA1 + c * 2 + 1), :]
        ici(2, c).start()
        ici(1, c).wait_recv()
        big[block(OWN + c * 8 + 5), :] = big[block(OWN + c * 8 + 5), :] + big[block(RB1 + c * 2 + 1), :]
        ici(3, c).start()

    def column_chunk(c, carry):
        @pl.when(c > 0)
        def _():
            def one(t, inner):
                down(c, t)
                return inner

            lax.fori_loop(0, steps, one, 0)

        @pl.when(c >= 2)
        def _():
            d2d(c - 2).wait_send()

        for d in range(4):
            part(1 - q, d, PBUF + (c % 2) * 8)

        @pl.when(c == 0)
        def _():
            pl.semaphore_wait(ready, 3)

        d2d(c).start()

        for d in range(4):
            part(q, d, OWN + c * 8)

        @pl.when(c >= LAG)
        def _():
            second_hop(c - LAG)

        d2d(c).wait_recv()

        def add(b, inner):
            big[block(OWN + c * 8 + b), :] = big[block(OWN + c * 8 + b), :] + big[block(DRECV + c * 8 + b), :]
            return inner

        lax.fori_loop(0, 8, add, 0)
        ici(0, c).start()
        ici(1, c).start()
        return carry

    lax.fori_loop(0, NC, column_chunk, 0)

    def tail(c, carry):
        second_hop(c)
        return carry

    lax.fori_loop(NC - LAG, NC, tail, 0)

    def final(c, carry):
        ici(2, c).wait_recv()
        a = big[block(OWN + c * 8), :] + big[block(RA1 + c * 2), :] + big[block(RA2 + c), :]
        ici(3, c).wait_recv()
        b = big[block(OWN + c * 8 + 4), :] + big[block(RB1 + c * 2), :] + big[block(RB2 + c), :]
        out_ref[:, pl.ds(pl.multiple_of(c * CC, CC), 128)] = a.astype(BF16)
        out_ref[:, pl.ds(pl.multiple_of(c * CC + 128, 128), 128)] = b.astype(BF16)
        for i in range(4):
            ici(i, c).wait_send()
        return carry

    lax.fori_loop(0, NC, final, 0)

    for c in (NC - 2, NC - 1):
        d2d(c).wait_send()
    for k in range(NK):
        for i in range(8):
            send(i, k).wait_send()
    for d in range(1, GROUP):
        r_copy(d, g, (g + d) % GROUP).wait_send()


def solution(mesh):
    group_axes = ("node", "expert")
    group_size = mesh.shape["node"] * mesh.shape["expert"]
    tok_spec = P(("data", "node", "expert"), None)
    weight_spec = P(("node", "expert"), None, None)

    def local_layer(tokens, expert_ids, gate_weights, slot_ids, w_gate, w_up, w_down):
        rows, width = tokens.shape
        top_k = expert_ids.shape[1]
        local_experts = w_gate.shape[0]
        slot_count = capacity(rows, top_k, local_experts * group_size)
        assert (rows, width, local_experts, slot_count, group_size) == (ROWS, WIDTH, LOCAL, CAP, GROUP)
        vmem = pl.BlockSpec(memory_space=pltpu.VMEM)
        hbm = pl.BlockSpec(memory_space=pl.ANY)
        dma = pltpu.SemaphoreType.DMA
        return pl.pallas_call(
            layer_kernel,
            out_shape=jax.ShapeDtypeStruct((rows, width), BF16),
            in_specs=[vmem, vmem, vmem, hbm, hbm, hbm, hbm],
            out_specs=vmem,
            scratch_shapes=[
                pltpu.VMEM((GROUP * 16, ROWS), F32),
                pltpu.VMEM((ROWS, GROUP * 16), F32),
                pltpu.VMEM((NK * GROUP * ROWS, KC), BF16),
                pltpu.VMEM((GROUP, SLOTS, ROWS), BF16),
                pltpu.VMEM((GROUP, 3 * ROWS, SLOTS), BF16),
                pltpu.VMEM((GROUP, SLOTS, KC), BF16),
                pltpu.VMEM((NBLK * 256, 128), F32),
                pltpu.VMEM((NB, 2, U, KC, FF), BF16),
                pltpu.VMEM((LOCAL, GROUP * CAP, FF), BF16),
                pltpu.VMEM((NBD, U, FF, CC), BF16),
                dma((NK,)),
                dma((GROUP - 1,)),
                dma((GROUP - 1,)),
                dma((8, NK)),
                dma((8, NK)),
                dma((NB, 2)),
                dma((NBD,)),
                dma((NC,)),
                dma((NC,)),
                dma((4, NC)),
                dma((4, NC)),
                pltpu.SemaphoreType.REGULAR,
            ],
            compiler_params=pltpu.CompilerParams(
                collective_id=0, has_side_effects=True, vmem_limit_bytes=67043328,
            ),
            cost_estimate=pl.CostEstimate(
                flops=6 * LOCAL * GROUP * CAP * WIDTH * FF,
                bytes_accessed=6 * LOCAL * WIDTH * FF,
                transcendentals=LOCAL * GROUP * CAP * FF,
            ),
            name="moe_layer",
        )(expert_ids.T, slot_ids.T, gate_weights.T, tokens, w_gate, w_up, w_down)

    return jax.shard_map(local_layer, mesh=mesh, in_specs=(tok_spec, tok_spec, tok_spec, tok_spec, weight_spec, weight_spec, weight_spec), out_specs=tok_spec, check_vma=False)
```

```python
import jax
import jax.numpy as jnp
from jax import lax
from jax.experimental import pallas as pl
from jax.experimental.pallas import tpu as pltpu
from jax.sharding import PartitionSpec as P

CAP_FACTOR = 2
MESH = pl.DeviceIdType.MESH
F32 = jnp.float32
BF16 = jnp.bfloat16

ROWS = 256
WIDTH = 2048
FF = 768
LOCAL = 16
CAP = 32
GROUP = 8
SLOTS = LOCAL * CAP
KC = 256
NK = WIDTH // KC
U = 4
NB = 3
CC = 256
NC = WIDTH // CC
NBD = 2
LAG = 2

OWN = 0
PBUF = 64
DRECV = 80
RA1 = 144
RB1 = 160
RA2 = 176
RB2 = 184
NBLK = 192


def capacity(rows, top_k, experts):
    return ((CAP_FACTOR * rows * top_k + 8 * experts - 1) // (8 * experts)) * 8


def layer_kernel(
    id_ref, slot_ref, gate_ref, tok_ref, wg_ref, wu_ref, wd_ref, out_ref,
    rall, rt, xall, pmat, gmat, gbuf, big, wbuf, hbuf, dbuf,
    lsem, rs_sem, rr_sem, xs_sem, xr_sem, w_sem, d_sem,
    ds_sem, dr_sem, is_sem, ir_sem, ready,
):
    data = lax.axis_index("data")
    y = lax.axis_index("node")
    ex = lax.axis_index("expert")
    x = ex // 2
    q = ex % 2
    g = y * 4 + ex
    flip = 1 - 2 * q
    gx = y * 4 + (1 - x) * 2 + q
    gy = (1 - y) * 4 + x * 2 + q
    gd = (1 - y) * 4 + (1 - x) * 2 + q
    gp = g + flip
    partner = (data, y, ex + flip)
    xn = (data, y, (1 - x) * 2 + q)
    yn = (data, 1 - y, ex)

    barrier = pltpu.get_barrier_semaphore()
    for d in range(1, GROUP):
        t = (g + d) % GROUP
        pl.semaphore_signal(barrier, inc=1, device_id=(data, t // 4, t % 4), device_id_type=MESH)

    def own_load(k):
        return pltpu.make_async_copy(
            tok_ref.at[:, pl.ds(pl.multiple_of(k * KC, KC), KC)],
            xall.at[pl.ds(pl.multiple_of((k * GROUP + g) * ROWS, ROWS), ROWS), :],
            lsem.at[k],
        )

    for k in range(NK):
        own_load(k).start()

    steps = LOCAL // U

    def w_load(i):
        k, e, slot = i // steps, (i % steps) * U, i % NB
        rows = pl.ds(pl.multiple_of(k * KC, KC), KC)
        return [
            pltpu.make_async_copy(ref.at[e + u, rows, :], wbuf.at[slot, j, u], w_sem.at[slot, j, u])
            for u in range(U)
            for j, ref in enumerate((wg_ref, wu_ref))
        ]

    def d_load(i):
        c, e, slot = i // steps, (i % steps) * U, i % NBD
        cols = pl.ds(pl.multiple_of(c * CC, CC), CC)
        return [
            pltpu.make_async_copy(wd_ref.at[e + u, :, cols], dbuf.at[slot, u], d_sem.at[slot, u])
            for u in range(U)
        ]

    for i in range(NB):
        for cp in w_load(i):
            cp.start()
    for i in range(NBD):
        for cp in d_load(i):
            cp.start()

    mine = pl.multiple_of(g * 16, 16)
    flat_pos = jnp.where(slot_ref[...] >= 0, id_ref[...] * CAP + slot_ref[...], -1)
    rall[pl.ds(mine, 8), :] = flat_pos.astype(F32)
    rall[pl.ds(mine + 8, 8), :] = gate_ref[...]
    pl.semaphore_wait(barrier, GROUP - 1)

    def r_copy(d, owner, dst):
        ref = rall.at[pl.ds(pl.multiple_of(owner * 16, 16), 16), :]
        return pltpu.make_async_remote_copy(
            src_ref=ref,
            dst_ref=ref,
            send_sem=rs_sem.at[d - 1],
            recv_sem=rr_sem.at[d - 1],
            device_id=(data, dst // 4, dst % 4),
            device_id_type=MESH,
        )

    for d in range(1, GROUP):
        r_copy(d, g, (g + d) % GROUP).start()

    def x_copy(i, k, s, dev, lo=0, n=ROWS):
        ref = xall.at[pl.ds(pl.multiple_of((k * GROUP + s) * ROWS + lo, 128), n), :]
        return pltpu.make_async_remote_copy(
            src_ref=ref, dst_ref=ref, send_sem=xs_sem.at[i, k], recv_sem=xr_sem.at[i, k],
            device_id=dev, device_id_type=MESH,
        )

    HALF = ROWS // 2

    def send(i, k):
        return x_copy(i, k, *(
            (g, partner),
            (g, xn),
            (g, yn),
            (gx, yn, 0, HALF),
            (gx, partner),
            (gy, xn, HALF, HALF),
            (gy, partner),
            (gd, partner),
        )[i])

    def arrival(i, k):
        return x_copy(i, k, *(
            (gp, partner),
            (gx, xn),
            (gy, yn),
            (gd, yn, 0, HALF),
            (gx + flip, partner),
            (gd, xn, HALF, HALF),
            (gy + flip, partner),
            (gd + flip, partner),
        )[i])

    def own(k):
        own_load(k).wait()
        for i in (1, 2, 0):
            send(i, k).start()

    def forward(k):
        arrival(1, k).wait_recv()
        send(3, k).start()
        send(4, k).start()
        arrival(2, k).wait_recv()
        send(5, k).start()
        send(6, k).start()

    def finish(k):
        arrival(3, k).wait_recv()
        arrival(5, k).wait_recv()
        send(7, k).start()
        for i in (0, 4, 6, 7):
            arrival(i, k).wait_recv()

    own(0)
    own(1)

    for d in range(1, GROUP):
        r_copy(d, (g + GROUP - d) % GROUP, g).wait_recv()
    rt[...] = jnp.transpose(rall[...])

    base = (g * SLOTS).astype(F32)
    ybuf = pmat
    PB = 64
    GB = 64

    def build_p(i, carry):
        s, b = i // (SLOTS // PB), i % (SLOTS // PB)
        want = lax.broadcasted_iota(jnp.int32, (PB, ROWS), 0).astype(F32) + (base + (b * PB).astype(F32))
        pos = rall[pl.ds(pl.multiple_of(s * 16, 16), 8), :]
        hit = jnp.zeros((PB, ROWS), F32)
        for j in range(8):
            hit = jnp.where(pos[j : j + 1, :] == want, 1.0, hit)
        pmat[s, pl.ds(pl.multiple_of(b * PB, PB), PB), :] = hit.astype(BF16)
        return carry

    def build_g(i, carry):
        s, b = i % GROUP, i // GROUP
        t0 = pl.multiple_of(b * GB, GB)
        v = pltpu.roll(rt[pl.ds(t0, GB), :], (128 - s * 16) % 128, 1)
        want = lax.broadcasted_iota(jnp.int32, (GB, SLOTS), 1).astype(F32) + base
        sel = jnp.zeros((GB, SLOTS), F32)
        for j in range(8):
            sel = jnp.where(v[:, j : j + 1] == want, v[:, 8 + j : 9 + j], sel)
        g1 = (sel * (1.0 - 2.0**-8)).astype(BF16)
        rest = sel - g1.astype(F32)
        g2 = rest.astype(BF16)
        g3 = (rest - g2.astype(F32)).astype(BF16)
        for p, part in enumerate((g1, g2, g3)):
            gmat[s, pl.ds(pl.multiple_of(p * 256 + t0, GB), GB), :] = part
        return carry

    lax.fori_loop(0, GROUP * SLOTS // PB, build_p, 0)
    forward(0)
    own(2)
    gn = GROUP * ROWS // GB
    lax.fori_loop(0, gn // 4, build_g, 0)
    forward(1)
    own(3)
    finish(0)

    def gather_rows(k):
        for s in range(GROUP):
            xs = xall[pl.ds(pl.multiple_of((k * GROUP + s) * ROWS, ROWS), ROWS), :]
            gbuf[s] = jnp.dot(pmat[s], xs, preferred_element_type=F32).astype(BF16)

    def block(i, n=1):
        return pl.ds(pl.multiple_of(i * 256, 256), n * 256)

    def down(c, t):
        i = c * steps + t
        slot = i % NBD
        for cp in d_load(i):
            cp.wait()
        rows = pl.ds(pl.multiple_of(t * U * CAP, U * CAP), U * CAP)
        for u in range(U):
            v = jnp.dot(hbuf[t * U + u], dbuf[slot, u], preferred_element_type=F32).astype(BF16)
            ybuf.at[:, rows, :][:, u * CAP : (u + 1) * CAP, :] = v.reshape(GROUP, CAP, CC)

        @pl.when(i + NBD < NC * steps)
        def _():
            for cp in d_load(i + NBD):
                cp.start()

    def experts(k, first=False, last=False):
        def body(t, carry):
            i = k * steps + t
            slot = i % NB
            for cp in w_load(i):
                cp.wait()
            lhs4 = gbuf.at[:, pl.ds(pl.multiple_of(t * U * CAP, U * CAP), U * CAP), :]
            big4 = big.at[block(t * U * 12, U * 12), :]
            for u in range(U):
                lhs = lhs4[:, u * CAP : (u + 1) * CAP, :].reshape(GROUP * CAP, KC)
                for n in range(FF // 256):
                    vals = []
                    for j in range(2):
                        v = jnp.dot(lhs, wbuf[slot, j, u, :, n * 256 : (n + 1) * 256], preferred_element_type=F32)
                        at = (u * 12 + j * 6 + n * 2) * 256
                        if not first:
                            v = v + jnp.concatenate([big4[at : at + 256, :], big4[at + 256 : at + 512, :]], axis=1)
                        if not last:
                            big4[at : at + 256, :] = v[:, :128]
                            big4[at + 256 : at + 512, :] = v[:, 128:]
                        vals.append(v)
                    if last:
                        hbuf[t * U + u, :, n * 256 : (n + 1) * 256] = (jax.nn.silu(vals[0]) * vals[1]).astype(BF16)

            @pl.when(i + NB < NK * steps)
            def _():
                for cp in w_load(i + NB):
                    cp.start()

            if last:
                down(0, t)
            elif not first:
                build_g(4 + k * 4 + t, 0)

            return carry

        lax.fori_loop(0, steps, body, 0)

    gather_rows(0)
    experts(0, first=True)
    forward(2)
    own(4)
    finish(1)

    def middle(k, carry):
        gather_rows(k)
        experts(k)

        @pl.when(k + 2 < NK)
        def _():
            forward(k + 2)

        @pl.when(k + 4 < NK)
        def _():
            own(k + 4)

        finish(k + 1)
        return carry

    lax.fori_loop(1, NK - 1, middle, 0)
    gather_rows(NK - 1)
    experts(NK - 1, last=True)

    for dev in (partner, xn, yn):
        pl.semaphore_signal(ready, inc=1, device_id=dev, device_id_type=MESH)

    def part(core, d, to):
        dx, dy = d % 2, d // 2
        s = ((y + dy) % 2) * 4 + ((x + dx) % 2) * 2 + core
        ys = ybuf[s]
        v = jnp.dot(gmat[s], ys, preferred_element_type=F32)
        v = v[0:256] + (v[256:512] + v[512:768])
        into = big.at[block(to, 8), :]
        a, b = (dx * 2 + dy) * 256, (4 + dy * 2 + dx) * 256
        into[a : a + 256, :] = v[:, :128]
        into[b : b + 256, :] = v[:, 128:]

    def d2d(c):
        return pltpu.make_async_remote_copy(
            src_ref=big.at[block(PBUF + (c % 2) * 8, 8), :],
            dst_ref=big.at[block(DRECV + c * 8, 8), :],
            send_sem=ds_sem.at[c], recv_sem=dr_sem.at[c],
            device_id=partner, device_id_type=MESH,
        )

    def ici(i, c):
        src, dst, n, dev = (
            (OWN + c * 8 + 2, RA1 + c * 2, 2, xn),
            (OWN + c * 8 + 6, RB1 + c * 2, 2, yn),
            (OWN + c * 8 + 1, RA2 + c, 1, yn),
            (OWN + c * 8 + 5, RB2 + c, 1, xn),
        )[i]
        return pltpu.make_async_remote_copy(
            src_ref=big.at[block(src, n), :], dst_ref=big.at[block(dst, n), :],
            send_sem=is_sem.at[i, c], recv_sem=ir_sem.at[i, c],
            device_id=dev, device_id_type=MESH,
        )

    def second_hop(c):
        ici(0, c).wait_recv()
        big[block(OWN + c * 8 + 1), :] = big[block(OWN + c * 8 + 1), :] + big[block(RA1 + c * 2 + 1), :]
        ici(2, c).start()
        ici(1, c).wait_recv()
        big[block(OWN + c * 8 + 5), :] = big[block(OWN + c * 8 + 5), :] + big[block(RB1 + c * 2 + 1), :]
        ici(3, c).start()

    def column_chunk(c, carry):
        @pl.when(c > 0)
        def _():
            def one(t, inner):
                down(c, t)
                return inner

            lax.fori_loop(0, steps, one, 0)

        @pl.when(c >= 2)
        def _():
            d2d(c - 2).wait_send()

        for d in range(4):
            part(1 - q, d, PBUF + (c % 2) * 8)

        @pl.when(c == 0)
        def _():
            pl.semaphore_wait(ready, 3)

        d2d(c).start()

        for d in range(4):
            part(q, d, OWN + c * 8)

        @pl.when(c >= LAG)
        def _():
            second_hop(c - LAG)

        d2d(c).wait_recv()

        def add(b, inner):
            big[block(OWN + c * 8 + b), :] = big[block(OWN + c * 8 + b), :] + big[block(DRECV + c * 8 + b), :]
            return inner

        lax.fori_loop(0, 8, add, 0)
        ici(0, c).start()
        ici(1, c).start()
        return carry

    lax.fori_loop(0, NC, column_chunk, 0)

    def tail(c, carry):
        second_hop(c)
        return carry

    lax.fori_loop(NC - LAG, NC, tail, 0)

    def final(c, carry):
        ici(2, c).wait_recv()
        a = big[block(OWN + c * 8), :] + big[block(RA1 + c * 2), :] + big[block(RA2 + c), :]
        ici(3, c).wait_recv()
        b = big[block(OWN + c * 8 + 4), :] + big[block(RB1 + c * 2), :] + big[block(RB2 + c), :]
        out_ref[:, pl.ds(pl.multiple_of(c * CC, CC), 128)] = a.astype(BF16)
        out_ref[:, pl.ds(pl.multiple_of(c * CC + 128, 128), 128)] = b.astype(BF16)
        for i in range(4):
            ici(i, c).wait_send()
        return carry

    lax.fori_loop(0, NC, final, 0)

    for c in (NC - 2, NC - 1):
        d2d(c).wait_send()
    for k in range(NK):
        for i in range(8):
            send(i, k).wait_send()
    for d in range(1, GROUP):
        r_copy(d, g, (g + d) % GROUP).wait_send()


def solution(mesh):
    group_axes = ("node", "expert")
    group_size = mesh.shape["node"] * mesh.shape["expert"]
    tok_spec = P(("data", "node", "expert"), None)
    weight_spec = P(("node", "expert"), None, None)

    def local_layer(tokens, expert_ids, gate_weights, slot_ids, w_gate, w_up, w_down):
        rows, width = tokens.shape
        top_k = expert_ids.shape[1]
        local_experts = w_gate.shape[0]
        slot_count = capacity(rows, top_k, local_experts * group_size)
        assert (rows, width, local_experts, slot_count, group_size) == (ROWS, WIDTH, LOCAL, CAP, GROUP)
        vmem = pl.BlockSpec(memory_space=pltpu.VMEM)
        hbm = pl.BlockSpec(memory_space=pl.ANY)
        dma = pltpu.SemaphoreType.DMA
        return pl.pallas_call(
            layer_kernel,
            out_shape=jax.ShapeDtypeStruct((rows, width), BF16),
            in_specs=[vmem, vmem, vmem, hbm, hbm, hbm, hbm],
            out_specs=vmem,
            scratch_shapes=[
                pltpu.VMEM((GROUP * 16, ROWS), F32),
                pltpu.VMEM((ROWS, GROUP * 16), F32),
                pltpu.VMEM((NK * GROUP * ROWS, KC), BF16),
                pltpu.VMEM((GROUP, SLOTS, ROWS), BF16),
                pltpu.VMEM((GROUP, 3 * ROWS, SLOTS), BF16),
                pltpu.VMEM((GROUP, SLOTS, KC), BF16),
                pltpu.VMEM((NBLK * 256, 128), F32),
                pltpu.VMEM((NB, 2, U, KC, FF), BF16),
                pltpu.VMEM((LOCAL, GROUP * CAP, FF), BF16),
                pltpu.VMEM((NBD, U, FF, CC), BF16),
                dma((NK,)),
                dma((GROUP - 1,)),
                dma((GROUP - 1,)),
                dma((8, NK)),
                dma((8, NK)),
                dma((NB, 2, U)),
                dma((NBD, U)),
                dma((NC,)),
                dma((NC,)),
                dma((4, NC)),
                dma((4, NC)),
                pltpu.SemaphoreType.REGULAR,
            ],
            compiler_params=pltpu.CompilerParams(
                collective_id=0, has_side_effects=True, vmem_limit_bytes=67043328,
            ),
            cost_estimate=pl.CostEstimate(
                flops=6 * LOCAL * GROUP * CAP * WIDTH * FF,
                bytes_accessed=6 * LOCAL * WIDTH * FF,
                transcendentals=LOCAL * GROUP * CAP * FF,
            ),
            name="moe_layer",
        )(expert_ids.T, slot_ids.T, gate_weights.T, tokens, w_gate, w_up, w_down)

    return jax.shard_map(local_layer, mesh=mesh, in_specs=(tok_spec, tok_spec, tok_spec, tok_spec, weight_spec, weight_spec, weight_spec), out_specs=tok_spec, check_vma=False)
```

```python
import jax
import jax.numpy as jnp
from jax import lax
from jax.experimental import pallas as pl
from jax.experimental.pallas import tpu as pltpu
from jax.sharding import PartitionSpec as P

CAP_FACTOR = 2
MESH = pl.DeviceIdType.MESH
F32 = jnp.float32
BF16 = jnp.bfloat16

ROWS = 256
WIDTH = 2048
FF = 768
LOCAL = 16
CAP = 32
GROUP = 8
SLOTS = LOCAL * CAP
KC = 256
NK = WIDTH // KC
U = 4
NB = 3
CC = 256
NC = WIDTH // CC
NBD = 2
LAG = 2

OWN = 0
PBUF = 64
DRECV = 80
RA1 = 144
RB1 = 160
RA2 = 176
RB2 = 184
NBLK = 192


def capacity(rows, top_k, experts):
    return ((CAP_FACTOR * rows * top_k + 8 * experts - 1) // (8 * experts)) * 8


def layer_kernel(
    id_ref, slot_ref, gate_ref, tok_ref, wg_ref, wu_ref, wd_ref, out_ref,
    rall, rt, xall, pmat, gmat, gbuf, big, wbuf, hbuf, dbuf,
    lsem, rs_sem, rr_sem, xs_sem, xr_sem, w_sem, d_sem,
    ds_sem, dr_sem, is_sem, ir_sem, ready,
):
    data = lax.axis_index("data")
    y = lax.axis_index("node")
    ex = lax.axis_index("expert")
    x = ex // 2
    q = ex % 2
    g = y * 4 + ex
    flip = 1 - 2 * q
    gx = y * 4 + (1 - x) * 2 + q
    gy = (1 - y) * 4 + x * 2 + q
    gd = (1 - y) * 4 + (1 - x) * 2 + q
    gp = g + flip
    partner = (data, y, ex + flip)
    xn = (data, y, (1 - x) * 2 + q)
    yn = (data, 1 - y, ex)

    barrier = pltpu.get_barrier_semaphore()
    for d in range(1, GROUP):
        t = (g + d) % GROUP
        pl.semaphore_signal(barrier, inc=1, device_id=(data, t // 4, t % 4), device_id_type=MESH)

    def own_load(k):
        return pltpu.make_async_copy(
            tok_ref.at[:, pl.ds(pl.multiple_of(k * KC, KC), KC)],
            xall.at[pl.ds(pl.multiple_of((k * GROUP + g) * ROWS, ROWS), ROWS), :],
            lsem.at[k],
        )

    for k in range(NK):
        own_load(k).start()

    steps = LOCAL // U

    def w_load(i):
        k, e, slot = i // steps, (i % steps) * U, i % NB
        rows = pl.ds(pl.multiple_of(k * KC, KC), KC)
        return [
            pltpu.make_async_copy(ref.at[pl.ds(e, U), rows, :], wbuf.at[slot, j], w_sem.at[slot, j])
            for j, ref in enumerate((wg_ref, wu_ref))
        ]

    def d_load(i):
        c, e, slot = i // steps, (i % steps) * U, i % NBD
        cols = pl.ds(pl.multiple_of(c * CC, CC), CC)
        return pltpu.make_async_copy(wd_ref.at[pl.ds(e, U), :, cols], dbuf.at[slot], d_sem.at[slot])

    for i in range(NB):
        for cp in w_load(i):
            cp.start()
    for i in range(NBD):
        d_load(i).start()

    mine = pl.multiple_of(g * 16, 16)
    flat_pos = jnp.where(slot_ref[...] >= 0, id_ref[...] * CAP + slot_ref[...], -1)
    rall[pl.ds(mine, 8), :] = flat_pos.astype(F32)
    rall[pl.ds(mine + 8, 8), :] = gate_ref[...]
    pl.semaphore_wait(barrier, GROUP - 1)

    def r_copy(d, owner, dst):
        ref = rall.at[pl.ds(pl.multiple_of(owner * 16, 16), 16), :]
        return pltpu.make_async_remote_copy(
            src_ref=ref,
            dst_ref=ref,
            send_sem=rs_sem.at[d - 1],
            recv_sem=rr_sem.at[d - 1],
            device_id=(data, dst // 4, dst % 4),
            device_id_type=MESH,
        )

    for d in range(1, GROUP):
        r_copy(d, g, (g + d) % GROUP).start()

    def x_copy(i, k, s, dev, lo=0, n=ROWS):
        ref = xall.at[pl.ds(pl.multiple_of((k * GROUP + s) * ROWS + lo, 128), n), :]
        return pltpu.make_async_remote_copy(
            src_ref=ref, dst_ref=ref, send_sem=xs_sem.at[i, k], recv_sem=xr_sem.at[i, k],
            device_id=dev, device_id_type=MESH,
        )

    HALF = ROWS // 2

    def send(i, k):
        return x_copy(i, k, *(
            (g, partner),
            (g, xn),
            (g, yn),
            (gx, yn, 0, HALF),
            (gx, partner),
            (gy, xn, HALF, HALF),
            (gy, partner),
            (gd, partner),
        )[i])

    def arrival(i, k):
        return x_copy(i, k, *(
            (gp, partner),
            (gx, xn),
            (gy, yn),
            (gd, yn, 0, HALF),
            (gx + flip, partner),
            (gd, xn, HALF, HALF),
            (gy + flip, partner),
            (gd + flip, partner),
        )[i])

    def own(k):
        own_load(k).wait()
        for i in (1, 2, 0):
            send(i, k).start()

    def forward(k):
        arrival(1, k).wait_recv()
        send(3, k).start()
        send(4, k).start()
        arrival(2, k).wait_recv()
        send(5, k).start()
        send(6, k).start()

    def diagonal(k):
        arrival(3, k).wait_recv()
        arrival(5, k).wait_recv()
        send(7, k).start()

    def finish(k):
        for i in (0, 4, 6, 7):
            arrival(i, k).wait_recv()

    own(0)
    own(1)

    for d in range(1, GROUP):
        r_copy(d, (g + GROUP - d) % GROUP, g).wait_recv()
    rt[...] = jnp.transpose(rall[...])

    base = (g * SLOTS).astype(F32)
    ybuf = pmat
    PB = 64
    GB = 64

    def build_p(i, carry):
        s, b = i // (SLOTS // PB), i % (SLOTS // PB)
        want = lax.broadcasted_iota(jnp.int32, (PB, ROWS), 0).astype(F32) + (base + (b * PB).astype(F32))
        pos = rall[pl.ds(pl.multiple_of(s * 16, 16), 8), :]
        hit = jnp.zeros((PB, ROWS), F32)
        for j in range(8):
            hit = jnp.where(pos[j : j + 1, :] == want, 1.0, hit)
        pmat[s, pl.ds(pl.multiple_of(b * PB, PB), PB), :] = hit.astype(BF16)
        return carry

    def build_g(i, carry):
        s, b = i % GROUP, i // GROUP
        t0 = pl.multiple_of(b * GB, GB)
        v = pltpu.roll(rt[pl.ds(t0, GB), :], (128 - s * 16) % 128, 1)
        want = lax.broadcasted_iota(jnp.int32, (GB, SLOTS), 1).astype(F32) + base
        sel = jnp.zeros((GB, SLOTS), F32)
        for j in range(8):
            sel = jnp.where(v[:, j : j + 1] == want, v[:, 8 + j : 9 + j], sel)
        g1 = (sel * (1.0 - 2.0**-8)).astype(BF16)
        rest = sel - g1.astype(F32)
        g2 = rest.astype(BF16)
        g3 = (rest - g2.astype(F32)).astype(BF16)
        for p, part in enumerate((g1, g2, g3)):
            gmat[s, pl.ds(pl.multiple_of(p * 256 + t0, GB), GB), :] = part
        return carry

    lax.fori_loop(0, GROUP * SLOTS // PB, build_p, 0)
    forward(0)
    own(2)
    gn = GROUP * ROWS // GB
    lax.fori_loop(0, gn // 4, build_g, 0)
    forward(1)
    own(3)
    diagonal(0)
    finish(0)

    def gather_rows(k):
        for s in range(GROUP):
            xs = xall[pl.ds(pl.multiple_of((k * GROUP + s) * ROWS, ROWS), ROWS), :]
            gbuf[s] = jnp.dot(pmat[s], xs, preferred_element_type=F32).astype(BF16)

    def block(i, n=1):
        return pl.ds(pl.multiple_of(i * 256, 256), n * 256)

    def down(c, t):
        i = c * steps + t
        slot = i % NBD
        d_load(i).wait()
        rows = pl.ds(pl.multiple_of(t * U * CAP, U * CAP), U * CAP)
        for u in range(U):
            v = jnp.dot(hbuf[t * U + u], dbuf[slot, u], preferred_element_type=F32).astype(BF16)
            ybuf.at[:, rows, :][:, u * CAP : (u + 1) * CAP, :] = v.reshape(GROUP, CAP, CC)

        @pl.when(i + NBD < NC * steps)
        def _():
            d_load(i + NBD).start()

    def experts(k, first=False, last=False):
        def body(t, carry):
            i = k * steps + t
            slot = i % NB
            for cp in w_load(i):
                cp.wait()
            lhs4 = gbuf.at[:, pl.ds(pl.multiple_of(t * U * CAP, U * CAP), U * CAP), :]
            big4 = big.at[block(t * U * 12, U * 12), :]
            for u in range(U):
                lhs = lhs4[:, u * CAP : (u + 1) * CAP, :].reshape(GROUP * CAP, KC)
                for n in range(FF // 256):
                    vals = []
                    for j in range(2):
                        v = jnp.dot(lhs, wbuf[slot, j, u, :, n * 256 : (n + 1) * 256], preferred_element_type=F32)
                        at = (u * 12 + j * 6 + n * 2) * 256
                        if not first:
                            v = v + jnp.concatenate([big4[at : at + 256, :], big4[at + 256 : at + 512, :]], axis=1)
                        if not last:
                            big4[at : at + 256, :] = v[:, :128]
                            big4[at + 256 : at + 512, :] = v[:, 128:]
                        vals.append(v)
                    if last:
                        hbuf[t * U + u, :, n * 256 : (n + 1) * 256] = (jax.nn.silu(vals[0]) * vals[1]).astype(BF16)

            @pl.when(i + NB < NK * steps)
            def _():
                for cp in w_load(i + NB):
                    cp.start()

            if last:
                down(0, t)
            else:
                if not first:
                    build_g(4 + k * 4 + t, 0)

                @pl.when(jnp.logical_and(t == 0, k + 2 < NK))
                def _():
                    forward(k + 2)

                @pl.when(jnp.logical_and(t == 0, k + 4 < NK))
                def _():
                    own(k + 4)

                @pl.when(t == 2)
                def _():
                    diagonal(k + 1)

            return carry

        lax.fori_loop(0, steps, body, 0)

    gather_rows(0)
    experts(0, first=True)
    finish(1)

    def middle(k, carry):
        gather_rows(k)
        experts(k)

        finish(k + 1)
        return carry

    lax.fori_loop(1, NK - 1, middle, 0)
    gather_rows(NK - 1)
    experts(NK - 1, last=True)

    for dev in (partner, xn, yn):
        pl.semaphore_signal(ready, inc=1, device_id=dev, device_id_type=MESH)

    def part(core, d, to):
        dx, dy = d % 2, d // 2
        s = ((y + dy) % 2) * 4 + ((x + dx) % 2) * 2 + core
        ys = ybuf[s]
        v = jnp.dot(gmat[s], ys, preferred_element_type=F32)
        v = v[0:256] + (v[256:512] + v[512:768])
        into = big.at[block(to, 8), :]
        a, b = (dx * 2 + dy) * 256, (4 + dy * 2 + dx) * 256
        into[a : a + 256, :] = v[:, :128]
        into[b : b + 256, :] = v[:, 128:]

    def d2d(c):
        return pltpu.make_async_remote_copy(
            src_ref=big.at[block(PBUF + (c % 2) * 8, 8), :],
            dst_ref=big.at[block(DRECV + c * 8, 8), :],
            send_sem=ds_sem.at[c], recv_sem=dr_sem.at[c],
            device_id=partner, device_id_type=MESH,
        )

    def ici(i, c):
        src, dst, n, dev = (
            (OWN + c * 8 + 2, RA1 + c * 2, 2, xn),
            (OWN + c * 8 + 6, RB1 + c * 2, 2, yn),
            (OWN + c * 8 + 1, RA2 + c, 1, yn),
            (OWN + c * 8 + 5, RB2 + c, 1, xn),
        )[i]
        return pltpu.make_async_remote_copy(
            src_ref=big.at[block(src, n), :], dst_ref=big.at[block(dst, n), :],
            send_sem=is_sem.at[i, c], recv_sem=ir_sem.at[i, c],
            device_id=dev, device_id_type=MESH,
        )

    def second_hop(c):
        ici(0, c).wait_recv()
        big[block(OWN + c * 8 + 1), :] = big[block(OWN + c * 8 + 1), :] + big[block(RA1 + c * 2 + 1), :]
        ici(2, c).start()
        ici(1, c).wait_recv()
        big[block(OWN + c * 8 + 5), :] = big[block(OWN + c * 8 + 5), :] + big[block(RB1 + c * 2 + 1), :]
        ici(3, c).start()

    def column_chunk(c, carry):
        @pl.when(c > 0)
        def _():
            def one(t, inner):
                down(c, t)
                return inner

            lax.fori_loop(0, steps, one, 0)

        @pl.when(c >= 2)
        def _():
            d2d(c - 2).wait_send()

        for d in range(4):
            part(1 - q, d, PBUF + (c % 2) * 8)

        @pl.when(c == 0)
        def _():
            pl.semaphore_wait(ready, 3)

        d2d(c).start()

        for d in range(4):
            part(q, d, OWN + c * 8)

        @pl.when(c >= LAG)
        def _():
            second_hop(c - LAG)

        d2d(c).wait_recv()

        def add(b, inner):
            big[block(OWN + c * 8 + b), :] = big[block(OWN + c * 8 + b), :] + big[block(DRECV + c * 8 + b), :]
            return inner

        lax.fori_loop(0, 8, add, 0)
        ici(0, c).start()
        ici(1, c).start()
        return carry

    lax.fori_loop(0, NC, column_chunk, 0)

    def tail(c, carry):
        second_hop(c)
        return carry

    lax.fori_loop(NC - LAG, NC, tail, 0)

    def final(c, carry):
        ici(2, c).wait_recv()
        a = big[block(OWN + c * 8), :] + big[block(RA1 + c * 2), :] + big[block(RA2 + c), :]
        ici(3, c).wait_recv()
        b = big[block(OWN + c * 8 + 4), :] + big[block(RB1 + c * 2), :] + big[block(RB2 + c), :]
        out_ref[:, pl.ds(pl.multiple_of(c * CC, CC), 128)] = a.astype(BF16)
        out_ref[:, pl.ds(pl.multiple_of(c * CC + 128, 128), 128)] = b.astype(BF16)
        for i in range(4):
            ici(i, c).wait_send()
        return carry

    lax.fori_loop(0, NC, final, 0)

    for c in (NC - 2, NC - 1):
        d2d(c).wait_send()
    for k in range(NK):
        for i in range(8):
            send(i, k).wait_send()
    for d in range(1, GROUP):
        r_copy(d, g, (g + d) % GROUP).wait_send()


def solution(mesh):
    group_axes = ("node", "expert")
    group_size = mesh.shape["node"] * mesh.shape["expert"]
    tok_spec = P(("data", "node", "expert"), None)
    weight_spec = P(("node", "expert"), None, None)

    def local_layer(tokens, expert_ids, gate_weights, slot_ids, w_gate, w_up, w_down):
        rows, width = tokens.shape
        top_k = expert_ids.shape[1]
        local_experts = w_gate.shape[0]
        slot_count = capacity(rows, top_k, local_experts * group_size)
        assert (rows, width, local_experts, slot_count, group_size) == (ROWS, WIDTH, LOCAL, CAP, GROUP)
        vmem = pl.BlockSpec(memory_space=pltpu.VMEM)
        hbm = pl.BlockSpec(memory_space=pl.ANY)
        dma = pltpu.SemaphoreType.DMA
        return pl.pallas_call(
            layer_kernel,
            out_shape=jax.ShapeDtypeStruct((rows, width), BF16),
            in_specs=[vmem, vmem, vmem, hbm, hbm, hbm, hbm],
            out_specs=vmem,
            scratch_shapes=[
                pltpu.VMEM((GROUP * 16, ROWS), F32),
                pltpu.VMEM((ROWS, GROUP * 16), F32),
                pltpu.VMEM((NK * GROUP * ROWS, KC), BF16),
                pltpu.VMEM((GROUP, SLOTS, ROWS), BF16),
                pltpu.VMEM((GROUP, 3 * ROWS, SLOTS), BF16),
                pltpu.VMEM((GROUP, SLOTS, KC), BF16),
                pltpu.VMEM((NBLK * 256, 128), F32),
                pltpu.VMEM((NB, 2, U, KC, FF), BF16),
                pltpu.VMEM((LOCAL, GROUP * CAP, FF), BF16),
                pltpu.VMEM((NBD, U, FF, CC), BF16),
                dma((NK,)),
                dma((GROUP - 1,)),
                dma((GROUP - 1,)),
                dma((8, NK)),
                dma((8, NK)),
                dma((NB, 2)),
                dma((NBD,)),
                dma((NC,)),
                dma((NC,)),
                dma((4, NC)),
                dma((4, NC)),
                pltpu.SemaphoreType.REGULAR,
            ],
            compiler_params=pltpu.CompilerParams(
                collective_id=0, has_side_effects=True, vmem_limit_bytes=67043328,
            ),
            cost_estimate=pl.CostEstimate(
                flops=6 * LOCAL * GROUP * CAP * WIDTH * FF,
                bytes_accessed=6 * LOCAL * WIDTH * FF,
                transcendentals=LOCAL * GROUP * CAP * FF,
            ),
            name="moe_layer",
        )(expert_ids.T, slot_ids.T, gate_weights.T, tokens, w_gate, w_up, w_down)

    return jax.shard_map(local_layer, mesh=mesh, in_specs=(tok_spec, tok_spec, tok_spec, tok_spec, weight_spec, weight_spec, weight_spec), out_specs=tok_spec, check_vma=False)
```

```python
import jax
import jax.numpy as jnp
from jax import lax
from jax.experimental import pallas as pl
from jax.experimental.pallas import tpu as pltpu
from jax.sharding import PartitionSpec as P

CAP_FACTOR = 2
MESH = pl.DeviceIdType.MESH
F32 = jnp.float32
BF16 = jnp.bfloat16

ROWS = 256
WIDTH = 2048
FF = 768
LOCAL = 16
CAP = 32
GROUP = 8
SLOTS = LOCAL * CAP
KC = 256
NK = WIDTH // KC
U = 4
NB = 3
NX = 2
CC = 256
NC = WIDTH // CC
NBD = 2
LAG = 2

OWN = 0
PBUF = 64
DRECV = 80
RA1 = 144
RB1 = 160
RA2 = 176
RB2 = 184
NBLK = 192


def capacity(rows, top_k, experts):
    return ((CAP_FACTOR * rows * top_k + 8 * experts - 1) // (8 * experts)) * 8


def layer_kernel(
    id_ref, slot_ref, gate_ref, tok_ref, wg_ref, wu_ref, wd_ref, out_ref,
    rall, rt, xall, pmat, gmat, gbuf, big, wbuf, dbuf, obuf,
    lsem, rs_sem, rr_sem, xs_sem, xr_sem, w_sem, d_sem,
    ds_sem, dr_sem, is_sem, ir_sem, o_sem, ready,
):
    data = lax.axis_index("data")
    y = lax.axis_index("node")
    ex = lax.axis_index("expert")
    x = ex // 2
    q = ex % 2
    g = y * 4 + ex
    flip = 1 - 2 * q
    gx = y * 4 + (1 - x) * 2 + q
    gy = (1 - y) * 4 + x * 2 + q
    gd = (1 - y) * 4 + (1 - x) * 2 + q
    gp = g + flip
    partner = (data, y, ex + flip)
    xn = (data, y, (1 - x) * 2 + q)
    yn = (data, 1 - y, ex)

    barrier = pltpu.get_barrier_semaphore()
    for d in range(1, GROUP):
        t = (g + d) % GROUP
        pl.semaphore_signal(barrier, inc=1, device_id=(data, t // 4, t % 4), device_id_type=MESH)

    def own_load(k):
        return pltpu.make_async_copy(
            tok_ref.at[:, pl.ds(pl.multiple_of(k * KC, KC), KC)],
            xall.at[pl.ds(pl.multiple_of((k * GROUP + g) * ROWS, ROWS), ROWS), :],
            lsem.at[k],
        )

    for k in range(NK):
        own_load(k).start()

    steps = LOCAL // U

    tail_step = (NK - 1) * steps
    hidden = 2 * U * NB

    def w_slot(i):
        return jnp.where(i < tail_step, i % (NB + NX), (i - tail_step) % NB) * (2 * U)

    def w_load(i):
        k, e, at = i // steps, (i % steps) * U, w_slot(i)
        rows = pl.ds(pl.multiple_of(k * KC, KC), KC)
        return [
            pltpu.make_async_copy(ref.at[pl.ds(e, U), rows, :], wbuf.at[pl.ds(at + j * U, U)], w_sem.at[at // (2 * U), j])
            for j, ref in enumerate((wg_ref, wu_ref))
        ]

    def d_load(i):
        c, e, slot = i // steps, (i % steps) * U, i % NBD
        cols = pl.ds(pl.multiple_of(c * CC, CC), CC)
        return pltpu.make_async_copy(wd_ref.at[pl.ds(e, U), :, cols], dbuf.at[slot], d_sem.at[slot])

    for i in range(NB + NX):
        for cp in w_load(i):
            cp.start()
    for i in range(NBD):
        d_load(i).start()

    mine = pl.multiple_of(g * 16, 16)
    flat_pos = jnp.where(slot_ref[...] >= 0, id_ref[...] * CAP + slot_ref[...], -1)
    rall[pl.ds(mine, 8), :] = flat_pos.astype(F32)
    rall[pl.ds(mine + 8, 8), :] = gate_ref[...]
    pl.semaphore_wait(barrier, GROUP - 1)

    def r_copy(d, owner, dst):
        ref = rall.at[pl.ds(pl.multiple_of(owner * 16, 16), 16), :]
        return pltpu.make_async_remote_copy(
            src_ref=ref,
            dst_ref=ref,
            send_sem=rs_sem.at[d - 1],
            recv_sem=rr_sem.at[d - 1],
            device_id=(data, dst // 4, dst % 4),
            device_id_type=MESH,
        )

    for d in range(1, GROUP):
        r_copy(d, g, (g + d) % GROUP).start()

    def x_copy(i, k, s, dev, lo=0, n=ROWS):
        ref = xall.at[pl.ds(pl.multiple_of((k * GROUP + s) * ROWS + lo, 128), n), :]
        return pltpu.make_async_remote_copy(
            src_ref=ref, dst_ref=ref, send_sem=xs_sem.at[i, k], recv_sem=xr_sem.at[i, k],
            device_id=dev, device_id_type=MESH,
        )

    HALF = ROWS // 2

    def send(i, k):
        return x_copy(i, k, *(
            (g, partner),
            (g, xn),
            (g, yn),
            (gx, yn, 0, HALF),
            (gx, partner),
            (gy, xn, HALF, HALF),
            (gy, partner),
            (gd, partner),
        )[i])

    def arrival(i, k):
        return x_copy(i, k, *(
            (gp, partner),
            (gx, xn),
            (gy, yn),
            (gd, yn, 0, HALF),
            (gx + flip, partner),
            (gd, xn, HALF, HALF),
            (gy + flip, partner),
            (gd + flip, partner),
        )[i])

    def own(k):
        own_load(k).wait()
        for i in (1, 2, 0):
            send(i, k).start()

    def forward(k):
        arrival(1, k).wait_recv()
        send(3, k).start()
        send(4, k).start()
        arrival(2, k).wait_recv()
        send(5, k).start()
        send(6, k).start()

    def diagonal(k):
        arrival(3, k).wait_recv()
        arrival(5, k).wait_recv()
        send(7, k).start()

    def finish(k):
        for i in (0, 4, 6, 7):
            arrival(i, k).wait_recv()

    own(0)
    own(1)

    for d in range(1, GROUP):
        r_copy(d, (g + GROUP - d) % GROUP, g).wait_recv()
    rt[...] = jnp.transpose(rall[...])

    base = (g * SLOTS).astype(F32)
    ybuf = pmat
    PB = 64
    GB = 64

    def build_p(i, carry):
        s, b = i // (SLOTS // PB), i % (SLOTS // PB)
        want = lax.broadcasted_iota(jnp.int32, (PB, ROWS), 0).astype(F32) + (base + (b * PB).astype(F32))
        pos = rall[pl.ds(pl.multiple_of(s * 16, 16), 8), :]
        hit = jnp.zeros((PB, ROWS), F32)
        for j in range(8):
            hit = jnp.where(pos[j : j + 1, :] == want, 1.0, hit)
        pmat[s, pl.ds(pl.multiple_of(b * PB, PB), PB), :] = hit.astype(BF16)
        return carry

    def build_g(i, carry):
        s, b = i % GROUP, i // GROUP
        t0 = pl.multiple_of(b * GB, GB)
        v = pltpu.roll(rt[pl.ds(t0, GB), :], (128 - s * 16) % 128, 1)
        want = lax.broadcasted_iota(jnp.int32, (GB, SLOTS), 1).astype(F32) + base
        sel = jnp.zeros((GB, SLOTS), F32)
        for j in range(8):
            sel = jnp.where(v[:, j : j + 1] == want, v[:, 8 + j : 9 + j], sel)
        g1 = (sel * (1.0 - 2.0**-8)).astype(BF16)
        rest = sel - g1.astype(F32)
        g2 = rest.astype(BF16)
        g3 = (rest - g2.astype(F32)).astype(BF16)
        for p, part in enumerate((g1, g2, g3)):
            gmat[s, pl.ds(pl.multiple_of(p * 256 + t0, GB), GB), :] = part
        return carry

    lax.fori_loop(0, GROUP * SLOTS // PB, build_p, 0)
    forward(0)
    own(2)
    gn = GROUP * ROWS // GB
    lax.fori_loop(0, gn // 4, build_g, 0)
    forward(1)
    own(3)
    diagonal(0)
    finish(0)

    def gather_rows(k):
        for s in range(GROUP):
            xs = xall[pl.ds(pl.multiple_of((k * GROUP + s) * ROWS, ROWS), ROWS), :]
            gbuf[s] = jnp.dot(pmat[s], xs, preferred_element_type=F32).astype(BF16)

    def block(i, n=1):
        return pl.ds(pl.multiple_of(i * 256, 256), n * 256)

    def down(c, t):
        i = c * steps + t
        slot = i % NBD
        d_load(i).wait()
        rows = pl.ds(pl.multiple_of(t * U * CAP, U * CAP), U * CAP)
        for u in range(U):
            v = jnp.dot(wbuf[hidden + t * U + u], dbuf[slot, u], preferred_element_type=F32).astype(BF16)
            ybuf.at[:, rows, :][:, u * CAP : (u + 1) * CAP, :] = v.reshape(GROUP, CAP, CC)

        @pl.when(i + NBD < NC * steps)
        def _():
            d_load(i + NBD).start()

    def experts(k, first=False, last=False):
        def body(t, carry):
            i = k * steps + t
            for cp in w_load(i):
                cp.wait()
            w4 = wbuf.at[pl.ds(w_slot(i), 2 * U)]
            lhs4 = gbuf.at[:, pl.ds(pl.multiple_of(t * U * CAP, U * CAP), U * CAP), :]
            big4 = big.at[block(t * U * 12, U * 12), :]
            for u in range(U):
                lhs = lhs4[:, u * CAP : (u + 1) * CAP, :].reshape(GROUP * CAP, KC)
                for n in range(FF // 256):
                    vals = []
                    for j in range(2):
                        v = jnp.dot(lhs, w4[j * U + u, :, n * 256 : (n + 1) * 256], preferred_element_type=F32)
                        at = (u * 12 + j * 6 + n * 2) * 256
                        if not first:
                            v = v + jnp.concatenate([big4[at : at + 256, :], big4[at + 256 : at + 512, :]], axis=1)
                        if not last:
                            big4[at : at + 256, :] = v[:, :128]
                            big4[at + 256 : at + 512, :] = v[:, 128:]
                        vals.append(v)
                    if last:
                        wbuf[hidden + t * U + u, :, n * 256 : (n + 1) * 256] = (jax.nn.silu(vals[0]) * vals[1]).astype(BF16)

            @pl.when(i + NB + NX < tail_step)
            def _():
                for cp in w_load(i + NB + NX):
                    cp.start()

            @pl.when(jnp.logical_and(i + NB >= tail_step, i + NB < NK * steps))
            def _():
                for cp in w_load(i + NB):
                    cp.start()

            if last:
                down(0, t)
            else:
                if not first:
                    build_g(4 + k * 4 + t, 0)

                @pl.when(jnp.logical_and(t == 0, k + 2 < NK))
                def _():
                    forward(k + 2)

                @pl.when(jnp.logical_and(t == 0, k + 4 < NK))
                def _():
                    own(k + 4)

                @pl.when(t == 2)
                def _():
                    diagonal(k + 1)

            return carry

        lax.fori_loop(0, steps, body, 0)

    gather_rows(0)
    experts(0, first=True)
    finish(1)

    def middle(k, carry):
        gather_rows(k)
        experts(k)

        finish(k + 1)
        return carry

    lax.fori_loop(1, NK - 1, middle, 0)
    gather_rows(NK - 1)
    experts(NK - 1, last=True)

    for dev in (partner, xn, yn):
        pl.semaphore_signal(ready, inc=1, device_id=dev, device_id_type=MESH)

    def part(core, d, to):
        dx, dy = d % 2, d // 2
        s = ((y + dy) % 2) * 4 + ((x + dx) % 2) * 2 + core
        ys = ybuf[s]
        v = jnp.dot(gmat[s], ys, preferred_element_type=F32)
        v = v[0:256] + (v[256:512] + v[512:768])
        into = big.at[block(to, 8), :]
        a, b = (dx * 2 + dy) * 256, (4 + dy * 2 + dx) * 256
        into[a : a + 256, :] = v[:, :128]
        into[b : b + 256, :] = v[:, 128:]

    def d2d(i, c):
        at = (2, 6, 0, 4)[i]
        return pltpu.make_async_remote_copy(
            src_ref=big.at[block(PBUF + (c % 2) * 8 + at, 2), :],
            dst_ref=big.at[block(DRECV + c * 8 + at, 2), :],
            send_sem=ds_sem.at[i, c], recv_sem=dr_sem.at[i, c],
            device_id=partner, device_id_type=MESH,
        )

    def pair_sum(i, c):
        at = (2, 6, 0, 4)[i]
        d2d(i, c).wait_recv()
        rows = block(OWN + c * 8 + at, 2)
        big[rows, :] = big[rows, :] + big[block(DRECV + c * 8 + at, 2), :]

    def ici(i, c):
        src, dst, n, dev = (
            (OWN + c * 8 + 2, RA1 + c * 2, 2, xn),
            (OWN + c * 8 + 6, RB1 + c * 2, 2, yn),
            (OWN + c * 8 + 1, RA2 + c, 1, yn),
            (OWN + c * 8 + 5, RB2 + c, 1, xn),
        )[i]
        return pltpu.make_async_remote_copy(
            src_ref=big.at[block(src, n), :], dst_ref=big.at[block(dst, n), :],
            send_sem=is_sem.at[i, c], recv_sem=ir_sem.at[i, c],
            device_id=dev, device_id_type=MESH,
        )

    def second_hop(c):
        ici(0, c).wait_recv()
        big[block(OWN + c * 8 + 1), :] = big[block(OWN + c * 8 + 1), :] + big[block(RA1 + c * 2 + 1), :]
        ici(2, c).start()
        ici(1, c).wait_recv()
        big[block(OWN + c * 8 + 5), :] = big[block(OWN + c * 8 + 5), :] + big[block(RB1 + c * 2 + 1), :]
        ici(3, c).start()

    def column_chunk(c, carry):
        @pl.when(c > 0)
        def _():
            def one(t, inner):
                down(c, t)
                return inner

            lax.fori_loop(0, steps, one, 0)

        @pl.when(c >= 2)
        def _():
            for i in range(4):
                d2d(i, c - 2).wait_send()

        for d in (3, 1, 2, 0):
            part(1 - q, d, PBUF + (c % 2) * 8)

        @pl.when(c == 0)
        def _():
            pl.semaphore_wait(ready, 3)

        for i in range(4):
            d2d(i, c).start()
        for d in (3, 1, 2, 0):
            part(q, d, OWN + c * 8)

        @pl.when(c >= LAG)
        def _():
            second_hop(c - LAG)

        pair_sum(0, c)
        ici(0, c).start()
        pair_sum(1, c)
        ici(1, c).start()
        pair_sum(2, c)
        pair_sum(3, c)
        return carry

    lax.fori_loop(0, NC, column_chunk, 0)

    def tail(c, carry):
        second_hop(c)
        return carry

    lax.fori_loop(NC - LAG, NC, tail, 0)

    def out_copy(c):
        cols = pl.ds(pl.multiple_of(c * CC, CC), CC)
        return pltpu.make_async_copy(obuf.at[c], out_ref.at[:, cols], o_sem.at[c])

    def final(c, carry):
        ici(2, c).wait_recv()
        a = big[block(OWN + c * 8), :] + big[block(RA1 + c * 2), :] + big[block(RA2 + c), :]
        ici(3, c).wait_recv()
        b = big[block(OWN + c * 8 + 4), :] + big[block(RB1 + c * 2), :] + big[block(RB2 + c), :]
        obuf[c, :, 0:128] = a.astype(BF16)
        obuf[c, :, 128:256] = b.astype(BF16)
        out_copy(c).start()
        for i in range(4):
            ici(i, c).wait_send()
        return carry

    lax.fori_loop(0, NC, final, 0)

    for c in range(NC):
        out_copy(c).wait()
    for c in (NC - 2, NC - 1):
        for i in range(4):
            d2d(i, c).wait_send()
    for k in range(NK):
        for i in range(8):
            send(i, k).wait_send()
    for d in range(1, GROUP):
        r_copy(d, g, (g + d) % GROUP).wait_send()


def solution(mesh):
    group_axes = ("node", "expert")
    group_size = mesh.shape["node"] * mesh.shape["expert"]
    tok_spec = P(("data", "node", "expert"), None)
    weight_spec = P(("node", "expert"), None, None)

    def local_layer(tokens, expert_ids, gate_weights, slot_ids, w_gate, w_up, w_down):
        rows, width = tokens.shape
        top_k = expert_ids.shape[1]
        local_experts = w_gate.shape[0]
        slot_count = capacity(rows, top_k, local_experts * group_size)
        assert (rows, width, local_experts, slot_count, group_size) == (ROWS, WIDTH, LOCAL, CAP, GROUP)
        vmem = pl.BlockSpec(memory_space=pltpu.VMEM)
        hbm = pl.BlockSpec(memory_space=pl.ANY)
        dma = pltpu.SemaphoreType.DMA
        return pl.pallas_call(
            layer_kernel,
            out_shape=jax.ShapeDtypeStruct((rows, width), BF16),
            in_specs=[vmem, vmem, vmem, hbm, hbm, hbm, hbm],
            out_specs=hbm,
            scratch_shapes=[
                pltpu.VMEM((GROUP * 16, ROWS), F32),
                pltpu.VMEM((ROWS, GROUP * 16), F32),
                pltpu.VMEM((NK * GROUP * ROWS, KC), BF16),
                pltpu.VMEM((GROUP, SLOTS, ROWS), BF16),
                pltpu.VMEM((GROUP, 3 * ROWS, SLOTS), BF16),
                pltpu.VMEM((GROUP, SLOTS, KC), BF16),
                pltpu.VMEM((NBLK * 256, 128), F32),
                pltpu.VMEM((2 * U * (NB + NX), KC, FF), BF16),
                pltpu.VMEM((NBD, U, FF, CC), BF16),
                pltpu.VMEM((NC, ROWS, CC), BF16),
                dma((NK,)),
                dma((GROUP - 1,)),
                dma((GROUP - 1,)),
                dma((8, NK)),
                dma((8, NK)),
                dma((NB + NX, 2)),
                dma((NBD,)),
                dma((4, NC)),
                dma((4, NC)),
                dma((4, NC)),
                dma((4, NC)),
                dma((NC,)),
                pltpu.SemaphoreType.REGULAR,
            ],
            compiler_params=pltpu.CompilerParams(
                collective_id=0, has_side_effects=True, vmem_limit_bytes=67043328,
            ),
            cost_estimate=pl.CostEstimate(
                flops=6 * LOCAL * GROUP * CAP * WIDTH * FF,
                bytes_accessed=6 * LOCAL * WIDTH * FF,
                transcendentals=LOCAL * GROUP * CAP * FF,
            ),
            name="moe_layer",
        )(expert_ids.T, slot_ids.T, gate_weights.T, tokens, w_gate, w_up, w_down)

    return jax.shard_map(local_layer, mesh=mesh, in_specs=(tok_spec, tok_spec, tok_spec, tok_spec, weight_spec, weight_spec, weight_spec), out_specs=tok_spec, check_vma=False)
```

```python
import jax
import jax.numpy as jnp
from jax import lax
from jax.experimental import pallas as pl
from jax.experimental.pallas import tpu as pltpu
from jax.sharding import PartitionSpec as P

CAP_FACTOR = 2
MESH = pl.DeviceIdType.MESH
F32 = jnp.float32
BF16 = jnp.bfloat16

ROWS = 256
WIDTH = 2048
FF = 768
LOCAL = 16
CAP = 32
GROUP = 8
SLOTS = LOCAL * CAP
KC = 256
NK = WIDTH // KC
U = 4
NB = 5
CC = 256
NC = WIDTH // CC
NBD = 2
LAG = 2

OWN = 0
PBUF = 64
DRECV = 80
RA1 = 144
RB1 = 160
RA2 = 176
RB2 = 184
NBLK = 192


def capacity(rows, top_k, experts):
    return ((CAP_FACTOR * rows * top_k + 8 * experts - 1) // (8 * experts)) * 8


def layer_kernel(
    id_ref, slot_ref, gate_ref, tok_ref, wg_ref, wu_ref, wd_ref, out_ref,
    rall, rt, xall, pmat, gmat, gbuf, big, wbuf, dbuf, obuf,
    lsem, rs_sem, rr_sem, xs_sem, xr_sem, w_sem, d_sem,
    ds_sem, dr_sem, is_sem, ir_sem, o_sem, ready,
):
    data = lax.axis_index("data")
    y = lax.axis_index("node")
    ex = lax.axis_index("expert")
    x = ex // 2
    q = ex % 2
    g = y * 4 + ex
    flip = 1 - 2 * q
    gx = y * 4 + (1 - x) * 2 + q
    gy = (1 - y) * 4 + x * 2 + q
    gd = (1 - y) * 4 + (1 - x) * 2 + q
    gp = g + flip
    partner = (data, y, ex + flip)
    xn = (data, y, (1 - x) * 2 + q)
    yn = (data, 1 - y, ex)

    barrier = pltpu.get_barrier_semaphore()
    for d in range(1, GROUP):
        t = (g + d) % GROUP
        pl.semaphore_signal(barrier, inc=1, device_id=(data, t // 4, t % 4), device_id_type=MESH)

    def own_load(k):
        return pltpu.make_async_copy(
            tok_ref.at[:, pl.ds(pl.multiple_of(k * KC, KC), KC)],
            xall.at[pl.ds(pl.multiple_of((k * GROUP + g) * ROWS, ROWS), ROWS), :],
            lsem.at[k],
        )

    for k in range(NK):
        own_load(k).start()

    steps = LOCAL // U

    def w_load(i):
        k, e, slot = i // steps, (i % steps) * U, i % NB
        rows = pl.ds(pl.multiple_of(k * KC, KC), KC)
        return [
            pltpu.make_async_copy(ref.at[pl.ds(e, U), rows, :], wbuf.at[slot, j], w_sem.at[slot, j])
            for j, ref in enumerate((wg_ref, wu_ref))
        ]

    def d_load(i):
        c, e, slot = i // steps, (i % steps) * U, i % NBD
        cols = pl.ds(pl.multiple_of(c * CC, CC), CC)
        return pltpu.make_async_copy(wd_ref.at[pl.ds(e, U), :, cols], dbuf.at[slot], d_sem.at[slot])

    for i in range(NB):
        for cp in w_load(i):
            cp.start()
    for i in range(NBD):
        d_load(i).start()

    mine = pl.multiple_of(g * 16, 16)
    flat_pos = jnp.where(slot_ref[...] >= 0, id_ref[...] * CAP + slot_ref[...], -1)
    rall[pl.ds(mine, 8), :] = flat_pos.astype(F32)
    rall[pl.ds(mine + 8, 8), :] = gate_ref[...]
    pl.semaphore_wait(barrier, GROUP - 1)

    def r_copy(d, owner, dst):
        ref = rall.at[pl.ds(pl.multiple_of(owner * 16, 16), 16), :]
        return pltpu.make_async_remote_copy(
            src_ref=ref,
            dst_ref=ref,
            send_sem=rs_sem.at[d - 1],
            recv_sem=rr_sem.at[d - 1],
            device_id=(data, dst // 4, dst % 4),
            device_id_type=MESH,
        )

    for d in range(1, GROUP):
        r_copy(d, g, (g + d) % GROUP).start()

    def x_copy(i, k, s, dev, lo=0, n=ROWS):
        ref = xall.at[pl.ds(pl.multiple_of((k * GROUP + s) * ROWS + lo, 128), n), :]
        return pltpu.make_async_remote_copy(
            src_ref=ref, dst_ref=ref, send_sem=xs_sem.at[i, k], recv_sem=xr_sem.at[i, k],
            device_id=dev, device_id_type=MESH,
        )

    HALF = ROWS // 2

    def send(i, k):
        return x_copy(i, k, *(
            (g, partner),
            (g, xn),
            (g, yn),
            (gx, yn, 0, HALF),
            (gx, partner),
            (gy, xn, HALF, HALF),
            (gy, partner),
            (gd, partner),
        )[i])

    def arrival(i, k):
        return x_copy(i, k, *(
            (gp, partner),
            (gx, xn),
            (gy, yn),
            (gd, yn, 0, HALF),
            (gx + flip, partner),
            (gd, xn, HALF, HALF),
            (gy + flip, partner),
            (gd + flip, partner),
        )[i])

    def own(k):
        own_load(k).wait()
        for i in (1, 2, 0):
            send(i, k).start()

    def forward(k):
        arrival(1, k).wait_recv()
        send(3, k).start()
        send(4, k).start()
        arrival(2, k).wait_recv()
        send(5, k).start()
        send(6, k).start()

    def diagonal(k):
        arrival(3, k).wait_recv()
        arrival(5, k).wait_recv()
        send(7, k).start()

    def finish(k):
        for i in (0, 4, 6, 7):
            arrival(i, k).wait_recv()

    own(0)
    own(1)

    for d in range(1, GROUP):
        r_copy(d, (g + GROUP - d) % GROUP, g).wait_recv()
    rt[...] = jnp.transpose(rall[...])

    base = (g * SLOTS).astype(F32)
    ybuf = pmat
    PB = 64
    GB = 64

    def build_p(i, carry):
        s, b = i // (SLOTS // PB), i % (SLOTS // PB)
        want = lax.broadcasted_iota(jnp.int32, (PB, ROWS), 0).astype(F32) + (base + (b * PB).astype(F32))
        pos = rall[pl.ds(pl.multiple_of(s * 16, 16), 8), :]
        hit = jnp.zeros((PB, ROWS), F32)
        for j in range(8):
            hit = jnp.where(pos[j : j + 1, :] == want, 1.0, hit)
        pmat[s, pl.ds(pl.multiple_of(b * PB, PB), PB), :] = hit.astype(BF16)
        return carry

    def build_g(i, carry):
        s, b = i % GROUP, i // GROUP
        t0 = pl.multiple_of(b * GB, GB)
        v = pltpu.roll(rt[pl.ds(t0, GB), :], (128 - s * 16) % 128, 1)
        want = lax.broadcasted_iota(jnp.int32, (GB, SLOTS), 1).astype(F32) + base
        sel = jnp.zeros((GB, SLOTS), F32)
        for j in range(8):
            sel = jnp.where(v[:, j : j + 1] == want, v[:, 8 + j : 9 + j], sel)
        g1 = (sel * (1.0 - 2.0**-8)).astype(BF16)
        rest = sel - g1.astype(F32)
        g2 = rest.astype(BF16)
        g3 = (rest - g2.astype(F32)).astype(BF16)
        for p, part in enumerate((g1, g2, g3)):
            gmat[s, pl.ds(pl.multiple_of(p * 256 + t0, GB), GB), :] = part
        return carry

    lax.fori_loop(0, GROUP * SLOTS // PB, build_p, 0)
    forward(0)
    own(2)
    gn = GROUP * ROWS // GB
    lax.fori_loop(0, gn // 4, build_g, 0)
    forward(1)
    own(3)
    diagonal(0)
    finish(0)

    def gather_rows(k):
        for s in range(GROUP):
            xs = xall[pl.ds(pl.multiple_of((k * GROUP + s) * ROWS, ROWS), ROWS), :]
            gbuf[s] = jnp.dot(pmat[s], xs, preferred_element_type=F32).astype(BF16)

    def block(i, n=1):
        return pl.ds(pl.multiple_of(i * 256, 256), n * 256)

    def down(c, t):
        i = c * steps + t
        slot = i % NBD
        d_load(i).wait()
        rows = pl.ds(pl.multiple_of(t * U * CAP, U * CAP), U * CAP)
        h4 = xall.at[block(t * U * 3, U * 3), :]
        for u in range(U):
            h = jnp.concatenate([h4[(u * 3 + n) * 256 : (u * 3 + n + 1) * 256, :] for n in range(3)], axis=1)
            v = jnp.dot(h, dbuf[slot, u], preferred_element_type=F32).astype(BF16)
            ybuf.at[:, rows, :][:, u * CAP : (u + 1) * CAP, :] = v.reshape(GROUP, CAP, CC)

        @pl.when(i + NBD < NC * steps)
        def _():
            d_load(i + NBD).start()

    def experts(k, first=False, last=False):
        def body(t, carry):
            i = k * steps + t
            for cp in w_load(i):
                cp.wait()
            w4 = wbuf.at[i % NB]
            lhs4 = gbuf.at[:, pl.ds(pl.multiple_of(t * U * CAP, U * CAP), U * CAP), :]
            h4 = xall.at[block(t * U * 3, U * 3), :]
            big4 = big.at[block(t * U * 12, U * 12), :]
            for u in range(U):
                lhs = lhs4[:, u * CAP : (u + 1) * CAP, :].reshape(GROUP * CAP, KC)
                for n in range(FF // 256):
                    vals = []
                    for j in range(2):
                        v = jnp.dot(lhs, w4[j, u, :, n * 256 : (n + 1) * 256], preferred_element_type=F32)
                        at = (u * 12 + j * 6 + n * 2) * 256
                        if not first:
                            v = v + jnp.concatenate([big4[at : at + 256, :], big4[at + 256 : at + 512, :]], axis=1)
                        if not last:
                            big4[at : at + 256, :] = v[:, :128]
                            big4[at + 256 : at + 512, :] = v[:, 128:]
                        vals.append(v)
                    if last:
                        h4[(u * 3 + n) * 256 : (u * 3 + n + 1) * 256, :] = (jax.nn.silu(vals[0]) * vals[1]).astype(BF16)

            @pl.when(i + NB < NK * steps)
            def _():
                for cp in w_load(i + NB):
                    cp.start()

            if last:
                down(0, t)
            else:
                if not first:
                    build_g(4 + k * 4 + t, 0)

                @pl.when(jnp.logical_and(t == 0, k + 2 < NK))
                def _():
                    forward(k + 2)

                @pl.when(jnp.logical_and(t == 0, k + 4 < NK))
                def _():
                    own(k + 4)

                @pl.when(t == 2)
                def _():
                    diagonal(k + 1)

            return carry

        lax.fori_loop(0, steps, body, 0)

    gather_rows(0)
    experts(0, first=True)
    finish(1)

    def middle(k, carry):
        gather_rows(k)
        experts(k)

        finish(k + 1)
        return carry

    lax.fori_loop(1, NK - 1, middle, 0)
    for k in range(6):
        for i in range(8):
            send(i, k).wait_send()
    gather_rows(NK - 1)
    experts(NK - 1, last=True)

    for dev in (partner, xn, yn):
        pl.semaphore_signal(ready, inc=1, device_id=dev, device_id_type=MESH)

    def part(core, d, to):
        dx, dy = d % 2, d // 2
        s = ((y + dy) % 2) * 4 + ((x + dx) % 2) * 2 + core
        ys = ybuf[s]
        v = jnp.dot(gmat[s], ys, preferred_element_type=F32)
        v = v[0:256] + (v[256:512] + v[512:768])
        into = big.at[block(to, 8), :]
        a, b = (dx * 2 + dy) * 256, (4 + dy * 2 + dx) * 256
        into[a : a + 256, :] = v[:, :128]
        into[b : b + 256, :] = v[:, 128:]

    def d2d(i, c):
        at = (2, 6, 0, 4)[i]
        return pltpu.make_async_remote_copy(
            src_ref=big.at[block(PBUF + (c % 2) * 8 + at, 2), :],
            dst_ref=big.at[block(DRECV + c * 8 + at, 2), :],
            send_sem=ds_sem.at[i, c], recv_sem=dr_sem.at[i, c],
            device_id=partner, device_id_type=MESH,
        )

    def pair_sum(i, c):
        at = (2, 6, 0, 4)[i]
        d2d(i, c).wait_recv()
        rows = block(OWN + c * 8 + at, 2)
        big[rows, :] = big[rows, :] + big[block(DRECV + c * 8 + at, 2), :]

    def ici(i, c):
        src, dst, n, dev = (
            (OWN + c * 8 + 2, RA1 + c * 2, 2, xn),
            (OWN + c * 8 + 6, RB1 + c * 2, 2, yn),
            (OWN + c * 8 + 1, RA2 + c, 1, yn),
            (OWN + c * 8 + 5, RB2 + c, 1, xn),
        )[i]
        return pltpu.make_async_remote_copy(
            src_ref=big.at[block(src, n), :], dst_ref=big.at[block(dst, n), :],
            send_sem=is_sem.at[i, c], recv_sem=ir_sem.at[i, c],
            device_id=dev, device_id_type=MESH,
        )

    def second_hop(c):
        ici(0, c).wait_recv()
        big[block(OWN + c * 8 + 1), :] = big[block(OWN + c * 8 + 1), :] + big[block(RA1 + c * 2 + 1), :]
        ici(2, c).start()
        ici(1, c).wait_recv()
        big[block(OWN + c * 8 + 5), :] = big[block(OWN + c * 8 + 5), :] + big[block(RB1 + c * 2 + 1), :]
        ici(3, c).start()

    def column_chunk(c, carry):
        @pl.when(c > 0)
        def _():
            def one(t, inner):
                down(c, t)
                return inner

            lax.fori_loop(0, steps, one, 0)

        @pl.when(c >= 2)
        def _():
            for i in range(4):
                d2d(i, c - 2).wait_send()

        for d in (3, 1, 2, 0):
            part(1 - q, d, PBUF + (c % 2) * 8)

        @pl.when(c == 0)
        def _():
            pl.semaphore_wait(ready, 3)

        for i in range(4):
            d2d(i, c).start()
        for d in (3, 1, 2, 0):
            part(q, d, OWN + c * 8)

        @pl.when(c >= LAG)
        def _():
            second_hop(c - LAG)

        pair_sum(0, c)
        ici(0, c).start()
        pair_sum(1, c)
        ici(1, c).start()
        pair_sum(2, c)
        pair_sum(3, c)
        return carry

    lax.fori_loop(0, NC, column_chunk, 0)

    def tail(c, carry):
        second_hop(c)
        return carry

    lax.fori_loop(NC - LAG, NC, tail, 0)

    def out_copy(c):
        cols = pl.ds(pl.multiple_of(c * CC, CC), CC)
        return pltpu.make_async_copy(obuf.at[c], out_ref.at[:, cols], o_sem.at[c])

    def final(c, carry):
        ici(2, c).wait_recv()
        a = big[block(OWN + c * 8), :] + big[block(RA1 + c * 2), :] + big[block(RA2 + c), :]
        ici(3, c).wait_recv()
        b = big[block(OWN + c * 8 + 4), :] + big[block(RB1 + c * 2), :] + big[block(RB2 + c), :]
        obuf[c, :, 0:128] = a.astype(BF16)
        obuf[c, :, 128:256] = b.astype(BF16)
        out_copy(c).start()
        for i in range(4):
            ici(i, c).wait_send()
        return carry

    lax.fori_loop(0, NC, final, 0)

    for c in range(NC):
        out_copy(c).wait()
    for c in (NC - 2, NC - 1):
        for i in range(4):
            d2d(i, c).wait_send()
    for k in range(6, NK):
        for i in range(8):
            send(i, k).wait_send()
    for d in range(1, GROUP):
        r_copy(d, g, (g + d) % GROUP).wait_send()


def solution(mesh):
    group_axes = ("node", "expert")
    group_size = mesh.shape["node"] * mesh.shape["expert"]
    tok_spec = P(("data", "node", "expert"), None)
    weight_spec = P(("node", "expert"), None, None)

    def local_layer(tokens, expert_ids, gate_weights, slot_ids, w_gate, w_up, w_down):
        rows, width = tokens.shape
        top_k = expert_ids.shape[1]
        local_experts = w_gate.shape[0]
        slot_count = capacity(rows, top_k, local_experts * group_size)
        assert (rows, width, local_experts, slot_count, group_size) == (ROWS, WIDTH, LOCAL, CAP, GROUP)
        vmem = pl.BlockSpec(memory_space=pltpu.VMEM)
        hbm = pl.BlockSpec(memory_space=pl.ANY)
        dma = pltpu.SemaphoreType.DMA
        return pl.pallas_call(
            layer_kernel,
            out_shape=jax.ShapeDtypeStruct((rows, width), BF16),
            in_specs=[vmem, vmem, vmem, hbm, hbm, hbm, hbm],
            out_specs=hbm,
            scratch_shapes=[
                pltpu.VMEM((GROUP * 16, ROWS), F32),
                pltpu.VMEM((ROWS, GROUP * 16), F32),
                pltpu.VMEM((NK * GROUP * ROWS, KC), BF16),
                pltpu.VMEM((GROUP, SLOTS, ROWS), BF16),
                pltpu.VMEM((GROUP, 3 * ROWS, SLOTS), BF16),
                pltpu.VMEM((GROUP, SLOTS, KC), BF16),
                pltpu.VMEM((NBLK * 256, 128), F32),
                pltpu.VMEM((NB, 2, U, KC, FF), BF16),
                pltpu.VMEM((NBD, U, FF, CC), BF16),
                pltpu.VMEM((NC, ROWS, CC), BF16),
                dma((NK,)),
                dma((GROUP - 1,)),
                dma((GROUP - 1,)),
                dma((8, NK)),
                dma((8, NK)),
                dma((NB, 2)),
                dma((NBD,)),
                dma((4, NC)),
                dma((4, NC)),
                dma((4, NC)),
                dma((4, NC)),
                dma((NC,)),
                pltpu.SemaphoreType.REGULAR,
            ],
            compiler_params=pltpu.CompilerParams(
                collective_id=0, has_side_effects=True, vmem_limit_bytes=67043328,
            ),
            cost_estimate=pl.CostEstimate(
                flops=6 * LOCAL * GROUP * CAP * WIDTH * FF,
                bytes_accessed=6 * LOCAL * WIDTH * FF,
                transcendentals=LOCAL * GROUP * CAP * FF,
            ),
            name="moe_layer",
        )(expert_ids.T, slot_ids.T, gate_weights.T, tokens, w_gate, w_up, w_down)

    return jax.shard_map(local_layer, mesh=mesh, in_specs=(tok_spec, tok_spec, tok_spec, tok_spec, weight_spec, weight_spec, weight_spec), out_specs=tok_spec, check_vma=False)
```

```python
import jax
import jax.numpy as jnp
from jax import lax
from jax.experimental import pallas as pl
from jax.experimental.pallas import tpu as pltpu
from jax.sharding import PartitionSpec as P

CAP_FACTOR = 2
MESH = pl.DeviceIdType.MESH
F32 = jnp.float32
BF16 = jnp.bfloat16

ROWS = 256
WIDTH = 2048
FF = 768
LOCAL = 16
CAP = 32
GROUP = 8
SLOTS = LOCAL * CAP
KC = 256
NK = WIDTH // KC
U = 4
NB = 5
CC = 256
NC = WIDTH // CC
NBD = 2
LAG = 2

OWN = 0
PBUF = 64
DRECV = 80
RA1 = 144
RB1 = 160
RA2 = 176
RB2 = 184
NBLK = 192


def capacity(rows, top_k, experts):
    return ((CAP_FACTOR * rows * top_k + 8 * experts - 1) // (8 * experts)) * 8


def layer_kernel(
    id_ref, slot_ref, gate_ref, tok_ref, wg_ref, wu_ref, wd_ref, out_ref,
    rall, rt, xall, pmat, gmat, gbuf, big, wbuf, dbuf, obuf,
    lsem, rs_sem, rr_sem, xs_sem, xr_sem, w_sem, d_sem,
    ds_sem, dr_sem, is_sem, ir_sem, o_sem, ready,
):
    data = lax.axis_index("data")
    y = lax.axis_index("node")
    ex = lax.axis_index("expert")
    x = ex // 2
    q = ex % 2
    g = y * 4 + ex
    flip = 1 - 2 * q
    gx = y * 4 + (1 - x) * 2 + q
    gy = (1 - y) * 4 + x * 2 + q
    gd = (1 - y) * 4 + (1 - x) * 2 + q
    gp = g + flip
    partner = (data, y, ex + flip)
    xn = (data, y, (1 - x) * 2 + q)
    yn = (data, 1 - y, ex)

    barrier = pltpu.get_barrier_semaphore()
    for d in range(1, GROUP):
        t = (g + d) % GROUP
        pl.semaphore_signal(barrier, inc=1, device_id=(data, t // 4, t % 4), device_id_type=MESH)

    def own_load(k):
        return pltpu.make_async_copy(
            tok_ref.at[:, pl.ds(pl.multiple_of(k * KC, KC), KC)],
            xall.at[pl.ds(pl.multiple_of((k * GROUP + g) * ROWS, ROWS), ROWS), :],
            lsem.at[k],
        )

    for k in range(NK):
        own_load(k).start()

    steps = LOCAL // U

    def w_load(i):
        k, e, slot = i // steps, (i % steps) * U, i % NB
        rows = pl.ds(pl.multiple_of(k * KC, KC), KC)
        return [
            pltpu.make_async_copy(ref.at[pl.ds(e, U), rows, :], wbuf.at[slot, j], w_sem.at[slot, j])
            for j, ref in enumerate((wg_ref, wu_ref))
        ]

    def d_load(i):
        c, e, slot = i // steps, (i % steps) * U, i % NBD
        cols = pl.ds(pl.multiple_of(c * CC, CC), CC)
        return pltpu.make_async_copy(wd_ref.at[pl.ds(e, U), :, cols], dbuf.at[slot], d_sem.at[slot])

    for i in range(NB):
        for cp in w_load(i):
            cp.start()
    for i in range(NBD):
        d_load(i).start()

    mine = pl.multiple_of(g * 16, 16)
    flat_pos = jnp.where(slot_ref[...] >= 0, id_ref[...] * CAP + slot_ref[...], -1)
    rall[pl.ds(mine, 8), :] = flat_pos.astype(F32)
    rall[pl.ds(mine + 8, 8), :] = gate_ref[...]
    pl.semaphore_wait(barrier, GROUP - 1)

    def r_copy(d, owner, dst):
        ref = rall.at[pl.ds(pl.multiple_of(owner * 16, 16), 16), :]
        return pltpu.make_async_remote_copy(
            src_ref=ref,
            dst_ref=ref,
            send_sem=rs_sem.at[d - 1],
            recv_sem=rr_sem.at[d - 1],
            device_id=(data, dst // 4, dst % 4),
            device_id_type=MESH,
        )

    for d in range(1, GROUP):
        r_copy(d, g, (g + d) % GROUP).start()

    def x_copy(i, k, s, dev, lo=0, n=ROWS):
        ref = xall.at[pl.ds(pl.multiple_of((k * GROUP + s) * ROWS + lo, 128), n), :]
        return pltpu.make_async_remote_copy(
            src_ref=ref, dst_ref=ref, send_sem=xs_sem.at[i, k], recv_sem=xr_sem.at[i, k],
            device_id=dev, device_id_type=MESH,
        )

    HALF = ROWS // 2

    def send(i, k):
        return x_copy(i, k, *(
            (g, partner),
            (g, xn),
            (g, yn),
            (gx, yn, 0, HALF),
            (gx, partner),
            (gy, xn, HALF, HALF),
            (gy, partner),
            (gd, partner),
        )[i])

    def arrival(i, k):
        return x_copy(i, k, *(
            (gp, partner),
            (gx, xn),
            (gy, yn),
            (gd, yn, 0, HALF),
            (gx + flip, partner),
            (gd, xn, HALF, HALF),
            (gy + flip, partner),
            (gd + flip, partner),
        )[i])

    def own(k):
        own_load(k).wait()
        for i in (1, 2, 0):
            send(i, k).start()

    def forward(k):
        arrival(1, k).wait_recv()
        send(3, k).start()
        send(4, k).start()
        arrival(2, k).wait_recv()
        send(5, k).start()
        send(6, k).start()

    def diagonal(k):
        arrival(3, k).wait_recv()
        arrival(5, k).wait_recv()
        send(7, k).start()

    def finish(k):
        for i in (0, 4, 6, 7):
            arrival(i, k).wait_recv()

    own(0)
    own(1)

    for d in range(1, GROUP):
        r_copy(d, (g + GROUP - d) % GROUP, g).wait_recv()
    rt[...] = jnp.transpose(rall[...])

    base = (g * SLOTS).astype(F32)
    ybuf = pmat
    PB = 64
    GB = 64

    def build_p(i, carry):
        s, b = i // (SLOTS // PB), i % (SLOTS // PB)
        want = lax.broadcasted_iota(jnp.int32, (PB, ROWS), 0).astype(F32) + (base + (b * PB).astype(F32))
        pos = rall[pl.ds(pl.multiple_of(s * 16, 16), 8), :]
        hit = jnp.zeros((PB, ROWS), F32)
        for j in range(8):
            hit = jnp.where(pos[j : j + 1, :] == want, 1.0, hit)
        pmat[s, pl.ds(pl.multiple_of(b * PB, PB), PB), :] = hit.astype(BF16)
        return carry

    def build_g(i, carry):
        s, b = i % GROUP, i // GROUP
        t0 = pl.multiple_of(b * GB, GB)
        v = pltpu.roll(rt[pl.ds(t0, GB), :], (128 - s * 16) % 128, 1)
        want = lax.broadcasted_iota(jnp.int32, (GB, SLOTS), 1).astype(F32) + base
        sel = jnp.zeros((GB, SLOTS), F32)
        for j in range(8):
            sel = jnp.where(v[:, j : j + 1] == want, v[:, 8 + j : 9 + j], sel)
        g1 = (sel * (1.0 - 2.0**-8)).astype(BF16)
        rest = sel - g1.astype(F32)
        g2 = rest.astype(BF16)
        g3 = (rest - g2.astype(F32)).astype(BF16)
        for p, part in enumerate((g1, g2, g3)):
            gmat[s, pl.ds(pl.multiple_of(p * 256 + t0, GB), GB), :] = part
        return carry

    lax.fori_loop(0, GROUP * SLOTS // PB, build_p, 0)
    forward(0)
    own(2)
    gn = GROUP * ROWS // GB
    lax.fori_loop(0, gn // 4, build_g, 0)
    forward(1)
    own(3)
    diagonal(0)
    finish(0)

    def gather_rows(k):
        for s in range(GROUP):
            xs = xall[pl.ds(pl.multiple_of((k * GROUP + s) * ROWS, ROWS), ROWS), :]
            gbuf[s] = jnp.dot(pmat[s], xs, preferred_element_type=F32).astype(BF16)

    def block(i, n=1):
        return pl.ds(pl.multiple_of(i * 256, 256), n * 256)

    def down(c, t):
        i = c * steps + t
        slot = i % NBD
        d_load(i).wait()
        rows = pl.ds(pl.multiple_of(t * U * CAP, U * CAP), U * CAP)
        h4 = xall.at[block(t * U * 3, U * 3), :]
        for u in range(U):
            h = jnp.concatenate([h4[(u * 3 + n) * 256 : (u * 3 + n + 1) * 256, :] for n in range(3)], axis=1)
            v = jnp.dot(h, dbuf[slot, u], preferred_element_type=F32).astype(BF16)
            ybuf.at[:, rows, :][:, u * CAP : (u + 1) * CAP, :] = v.reshape(GROUP, CAP, CC)

        @pl.when(i + NBD < NC * steps)
        def _():
            d_load(i + NBD).start()

    def experts(k, first=False, last=False):
        wide = 1 if last else 2

        def body(tt, carry):
            i = k * steps + tt * wide
            for w in range(wide):
                for cp in w_load(i + w):
                    cp.wait()
            for w in range(wide):
                one_step(tt * wide + w, wbuf.at[(i + w) % NB])
            for w in range(wide):

                @pl.when(i + w + NB < NK * steps)
                def _():
                    for cp in w_load(i + w + NB):
                        cp.start()

            if last:
                down(0, tt)
            else:
                if not first:
                    for w in range(wide):
                        build_g(4 + k * 4 + tt * wide + w, 0)

                @pl.when(jnp.logical_and(tt == 0, k + 2 < NK))
                def _():
                    forward(k + 2)

                @pl.when(jnp.logical_and(tt == 0, k + 4 < NK))
                def _():
                    own(k + 4)

                @pl.when(tt == 0)
                def _():
                    diagonal(k + 1)

            return carry

        def one_step(t, w4):
            lhs4 = gbuf.at[:, pl.ds(pl.multiple_of(t * U * CAP, U * CAP), U * CAP), :]
            h4 = xall.at[block(t * U * 3, U * 3), :]
            big4 = big.at[block(t * U * 12, U * 12), :]
            for u in range(U):
                lhs = lhs4[:, u * CAP : (u + 1) * CAP, :].reshape(GROUP * CAP, KC)
                for n in range(FF // 256):
                    vals = []
                    for j in range(2):
                        v = jnp.dot(lhs, w4[j, u, :, n * 256 : (n + 1) * 256], preferred_element_type=F32)
                        at = (u * 12 + j * 6 + n * 2) * 256
                        if not first:
                            v = v + jnp.concatenate([big4[at : at + 256, :], big4[at + 256 : at + 512, :]], axis=1)
                        if not last:
                            big4[at : at + 256, :] = v[:, :128]
                            big4[at + 256 : at + 512, :] = v[:, 128:]
                        vals.append(v)
                    if last:
                        h4[(u * 3 + n) * 256 : (u * 3 + n + 1) * 256, :] = (jax.nn.silu(vals[0]) * vals[1]).astype(BF16)

        lax.fori_loop(0, steps // wide, body, 0)

    gather_rows(0)
    experts(0, first=True)
    finish(1)

    def middle(k, carry):
        gather_rows(k)
        experts(k)

        finish(k + 1)
        return carry

    lax.fori_loop(1, NK - 1, middle, 0)
    for k in range(6):
        for i in range(8):
            send(i, k).wait_send()
    gather_rows(NK - 1)
    experts(NK - 1, last=True)

    for dev in (partner, xn, yn):
        pl.semaphore_signal(ready, inc=1, device_id=dev, device_id_type=MESH)

    def part(core, d, to):
        dx, dy = d % 2, d // 2
        s = ((y + dy) % 2) * 4 + ((x + dx) % 2) * 2 + core
        ys = ybuf[s]
        v = jnp.dot(gmat[s], ys, preferred_element_type=F32)
        v = v[0:256] + (v[256:512] + v[512:768])
        into = big.at[block(to, 8), :]
        a, b = (dx * 2 + dy) * 256, (4 + dy * 2 + dx) * 256
        into[a : a + 256, :] = v[:, :128]
        into[b : b + 256, :] = v[:, 128:]

    def d2d(i, c):
        at = (2, 6, 0, 4)[i]
        return pltpu.make_async_remote_copy(
            src_ref=big.at[block(PBUF + (c % 2) * 8 + at, 2), :],
            dst_ref=big.at[block(DRECV + c * 8 + at, 2), :],
            send_sem=ds_sem.at[i, c], recv_sem=dr_sem.at[i, c],
            device_id=partner, device_id_type=MESH,
        )

    def pair_sum(i, c):
        at = (2, 6, 0, 4)[i]
        d2d(i, c).wait_recv()
        rows = block(OWN + c * 8 + at, 2)
        big[rows, :] = big[rows, :] + big[block(DRECV + c * 8 + at, 2), :]

    def ici(i, c):
        src, dst, n, dev = (
            (OWN + c * 8 + 2, RA1 + c * 2, 2, xn),
            (OWN + c * 8 + 6, RB1 + c * 2, 2, yn),
            (OWN + c * 8 + 1, RA2 + c, 1, yn),
            (OWN + c * 8 + 5, RB2 + c, 1, xn),
        )[i]
        return pltpu.make_async_remote_copy(
            src_ref=big.at[block(src, n), :], dst_ref=big.at[block(dst, n), :],
            send_sem=is_sem.at[i, c], recv_sem=ir_sem.at[i, c],
            device_id=dev, device_id_type=MESH,
        )

    def second_hop(c):
        ici(0, c).wait_recv()
        big[block(OWN + c * 8 + 1), :] = big[block(OWN + c * 8 + 1), :] + big[block(RA1 + c * 2 + 1), :]
        ici(2, c).start()
        ici(1, c).wait_recv()
        big[block(OWN + c * 8 + 5), :] = big[block(OWN + c * 8 + 5), :] + big[block(RB1 + c * 2 + 1), :]
        ici(3, c).start()

    def column_chunk(c, carry):
        @pl.when(c > 0)
        def _():
            def one(t, inner):
                down(c, t)
                return inner

            lax.fori_loop(0, steps, one, 0)

        @pl.when(c >= 2)
        def _():
            for i in range(4):
                d2d(i, c - 2).wait_send()

        for d in (3, 1, 2, 0):
            part(1 - q, d, PBUF + (c % 2) * 8)

        @pl.when(c == 0)
        def _():
            pl.semaphore_wait(ready, 3)

        for i in range(4):
            d2d(i, c).start()
        for d in (3, 1, 2, 0):
            part(q, d, OWN + c * 8)

        @pl.when(c >= LAG)
        def _():
            second_hop(c - LAG)

        pair_sum(0, c)
        ici(0, c).start()
        pair_sum(1, c)
        ici(1, c).start()
        pair_sum(2, c)
        pair_sum(3, c)
        return carry

    lax.fori_loop(0, NC, column_chunk, 0)

    def tail(c, carry):
        second_hop(c)
        return carry

    lax.fori_loop(NC - LAG, NC, tail, 0)

    def out_copy(c):
        cols = pl.ds(pl.multiple_of(c * CC, CC), CC)
        return pltpu.make_async_copy(obuf.at[c], out_ref.at[:, cols], o_sem.at[c])

    def final(c, carry):
        ici(2, c).wait_recv()
        a = big[block(OWN + c * 8), :] + big[block(RA1 + c * 2), :] + big[block(RA2 + c), :]
        ici(3, c).wait_recv()
        b = big[block(OWN + c * 8 + 4), :] + big[block(RB1 + c * 2), :] + big[block(RB2 + c), :]
        obuf[c, :, 0:128] = a.astype(BF16)
        obuf[c, :, 128:256] = b.astype(BF16)
        out_copy(c).start()
        for i in range(4):
            ici(i, c).wait_send()
        return carry

    lax.fori_loop(0, NC, final, 0)

    for c in range(NC):
        out_copy(c).wait()
    for c in (NC - 2, NC - 1):
        for i in range(4):
            d2d(i, c).wait_send()
    for k in range(6, NK):
        for i in range(8):
            send(i, k).wait_send()
    for d in range(1, GROUP):
        r_copy(d, g, (g + d) % GROUP).wait_send()


def solution(mesh):
    group_axes = ("node", "expert")
    group_size = mesh.shape["node"] * mesh.shape["expert"]
    tok_spec = P(("data", "node", "expert"), None)
    weight_spec = P(("node", "expert"), None, None)

    def local_layer(tokens, expert_ids, gate_weights, slot_ids, w_gate, w_up, w_down):
        rows, width = tokens.shape
        top_k = expert_ids.shape[1]
        local_experts = w_gate.shape[0]
        slot_count = capacity(rows, top_k, local_experts * group_size)
        assert (rows, width, local_experts, slot_count, group_size) == (ROWS, WIDTH, LOCAL, CAP, GROUP)
        vmem = pl.BlockSpec(memory_space=pltpu.VMEM)
        hbm = pl.BlockSpec(memory_space=pl.ANY)
        dma = pltpu.SemaphoreType.DMA
        return pl.pallas_call(
            layer_kernel,
            out_shape=jax.ShapeDtypeStruct((rows, width), BF16),
            in_specs=[vmem, vmem, vmem, hbm, hbm, hbm, hbm],
            out_specs=hbm,
            scratch_shapes=[
                pltpu.VMEM((GROUP * 16, ROWS), F32),
                pltpu.VMEM((ROWS, GROUP * 16), F32),
                pltpu.VMEM((NK * GROUP * ROWS, KC), BF16),
                pltpu.VMEM((GROUP, SLOTS, ROWS), BF16),
                pltpu.VMEM((GROUP, 3 * ROWS, SLOTS), BF16),
                pltpu.VMEM((GROUP, SLOTS, KC), BF16),
                pltpu.VMEM((NBLK * 256, 128), F32),
                pltpu.VMEM((NB, 2, U, KC, FF), BF16),
                pltpu.VMEM((NBD, U, FF, CC), BF16),
                pltpu.VMEM((NC, ROWS, CC), BF16),
                dma((NK,)),
                dma((GROUP - 1,)),
                dma((GROUP - 1,)),
                dma((8, NK)),
                dma((8, NK)),
                dma((NB, 2)),
                dma((NBD,)),
                dma((4, NC)),
                dma((4, NC)),
                dma((4, NC)),
                dma((4, NC)),
                dma((NC,)),
                pltpu.SemaphoreType.REGULAR,
            ],
            compiler_params=pltpu.CompilerParams(
                collective_id=0, has_side_effects=True, vmem_limit_bytes=67043328,
            ),
            cost_estimate=pl.CostEstimate(
                flops=6 * LOCAL * GROUP * CAP * WIDTH * FF,
                bytes_accessed=6 * LOCAL * WIDTH * FF,
                transcendentals=LOCAL * GROUP * CAP * FF,
            ),
            name="moe_layer",
        )(expert_ids.T, slot_ids.T, gate_weights.T, tokens, w_gate, w_up, w_down)

    return jax.shard_map(local_layer, mesh=mesh, in_specs=(tok_spec, tok_spec, tok_spec, tok_spec, weight_spec, weight_spec, weight_spec), out_specs=tok_spec, check_vma=False)
```

```python
import jax
import jax.numpy as jnp
from jax import lax
from jax.experimental import pallas as pl
from jax.experimental.pallas import tpu as pltpu
from jax.sharding import PartitionSpec as P

CAP_FACTOR = 2
MESH = pl.DeviceIdType.MESH
F32 = jnp.float32
BF16 = jnp.bfloat16

ROWS = 256
WIDTH = 2048
FF = 768
LOCAL = 16
CAP = 32
GROUP = 8
SLOTS = LOCAL * CAP
KC = 256
NK = WIDTH // KC
U = 4
NB = 5
CC = 256
NC = WIDTH // CC
NBD = 2
LAG = 2

OWN = 0
PBUF = 64
DRECV = 80
RA1 = 144
RB1 = 160
RA2 = 176
RB2 = 184
NBLK = 192


def capacity(rows, top_k, experts):
    return ((CAP_FACTOR * rows * top_k + 8 * experts - 1) // (8 * experts)) * 8


def layer_kernel(
    id_ref, slot_ref, gate_ref, tok_ref, wg_ref, wu_ref, wd_ref, out_ref,
    rall, rt, xall, pmat, gmat, gbuf, big, wbuf, dbuf,
    lsem, rs_sem, rr_sem, xs_sem, xr_sem, w_sem, d_sem,
    ds_sem, dr_sem, is_sem, ir_sem, ready,
):
    data = lax.axis_index("data")
    y = lax.axis_index("node")
    ex = lax.axis_index("expert")
    x = ex // 2
    q = ex % 2
    g = y * 4 + ex
    flip = 1 - 2 * q
    gx = y * 4 + (1 - x) * 2 + q
    gy = (1 - y) * 4 + x * 2 + q
    gd = (1 - y) * 4 + (1 - x) * 2 + q
    gp = g + flip
    partner = (data, y, ex + flip)
    xn = (data, y, (1 - x) * 2 + q)
    yn = (data, 1 - y, ex)

    barrier = pltpu.get_barrier_semaphore()
    for d in range(1, GROUP):
        t = (g + d) % GROUP
        pl.semaphore_signal(barrier, inc=1, device_id=(data, t // 4, t % 4), device_id_type=MESH)

    def own_load(k):
        return pltpu.make_async_copy(
            tok_ref.at[:, pl.ds(pl.multiple_of(k * KC, KC), KC)],
            xall.at[pl.ds(pl.multiple_of((k * GROUP + g) * ROWS, ROWS), ROWS), :],
            lsem.at[k],
        )

    for k in range(NK):
        own_load(k).start()

    steps = LOCAL // U

    def w_load(i):
        k, e, slot = i // steps, (i % steps) * U, i % NB
        rows = pl.ds(pl.multiple_of(k * KC, KC), KC)
        return [
            pltpu.make_async_copy(ref.at[pl.ds(e, U), rows, :], wbuf.at[slot, j], w_sem.at[slot, j])
            for j, ref in enumerate((wg_ref, wu_ref))
        ]

    def d_load(i):
        c, e, slot = i // steps, (i % steps) * U, i % NBD
        cols = pl.ds(pl.multiple_of(c * CC, CC), CC)
        return pltpu.make_async_copy(wd_ref.at[pl.ds(e, U), :, cols], dbuf.at[slot], d_sem.at[slot])

    for i in range(NB):
        for cp in w_load(i):
            cp.start()
    for i in range(NBD):
        d_load(i).start()

    mine = pl.multiple_of(g * 16, 16)
    flat_pos = jnp.where(slot_ref[...] >= 0, id_ref[...] * CAP + slot_ref[...], -1)
    rall[pl.ds(mine, 8), :] = flat_pos.astype(F32)
    rall[pl.ds(mine + 8, 8), :] = gate_ref[...]
    pl.semaphore_wait(barrier, GROUP - 1)

    def r_copy(d, half, owner, dst):
        ref = rall.at[pl.ds(pl.multiple_of(owner * 16 + half * 8, 8), 8), :]
        return pltpu.make_async_remote_copy(
            src_ref=ref,
            dst_ref=ref,
            send_sem=rs_sem.at[half, d - 1],
            recv_sem=rr_sem.at[half, d - 1],
            device_id=(data, dst // 4, dst % 4),
            device_id_type=MESH,
        )

    for d in range(1, GROUP):
        r_copy(d, 0, g, (g + d) % GROUP).start()

    def x_copy(i, k, s, dev, lo=0, n=ROWS):
        ref = xall.at[pl.ds(pl.multiple_of((k * GROUP + s) * ROWS + lo, 128), n), :]
        return pltpu.make_async_remote_copy(
            src_ref=ref, dst_ref=ref, send_sem=xs_sem.at[i, k], recv_sem=xr_sem.at[i, k],
            device_id=dev, device_id_type=MESH,
        )

    HALF = ROWS // 2

    def send(i, k):
        return x_copy(i, k, *(
            (g, partner),
            (g, xn),
            (g, yn),
            (gx, yn, 0, HALF),
            (gx, partner),
            (gy, xn, HALF, HALF),
            (gy, partner),
            (gd, partner),
        )[i])

    def arrival(i, k):
        return x_copy(i, k, *(
            (gp, partner),
            (gx, xn),
            (gy, yn),
            (gd, yn, 0, HALF),
            (gx + flip, partner),
            (gd, xn, HALF, HALF),
            (gy + flip, partner),
            (gd + flip, partner),
        )[i])

    def own(k):
        own_load(k).wait()
        for i in (1, 2, 0):
            send(i, k).start()

    def forward(k):
        arrival(1, k).wait_recv()
        send(3, k).start()
        send(4, k).start()
        arrival(2, k).wait_recv()
        send(5, k).start()
        send(6, k).start()

    def diagonal(k):
        arrival(3, k).wait_recv()
        arrival(5, k).wait_recv()
        send(7, k).start()

    def finish(k):
        for i in (0, 4, 6, 7):
            arrival(i, k).wait_recv()

    own(0)
    own(1)
    for d in range(1, GROUP):
        r_copy(d, 1, g, (g + d) % GROUP).start()

    for d in range(1, GROUP):
        r_copy(d, 0, (g + GROUP - d) % GROUP, g).wait_recv()

    base = (g * SLOTS).astype(F32)
    ybuf = pmat
    PB = 64
    GB = 64

    def build_p(i, carry):
        s, b = i // (SLOTS // PB), i % (SLOTS // PB)
        want = lax.broadcasted_iota(jnp.int32, (PB, ROWS), 0).astype(F32) + (base + (b * PB).astype(F32))
        pos = rall[pl.ds(pl.multiple_of(s * 16, 16), 8), :]
        hit = jnp.zeros((PB, ROWS), F32)
        for j in range(8):
            hit = jnp.where(pos[j : j + 1, :] == want, 1.0, hit)
        pmat[s, pl.ds(pl.multiple_of(b * PB, PB), PB), :] = hit.astype(BF16)
        return carry

    def build_g(i, carry):
        s, b = i % GROUP, i // GROUP
        t0 = pl.multiple_of(b * GB, GB)
        v = pltpu.roll(rt[pl.ds(t0, GB), :], (128 - s * 16) % 128, 1)
        want = lax.broadcasted_iota(jnp.int32, (GB, SLOTS), 1).astype(F32) + base
        sel = jnp.zeros((GB, SLOTS), F32)
        for j in range(8):
            sel = jnp.where(v[:, j : j + 1] == want, v[:, 8 + j : 9 + j], sel)
        g1 = (sel * (1.0 - 2.0**-8)).astype(BF16)
        rest = sel - g1.astype(F32)
        g2 = rest.astype(BF16)
        g3 = (rest - g2.astype(F32)).astype(BF16)
        for p, part in enumerate((g1, g2, g3)):
            gmat[s, pl.ds(pl.multiple_of(p * 256 + t0, GB), GB), :] = part
        return carry

    lax.fori_loop(0, GROUP * SLOTS // PB, build_p, 0)
    forward(0)
    own(2)
    for d in range(1, GROUP):
        r_copy(d, 1, (g + GROUP - d) % GROUP, g).wait_recv()
    rt[...] = jnp.transpose(rall[...])
    gn = GROUP * ROWS // GB
    lax.fori_loop(0, gn // 4, build_g, 0)
    forward(1)
    own(3)
    diagonal(0)
    finish(0)

    def gather_rows(k):
        for s in range(GROUP):
            xs = xall[pl.ds(pl.multiple_of((k * GROUP + s) * ROWS, ROWS), ROWS), :]
            gbuf[s] = jnp.dot(pmat[s], xs, preferred_element_type=F32).astype(BF16)

    def block(i, n=1):
        return pl.ds(pl.multiple_of(i * 256, 256), n * 256)

    def down(c, t):
        i = c * steps + t
        slot = i % NBD
        d_load(i).wait()
        rows = pl.ds(pl.multiple_of(t * U * CAP, U * CAP), U * CAP)
        h4 = xall.at[block(t * U * 3, U * 3), :]
        for u in range(U):
            h = jnp.concatenate([h4[(u * 3 + n) * 256 : (u * 3 + n + 1) * 256, :] for n in range(3)], axis=1)
            v = jnp.dot(h, dbuf[slot, u], preferred_element_type=F32).astype(BF16)
            ybuf.at[:, rows, :][:, u * CAP : (u + 1) * CAP, :] = v.reshape(GROUP, CAP, CC)

        @pl.when(i + NBD < NC * steps)
        def _():
            d_load(i + NBD).start()

    def experts(k, first=False, last=False):
        wide = 1 if last else 2

        def body(tt, carry):
            i = k * steps + tt * wide
            for w in range(wide):
                for cp in w_load(i + w):
                    cp.wait()
            for w in range(wide):
                one_step(tt * wide + w, wbuf.at[(i + w) % NB])
            for w in range(wide):

                @pl.when(i + w + NB < NK * steps)
                def _():
                    for cp in w_load(i + w + NB):
                        cp.start()

            if last:
                down(0, tt)
            else:
                if not first:
                    for w in range(wide):
                        build_g(4 + k * 4 + tt * wide + w, 0)

                @pl.when(jnp.logical_and(tt == 0, k + 2 < NK))
                def _():
                    forward(k + 2)

                @pl.when(jnp.logical_and(tt == 0, k + 4 < NK))
                def _():
                    own(k + 4)

                @pl.when(tt == 0)
                def _():
                    diagonal(k + 1)

            return carry

        def one_step(t, w4):
            lhs4 = gbuf.at[:, pl.ds(pl.multiple_of(t * U * CAP, U * CAP), U * CAP), :]
            h4 = xall.at[block(t * U * 3, U * 3), :]
            big4 = big.at[block(t * U * 12, U * 12), :]
            for u in range(U):
                lhs = lhs4[:, u * CAP : (u + 1) * CAP, :].reshape(GROUP * CAP, KC)
                for n in range(FF // 256):
                    vals = []
                    for j in range(2):
                        v = jnp.dot(lhs, w4[j, u, :, n * 256 : (n + 1) * 256], preferred_element_type=F32)
                        at = (u * 12 + j * 6 + n * 2) * 256
                        if not first:
                            v = v + jnp.concatenate([big4[at : at + 256, :], big4[at + 256 : at + 512, :]], axis=1)
                        if not last:
                            big4[at : at + 256, :] = v[:, :128]
                            big4[at + 256 : at + 512, :] = v[:, 128:]
                        vals.append(v)
                    if last:
                        h4[(u * 3 + n) * 256 : (u * 3 + n + 1) * 256, :] = (jax.nn.silu(vals[0]) * vals[1]).astype(BF16)

        lax.fori_loop(0, steps // wide, body, 0)

    gather_rows(0)
    experts(0, first=True)
    finish(1)

    def middle(k, carry):
        gather_rows(k)
        experts(k)

        finish(k + 1)
        return carry

    lax.fori_loop(1, NK - 1, middle, 0)
    for k in range(6):
        for i in range(8):
            send(i, k).wait_send()
    gather_rows(NK - 1)
    experts(NK - 1, last=True)

    for dev in (partner, xn, yn):
        pl.semaphore_signal(ready, inc=1, device_id=dev, device_id_type=MESH)

    def part(core, d, to):
        dx, dy = d % 2, d // 2
        s = ((y + dy) % 2) * 4 + ((x + dx) % 2) * 2 + core
        ys = ybuf[s]
        v = jnp.dot(gmat[s], ys, preferred_element_type=F32)
        v = v[0:256] + (v[256:512] + v[512:768])
        into = big.at[block(to, 8), :]
        a, b = (dx * 2 + dy) * 256, (4 + dy * 2 + dx) * 256
        into[a : a + 256, :] = v[:, :128]
        into[b : b + 256, :] = v[:, 128:]

    def d2d(i, c):
        at = (2, 6, 0, 4)[i]
        return pltpu.make_async_remote_copy(
            src_ref=big.at[block(PBUF + (c % 2) * 8 + at, 2), :],
            dst_ref=big.at[block(DRECV + c * 8 + at, 2), :],
            send_sem=ds_sem.at[i, c], recv_sem=dr_sem.at[i, c],
            device_id=partner, device_id_type=MESH,
        )

    def pair_sum(i, c):
        at = (2, 6, 0, 4)[i]
        d2d(i, c).wait_recv()
        rows = block(OWN + c * 8 + at, 2)
        big[rows, :] = big[rows, :] + big[block(DRECV + c * 8 + at, 2), :]

    def ici(i, c):
        src, dst, n, dev = (
            (OWN + c * 8 + 2, RA1 + c * 2, 2, xn),
            (OWN + c * 8 + 6, RB1 + c * 2, 2, yn),
            (OWN + c * 8 + 1, RA2 + c, 1, yn),
            (OWN + c * 8 + 5, RB2 + c, 1, xn),
        )[i]
        return pltpu.make_async_remote_copy(
            src_ref=big.at[block(src, n), :], dst_ref=big.at[block(dst, n), :],
            send_sem=is_sem.at[i, c], recv_sem=ir_sem.at[i, c],
            device_id=dev, device_id_type=MESH,
        )

    def second_hop(c):
        ici(0, c).wait_recv()
        big[block(OWN + c * 8 + 1), :] = big[block(OWN + c * 8 + 1), :] + big[block(RA1 + c * 2 + 1), :]
        ici(2, c).start()
        ici(1, c).wait_recv()
        big[block(OWN + c * 8 + 5), :] = big[block(OWN + c * 8 + 5), :] + big[block(RB1 + c * 2 + 1), :]
        ici(3, c).start()

    def column_chunk(c, carry):
        @pl.when(c > 0)
        def _():
            def one(t, inner):
                down(c, t)
                return inner

            lax.fori_loop(0, steps, one, 0)

        @pl.when(c >= 2)
        def _():
            for i in range(4):
                d2d(i, c - 2).wait_send()

        for d in (3, 1, 2, 0):
            part(1 - q, d, PBUF + (c % 2) * 8)

        @pl.when(c == 0)
        def _():
            pl.semaphore_wait(ready, 3)

        for i in range(4):
            d2d(i, c).start()
        for d in (3, 1, 2, 0):
            part(q, d, OWN + c * 8)

        @pl.when(c >= LAG)
        def _():
            second_hop(c - LAG)

        pair_sum(0, c)
        ici(0, c).start()
        pair_sum(1, c)
        ici(1, c).start()
        pair_sum(2, c)
        pair_sum(3, c)
        return carry

    lax.fori_loop(0, NC, column_chunk, 0)

    def tail(c, carry):
        second_hop(c)
        return carry

    lax.fori_loop(NC - LAG, NC, tail, 0)

    def final(c, carry):
        ici(2, c).wait_recv()
        a = big[block(OWN + c * 8), :] + big[block(RA1 + c * 2), :] + big[block(RA2 + c), :]
        ici(3, c).wait_recv()
        b = big[block(OWN + c * 8 + 4), :] + big[block(RB1 + c * 2), :] + big[block(RB2 + c), :]
        out_ref[:, pl.ds(pl.multiple_of(c * CC, CC), 128)] = a.astype(BF16)
        out_ref[:, pl.ds(pl.multiple_of(c * CC + 128, 128), 128)] = b.astype(BF16)
        for i in range(4):
            ici(i, c).wait_send()
        return carry

    lax.fori_loop(0, NC, final, 0)

    for c in (NC - 2, NC - 1):
        for i in range(4):
            d2d(i, c).wait_send()
    for k in range(6, NK):
        for i in range(8):
            send(i, k).wait_send()
    for d in range(1, GROUP):
        for half in range(2):
            r_copy(d, half, g, (g + d) % GROUP).wait_send()


def solution(mesh):
    group_axes = ("node", "expert")
    group_size = mesh.shape["node"] * mesh.shape["expert"]
    tok_spec = P(("data", "node", "expert"), None)
    weight_spec = P(("node", "expert"), None, None)

    def local_layer(tokens, expert_ids, gate_weights, slot_ids, w_gate, w_up, w_down):
        rows, width = tokens.shape
        top_k = expert_ids.shape[1]
        local_experts = w_gate.shape[0]
        slot_count = capacity(rows, top_k, local_experts * group_size)
        assert (rows, width, local_experts, slot_count, group_size) == (ROWS, WIDTH, LOCAL, CAP, GROUP)
        vmem = pl.BlockSpec(memory_space=pltpu.VMEM)
        hbm = pl.BlockSpec(memory_space=pl.ANY)
        dma = pltpu.SemaphoreType.DMA
        return pl.pallas_call(
            layer_kernel,
            out_shape=pltpu.VMEM((rows, width), BF16),
            in_specs=[vmem, vmem, vmem, hbm, hbm, hbm, hbm],
            out_specs=vmem,
            scratch_shapes=[
                pltpu.VMEM((GROUP * 16, ROWS), F32),
                pltpu.VMEM((ROWS, GROUP * 16), F32),
                pltpu.VMEM((NK * GROUP * ROWS, KC), BF16),
                pltpu.VMEM((GROUP, SLOTS, ROWS), BF16),
                pltpu.VMEM((GROUP, 3 * ROWS, SLOTS), BF16),
                pltpu.VMEM((GROUP, SLOTS, KC), BF16),
                pltpu.VMEM((NBLK * 256, 128), F32),
                pltpu.VMEM((NB, 2, U, KC, FF), BF16),
                pltpu.VMEM((NBD, U, FF, CC), BF16),
                dma((NK,)),
                dma((2, GROUP - 1)),
                dma((2, GROUP - 1)),
                dma((8, NK)),
                dma((8, NK)),
                dma((NB, 2)),
                dma((NBD,)),
                dma((4, NC)),
                dma((4, NC)),
                dma((4, NC)),
                dma((4, NC)),
                pltpu.SemaphoreType.REGULAR,
            ],
            compiler_params=pltpu.CompilerParams(
                collective_id=0, has_side_effects=True, vmem_limit_bytes=65900000,
            ),
            cost_estimate=pl.CostEstimate(
                flops=6 * LOCAL * GROUP * CAP * WIDTH * FF,
                bytes_accessed=6 * LOCAL * WIDTH * FF,
                transcendentals=LOCAL * GROUP * CAP * FF,
            ),
            name="moe_layer",
        )(expert_ids.T, slot_ids.T, gate_weights.T, tokens, w_gate, w_up, w_down)

    return jax.shard_map(local_layer, mesh=mesh, in_specs=(tok_spec, tok_spec, tok_spec, tok_spec, weight_spec, weight_spec, weight_spec), out_specs=tok_spec, check_vma=False)
```

```python
import jax
import jax.numpy as jnp
from jax import lax
from jax.experimental import pallas as pl
from jax.experimental.pallas import tpu as pltpu
from jax.sharding import PartitionSpec as P

CAP_FACTOR = 2
MESH = pl.DeviceIdType.MESH
F32 = jnp.float32
BF16 = jnp.bfloat16

ROWS = 256
WIDTH = 2048
FF = 768
LOCAL = 16
CAP = 32
GROUP = 8
SLOTS = LOCAL * CAP
KC = 256
NK = WIDTH // KC
U = 4
NB = 5
CC = 256
NC = WIDTH // CC
NBD = 2
LAG = 2

OWN = 0
PBUF = 64
DRECV = 80
RA1 = 144
RB1 = 160
RA2 = 176
RB2 = 184
NBLK = 192


def capacity(rows, top_k, experts):
    return ((CAP_FACTOR * rows * top_k + 8 * experts - 1) // (8 * experts)) * 8


def layer_kernel(
    id_ref, slot_ref, gate_ref, tok_ref, wg_ref, wu_ref, wd_ref, out_ref,
    rall, rt, xall, pmat, gmat, gbuf, big, wbuf, dbuf,
    lsem, rs_sem, rr_sem, xs_sem, xr_sem, w_sem, d_sem,
    ds_sem, dr_sem, is_sem, ir_sem, ready,
):
    data = lax.axis_index("data")
    y = lax.axis_index("node")
    ex = lax.axis_index("expert")
    x = ex // 2
    q = ex % 2
    g = y * 4 + ex
    flip = 1 - 2 * q
    gx = y * 4 + (1 - x) * 2 + q
    gy = (1 - y) * 4 + x * 2 + q
    gd = (1 - y) * 4 + (1 - x) * 2 + q
    gp = g + flip
    partner = (data, y, ex + flip)
    xn = (data, y, (1 - x) * 2 + q)
    yn = (data, 1 - y, ex)

    barrier = pltpu.get_barrier_semaphore()
    for d in range(1, GROUP):
        t = (g + d) % GROUP
        pl.semaphore_signal(barrier, inc=1, device_id=(data, t // 4, t % 4), device_id_type=MESH)

    def own_load(k):
        return pltpu.make_async_copy(
            tok_ref.at[:, pl.ds(pl.multiple_of(k * KC, KC), KC)],
            xall.at[pl.ds(pl.multiple_of((k * GROUP + g) * ROWS, ROWS), ROWS), :],
            lsem.at[k],
        )

    for k in range(NK):
        own_load(k).start()

    steps = LOCAL // U

    def w_load(i):
        k, e, slot = i // steps, (i % steps) * U, i % NB
        rows = pl.ds(pl.multiple_of(k * KC, KC), KC)
        return [
            pltpu.make_async_copy(ref.at[pl.ds(e, U), rows, :], wbuf.at[slot, j], w_sem.at[slot, j])
            for j, ref in enumerate((wg_ref, wu_ref))
        ]

    def d_load(i):
        c, e, slot = i // steps, (i % steps) * U, i % NBD
        cols = pl.ds(pl.multiple_of(c * CC, CC), CC)
        return pltpu.make_async_copy(wd_ref.at[pl.ds(e, U), :, cols], dbuf.at[slot], d_sem.at[slot])

    for i in range(NB):
        for cp in w_load(i):
            cp.start()
    for i in range(NBD):
        d_load(i).start()

    mine = pl.multiple_of(g * 16, 16)
    flat_pos = jnp.where(slot_ref[...] >= 0, id_ref[...] * CAP + slot_ref[...], -1)
    rall[pl.ds(mine, 8), :] = flat_pos.astype(F32)
    rall[pl.ds(mine + 8, 8), :] = gate_ref[...]
    pl.semaphore_wait(barrier, GROUP - 1)

    def r_copy(d, half, owner, dst):
        ref = rall.at[pl.ds(pl.multiple_of(owner * 16 + half * 8, 8), 8), :]
        return pltpu.make_async_remote_copy(
            src_ref=ref,
            dst_ref=ref,
            send_sem=rs_sem.at[half, d - 1],
            recv_sem=rr_sem.at[half, d - 1],
            device_id=(data, dst // 4, dst % 4),
            device_id_type=MESH,
        )

    for d in range(1, GROUP):
        r_copy(d, 0, g, (g + d) % GROUP).start()

    def x_copy(i, k, s, dev, lo=0, n=ROWS):
        ref = xall.at[pl.ds(pl.multiple_of((k * GROUP + s) * ROWS + lo, 128), n), :]
        return pltpu.make_async_remote_copy(
            src_ref=ref, dst_ref=ref, send_sem=xs_sem.at[i, k], recv_sem=xr_sem.at[i, k],
            device_id=dev, device_id_type=MESH,
        )

    HALF = ROWS // 2

    def send(i, k):
        return x_copy(i, k, *(
            (g, partner),
            (g, xn),
            (g, yn),
            (gx, yn, 0, HALF),
            (gx, partner),
            (gy, xn, HALF, HALF),
            (gy, partner),
            (gd, partner),
        )[i])

    def arrival(i, k):
        return x_copy(i, k, *(
            (gp, partner),
            (gx, xn),
            (gy, yn),
            (gd, yn, 0, HALF),
            (gx + flip, partner),
            (gd, xn, HALF, HALF),
            (gy + flip, partner),
            (gd + flip, partner),
        )[i])

    def own(k):
        own_load(k).wait()
        for i in (1, 2, 0):
            send(i, k).start()

    def forward(k):
        arrival(1, k).wait_recv()
        send(3, k).start()
        send(4, k).start()
        arrival(2, k).wait_recv()
        send(5, k).start()
        send(6, k).start()

    def diagonal(k):
        arrival(3, k).wait_recv()
        arrival(5, k).wait_recv()
        send(7, k).start()

    def finish(k):
        for i in (0, 4, 6, 7):
            arrival(i, k).wait_recv()

    own(0)
    own(1)
    for d in range(1, GROUP):
        r_copy(d, 1, g, (g + d) % GROUP).start()

    for d in range(1, GROUP):
        r_copy(d, 0, (g + GROUP - d) % GROUP, g).wait_recv()

    base = (g * SLOTS).astype(F32)
    ybuf = pmat
    PB = 64
    GB = 64

    def build_p(i, carry):
        s, b = i // (SLOTS // PB), i % (SLOTS // PB)
        want = lax.broadcasted_iota(jnp.int32, (PB, ROWS), 0).astype(F32) + (base + (b * PB).astype(F32))
        pos = rall[pl.ds(pl.multiple_of(s * 16, 16), 8), :]
        hit = jnp.zeros((PB, ROWS), F32)
        for j in range(8):
            hit = jnp.where(pos[j : j + 1, :] == want, 1.0, hit)
        pmat[s, pl.ds(pl.multiple_of(b * PB, PB), PB), :] = hit.astype(BF16)
        return carry

    def build_g(i, carry):
        s, b = i % GROUP, i // GROUP
        t0 = pl.multiple_of(b * GB, GB)
        v = pltpu.roll(rt[pl.ds(t0, GB), :], (128 - s * 16) % 128, 1)
        want = lax.broadcasted_iota(jnp.int32, (GB, SLOTS), 1).astype(F32) + base
        sel = jnp.zeros((GB, SLOTS), F32)
        for j in range(8):
            sel = jnp.where(v[:, j : j + 1] == want, v[:, 8 + j : 9 + j], sel)
        g1 = (sel * (1.0 - 2.0**-8)).astype(BF16)
        rest = sel - g1.astype(F32)
        g2 = rest.astype(BF16)
        g3 = (rest - g2.astype(F32)).astype(BF16)
        for p, part in enumerate((g1, g2, g3)):
            gmat[s, pl.ds(pl.multiple_of(p * 256 + t0, GB), GB), :] = part
        return carry

    lax.fori_loop(0, GROUP * SLOTS // PB, build_p, 0)
    forward(0)
    own(2)
    forward(1)
    own(3)
    diagonal(0)
    for d in range(1, GROUP):
        r_copy(d, 1, (g + GROUP - d) % GROUP, g).wait_recv()
    rt[...] = jnp.transpose(rall[...])
    finish(0)

    def gather_rows(k):
        for s in range(GROUP):
            xs = xall[pl.ds(pl.multiple_of((k * GROUP + s) * ROWS, ROWS), ROWS), :]
            gbuf[s] = jnp.dot(pmat[s], xs, preferred_element_type=F32).astype(BF16)

    def block(i, n=1):
        return pl.ds(pl.multiple_of(i * 256, 256), n * 256)

    def down(c, t):
        i = c * steps + t
        slot = i % NBD
        d_load(i).wait()
        rows = pl.ds(pl.multiple_of(t * U * CAP, U * CAP), U * CAP)
        h4 = xall.at[block(t * U * 3, U * 3), :]
        for u in range(U):
            h = jnp.concatenate([h4[(u * 3 + n) * 256 : (u * 3 + n + 1) * 256, :] for n in range(3)], axis=1)
            v = jnp.dot(h, dbuf[slot, u], preferred_element_type=F32).astype(BF16)
            ybuf.at[:, rows, :][:, u * CAP : (u + 1) * CAP, :] = v.reshape(GROUP, CAP, CC)

        @pl.when(i + NBD < NC * steps)
        def _():
            d_load(i + NBD).start()

    def experts(k, first=False, last=False):
        wide = 1 if last else 2

        def body(tt, carry):
            i = k * steps + tt * wide
            for w in range(wide):
                for cp in w_load(i + w):
                    cp.wait()
            for w in range(wide):
                one_step(tt * wide + w, wbuf.at[(i + w) % NB])
            for w in range(wide):

                @pl.when(i + w + NB < NK * steps)
                def _():
                    for cp in w_load(i + w + NB):
                        cp.start()

            if last:
                down(0, tt)
            else:
                each = 4 if first else 2
                for w in range(each):
                    build_g((0 if first else 4 + k * 4) + tt * each + w, 0)

                @pl.when(jnp.logical_and(tt == 0, k + 2 < NK))
                def _():
                    forward(k + 2)

                @pl.when(jnp.logical_and(tt == 0, k + 4 < NK))
                def _():
                    own(k + 4)

                @pl.when(tt == 0)
                def _():
                    diagonal(k + 1)

            return carry

        def one_step(t, w4):
            lhs4 = gbuf.at[:, pl.ds(pl.multiple_of(t * U * CAP, U * CAP), U * CAP), :]
            h4 = xall.at[block(t * U * 3, U * 3), :]
            big4 = big.at[block(t * U * 12, U * 12), :]
            for u in range(U):
                lhs = lhs4[:, u * CAP : (u + 1) * CAP, :].reshape(GROUP * CAP, KC)
                for n in range(FF // 256):
                    vals = []
                    for j in range(2):
                        v = jnp.dot(lhs, w4[j, u, :, n * 256 : (n + 1) * 256], preferred_element_type=F32)
                        at = (u * 12 + j * 6 + n * 2) * 256
                        if not first:
                            v = v + jnp.concatenate([big4[at : at + 256, :], big4[at + 256 : at + 512, :]], axis=1)
                        if not last:
                            big4[at : at + 256, :] = v[:, :128]
                            big4[at + 256 : at + 512, :] = v[:, 128:]
                        vals.append(v)
                    if last:
                        h4[(u * 3 + n) * 256 : (u * 3 + n + 1) * 256, :] = (jax.nn.silu(vals[0]) * vals[1]).astype(BF16)

        lax.fori_loop(0, steps // wide, body, 0)

    gather_rows(0)
    experts(0, first=True)
    finish(1)

    def middle(k, carry):
        gather_rows(k)
        experts(k)

        finish(k + 1)
        return carry

    lax.fori_loop(1, NK - 1, middle, 0)
    for k in range(6):
        for i in range(8):
            send(i, k).wait_send()
    gather_rows(NK - 1)
    experts(NK - 1, last=True)

    for dev in (partner, xn, yn):
        pl.semaphore_signal(ready, inc=1, device_id=dev, device_id_type=MESH)

    def part(core, d, to):
        dx, dy = d % 2, d // 2
        s = ((y + dy) % 2) * 4 + ((x + dx) % 2) * 2 + core
        ys = ybuf[s]
        v = jnp.dot(gmat[s], ys, preferred_element_type=F32)
        v = v[0:256] + (v[256:512] + v[512:768])
        into = big.at[block(to, 8), :]
        a, b = (dx * 2 + dy) * 256, (4 + dy * 2 + dx) * 256
        into[a : a + 256, :] = v[:, :128]
        into[b : b + 256, :] = v[:, 128:]

    def d2d(i, c):
        at = (2, 6, 0, 4)[i]
        return pltpu.make_async_remote_copy(
            src_ref=big.at[block(PBUF + (c % 2) * 8 + at, 2), :],
            dst_ref=big.at[block(DRECV + c * 8 + at, 2), :],
            send_sem=ds_sem.at[i, c], recv_sem=dr_sem.at[i, c],
            device_id=partner, device_id_type=MESH,
        )

    def pair_sum(i, c):
        at = (2, 6, 0, 4)[i]
        d2d(i, c).wait_recv()
        rows = block(OWN + c * 8 + at, 2)
        big[rows, :] = big[rows, :] + big[block(DRECV + c * 8 + at, 2), :]

    def ici(i, c):
        src, dst, n, dev = (
            (OWN + c * 8 + 2, RA1 + c * 2, 2, xn),
            (OWN + c * 8 + 6, RB1 + c * 2, 2, yn),
            (OWN + c * 8 + 1, RA2 + c, 1, yn),
            (OWN + c * 8 + 5, RB2 + c, 1, xn),
        )[i]
        return pltpu.make_async_remote_copy(
            src_ref=big.at[block(src, n), :], dst_ref=big.at[block(dst, n), :],
            send_sem=is_sem.at[i, c], recv_sem=ir_sem.at[i, c],
            device_id=dev, device_id_type=MESH,
        )

    def second_hop(c):
        ici(0, c).wait_recv()
        big[block(OWN + c * 8 + 1), :] = big[block(OWN + c * 8 + 1), :] + big[block(RA1 + c * 2 + 1), :]
        ici(2, c).start()
        ici(1, c).wait_recv()
        big[block(OWN + c * 8 + 5), :] = big[block(OWN + c * 8 + 5), :] + big[block(RB1 + c * 2 + 1), :]
        ici(3, c).start()

    def column_chunk(c, carry):
        @pl.when(c > 0)
        def _():
            def one(t, inner):
                down(c, t)
                return inner

            lax.fori_loop(0, steps, one, 0)

        @pl.when(c >= 2)
        def _():
            for i in range(4):
                d2d(i, c - 2).wait_send()

        for d in (3, 1, 2, 0):
            part(1 - q, d, PBUF + (c % 2) * 8)

        @pl.when(c == 0)
        def _():
            pl.semaphore_wait(ready, 3)

        for i in range(4):
            d2d(i, c).start()
        for d in (3, 1, 2, 0):
            part(q, d, OWN + c * 8)

        @pl.when(c >= LAG)
        def _():
            second_hop(c - LAG)

        pair_sum(0, c)
        ici(0, c).start()
        pair_sum(1, c)
        ici(1, c).start()
        pair_sum(2, c)
        pair_sum(3, c)
        return carry

    lax.fori_loop(0, NC, column_chunk, 0)

    def tail(c, carry):
        second_hop(c)
        return carry

    lax.fori_loop(NC - LAG, NC, tail, 0)

    def final(c, carry):
        ici(2, c).wait_recv()
        a = big[block(OWN + c * 8), :] + big[block(RA1 + c * 2), :] + big[block(RA2 + c), :]
        ici(3, c).wait_recv()
        b = big[block(OWN + c * 8 + 4), :] + big[block(RB1 + c * 2), :] + big[block(RB2 + c), :]
        out_ref[:, pl.ds(pl.multiple_of(c * CC, CC), 128)] = a.astype(BF16)
        out_ref[:, pl.ds(pl.multiple_of(c * CC + 128, 128), 128)] = b.astype(BF16)
        for i in range(4):
            ici(i, c).wait_send()
        return carry

    lax.fori_loop(0, NC, final, 0)

    for c in (NC - 2, NC - 1):
        for i in range(4):
            d2d(i, c).wait_send()
    for k in range(6, NK):
        for i in range(8):
            send(i, k).wait_send()
    for d in range(1, GROUP):
        for half in range(2):
            r_copy(d, half, g, (g + d) % GROUP).wait_send()


def solution(mesh):
    group_axes = ("node", "expert")
    group_size = mesh.shape["node"] * mesh.shape["expert"]
    tok_spec = P(("data", "node", "expert"), None)
    weight_spec = P(("node", "expert"), None, None)

    def local_layer(tokens, expert_ids, gate_weights, slot_ids, w_gate, w_up, w_down):
        rows, width = tokens.shape
        top_k = expert_ids.shape[1]
        local_experts = w_gate.shape[0]
        slot_count = capacity(rows, top_k, local_experts * group_size)
        assert (rows, width, local_experts, slot_count, group_size) == (ROWS, WIDTH, LOCAL, CAP, GROUP)
        vmem = pl.BlockSpec(memory_space=pltpu.VMEM)
        hbm = pl.BlockSpec(memory_space=pl.ANY)
        dma = pltpu.SemaphoreType.DMA
        return pl.pallas_call(
            layer_kernel,
            out_shape=pltpu.VMEM((rows, width), BF16),
            in_specs=[vmem, vmem, vmem, hbm, hbm, hbm, hbm],
            out_specs=vmem,
            scratch_shapes=[
                pltpu.VMEM((GROUP * 16, ROWS), F32),
                pltpu.VMEM((ROWS, GROUP * 16), F32),
                pltpu.VMEM((NK * GROUP * ROWS, KC), BF16),
                pltpu.VMEM((GROUP, SLOTS, ROWS), BF16),
                pltpu.VMEM((GROUP, 3 * ROWS, SLOTS), BF16),
                pltpu.VMEM((GROUP, SLOTS, KC), BF16),
                pltpu.VMEM((NBLK * 256, 128), F32),
                pltpu.VMEM((NB, 2, U, KC, FF), BF16),
                pltpu.VMEM((NBD, U, FF, CC), BF16),
                dma((NK,)),
                dma((2, GROUP - 1)),
                dma((2, GROUP - 1)),
                dma((8, NK)),
                dma((8, NK)),
                dma((NB, 2)),
                dma((NBD,)),
                dma((4, NC)),
                dma((4, NC)),
                dma((4, NC)),
                dma((4, NC)),
                pltpu.SemaphoreType.REGULAR,
            ],
            compiler_params=pltpu.CompilerParams(
                collective_id=0, has_side_effects=True, vmem_limit_bytes=65900000,
            ),
            cost_estimate=pl.CostEstimate(
                flops=6 * LOCAL * GROUP * CAP * WIDTH * FF,
                bytes_accessed=6 * LOCAL * WIDTH * FF,
                transcendentals=LOCAL * GROUP * CAP * FF,
            ),
            name="moe_layer",
        )(expert_ids.T, slot_ids.T, gate_weights.T, tokens, w_gate, w_up, w_down)

    return jax.shard_map(local_layer, mesh=mesh, in_specs=(tok_spec, tok_spec, tok_spec, tok_spec, weight_spec, weight_spec, weight_spec), out_specs=tok_spec, check_vma=False)
```

```python
import jax
import jax.numpy as jnp
from jax import lax
from jax.experimental import pallas as pl
from jax.experimental.pallas import tpu as pltpu
from jax.sharding import PartitionSpec as P

CAP_FACTOR = 2
MESH = pl.DeviceIdType.MESH
F32 = jnp.float32
BF16 = jnp.bfloat16

ROWS = 256
WIDTH = 2048
FF = 768
LOCAL = 16
CAP = 32
GROUP = 8
SLOTS = LOCAL * CAP
KC = 256
NK = WIDTH // KC
U = 4
NB = 5
CC = 256
NC = WIDTH // CC
NBD = 2
LAG = 2

OWN = 0
PBUF = 64
DRECV = 80
RA1 = 144
RB1 = 160
RA2 = 176
RB2 = 184
NBLK = 192


def capacity(rows, top_k, experts):
    return ((CAP_FACTOR * rows * top_k + 8 * experts - 1) // (8 * experts)) * 8


def layer_kernel(
    id_ref, slot_ref, gate_ref, tok_ref, wg_ref, wu_ref, wd_ref, out_ref,
    rall, rt, xall, pmat, gmat, gbuf, big, wbuf, dbuf,
    lsem, rs_sem, rr_sem, xs_sem, xr_sem, w_sem, d_sem,
    ds_sem, dr_sem, is_sem, ir_sem, ready,
):
    data = lax.axis_index("data")
    y = lax.axis_index("node")
    ex = lax.axis_index("expert")
    x = ex // 2
    q = ex % 2
    g = y * 4 + ex
    flip = 1 - 2 * q
    gx = y * 4 + (1 - x) * 2 + q
    gy = (1 - y) * 4 + x * 2 + q
    gd = (1 - y) * 4 + (1 - x) * 2 + q
    gp = g + flip
    partner = (data, y, ex + flip)
    xn = (data, y, (1 - x) * 2 + q)
    yn = (data, 1 - y, ex)

    barrier = pltpu.get_barrier_semaphore()
    for d in range(1, GROUP):
        t = (g + d) % GROUP
        pl.semaphore_signal(barrier, inc=1, device_id=(data, t // 4, t % 4), device_id_type=MESH)

    def own_load(k):
        return pltpu.make_async_copy(
            tok_ref.at[:, pl.ds(pl.multiple_of(k * KC, KC), KC)],
            xall.at[pl.ds(pl.multiple_of((k * GROUP + g) * ROWS, ROWS), ROWS), :],
            lsem.at[k],
        )

    for k in range(NK):
        own_load(k).start()

    steps = LOCAL // U

    def w_load(i):
        k, e, slot = i // steps, (i % steps) * U, i % NB
        rows = pl.ds(pl.multiple_of(k * KC, KC), KC)
        return [
            pltpu.make_async_copy(ref.at[pl.ds(e, U), rows, :], wbuf.at[slot, j], w_sem.at[slot, j])
            for j, ref in enumerate((wg_ref, wu_ref))
        ]

    def d_load(i):
        c, e, slot = i // steps, (i % steps) * U, i % NBD
        cols = pl.ds(pl.multiple_of(c * CC, CC), CC)
        return pltpu.make_async_copy(wd_ref.at[pl.ds(e, U), :, cols], dbuf.at[slot], d_sem.at[slot])

    for i in range(NB):
        for cp in w_load(i):
            cp.start()
    for i in range(NBD):
        d_load(i).start()

    mine = pl.multiple_of(g * 16, 16)
    flat_pos = jnp.where(slot_ref[...] >= 0, id_ref[...] * CAP + slot_ref[...], -1)
    rall[pl.ds(mine, 8), :] = flat_pos.astype(F32)
    rall[pl.ds(mine + 8, 8), :] = gate_ref[...]
    pl.semaphore_wait(barrier, GROUP - 1)

    def r_copy(d, half, owner, dst):
        ref = rall.at[pl.ds(pl.multiple_of(owner * 16 + half * 8, 8), 8), :]
        return pltpu.make_async_remote_copy(
            src_ref=ref,
            dst_ref=ref,
            send_sem=rs_sem.at[half, d - 1],
            recv_sem=rr_sem.at[half, d - 1],
            device_id=(data, dst // 4, dst % 4),
            device_id_type=MESH,
        )

    for d in range(1, GROUP):
        r_copy(d, 0, g, (g + d) % GROUP).start()

    def x_copy(i, k, s, dev, lo=0, n=ROWS):
        ref = xall.at[pl.ds(pl.multiple_of((k * GROUP + s) * ROWS + lo, 128), n), :]
        return pltpu.make_async_remote_copy(
            src_ref=ref, dst_ref=ref, send_sem=xs_sem.at[i, k], recv_sem=xr_sem.at[i, k],
            device_id=dev, device_id_type=MESH,
        )

    HALF = ROWS // 2

    def send(i, k):
        return x_copy(i, k, *(
            (g, partner),
            (g, xn),
            (g, yn),
            (gx, yn, 0, HALF),
            (gx, partner),
            (gy, xn, HALF, HALF),
            (gy, partner),
            (gd, partner),
        )[i])

    def arrival(i, k):
        return x_copy(i, k, *(
            (gp, partner),
            (gx, xn),
            (gy, yn),
            (gd, yn, 0, HALF),
            (gx + flip, partner),
            (gd, xn, HALF, HALF),
            (gy + flip, partner),
            (gd + flip, partner),
        )[i])

    def own(k):
        own_load(k).wait()
        for i in (1, 2, 0):
            send(i, k).start()

    def forward(k):
        arrival(1, k).wait_recv()
        send(3, k).start()
        send(4, k).start()
        arrival(2, k).wait_recv()
        send(5, k).start()
        send(6, k).start()

    def diagonal(k):
        arrival(3, k).wait_recv()
        arrival(5, k).wait_recv()
        send(7, k).start()

    def finish(k):
        for i in (0, 4, 6, 7):
            arrival(i, k).wait_recv()

    own(0)
    own(1)
    for d in range(1, GROUP):
        r_copy(d, 1, g, (g + d) % GROUP).start()

    for d in range(1, GROUP):
        r_copy(d, 0, (g + GROUP - d) % GROUP, g).wait_recv()

    base = (g * SLOTS).astype(F32)
    ybuf = pmat
    PB = 64
    GB = 64

    def build_p(i, carry):
        s, b = i // (SLOTS // PB), i % (SLOTS // PB)
        want = lax.broadcasted_iota(jnp.int32, (PB, ROWS), 0).astype(F32) + (base + (b * PB).astype(F32))
        pos = rall[pl.ds(pl.multiple_of(s * 16, 16), 8), :]
        hit = jnp.zeros((PB, ROWS), F32)
        for j in range(8):
            hit = jnp.where(pos[j : j + 1, :] == want, 1.0, hit)
        pmat[s, pl.ds(pl.multiple_of(b * PB, PB), PB), :] = hit.astype(BF16)
        return carry

    def build_g(i, carry):
        s, b = i % GROUP, i // GROUP
        t0 = pl.multiple_of(b * GB, GB)
        v = pltpu.roll(rt[pl.ds(t0, GB), :], (128 - s * 16) % 128, 1)
        want = lax.broadcasted_iota(jnp.int32, (GB, SLOTS), 1).astype(F32) + base
        sel = jnp.zeros((GB, SLOTS), F32)
        for j in range(8):
            sel = jnp.where(v[:, j : j + 1] == want, v[:, 8 + j : 9 + j], sel)
        g1 = (sel * (1.0 - 2.0**-8)).astype(BF16)
        rest = sel - g1.astype(F32)
        g2 = rest.astype(BF16)
        g3 = (rest - g2.astype(F32)).astype(BF16)
        for p, part in enumerate((g1, g2, g3)):
            gmat[s, pl.ds(pl.multiple_of(p * 256 + t0, GB), GB), :] = part
        return carry

    lax.fori_loop(0, GROUP * SLOTS // PB, build_p, 0)
    forward(0)
    own(2)
    forward(1)
    own(3)
    diagonal(0)
    for d in range(1, GROUP):
        r_copy(d, 1, (g + GROUP - d) % GROUP, g).wait_recv()
    rt[...] = jnp.transpose(rall[...])
    finish(0)

    def gather_rows(k):
        for s in range(GROUP):
            xs = xall[pl.ds(pl.multiple_of((k * GROUP + s) * ROWS, ROWS), ROWS), :]
            gbuf[s] = jnp.dot(pmat[s], xs, preferred_element_type=F32).astype(BF16)

    def block(i, n=1):
        return pl.ds(pl.multiple_of(i * 256, 256), n * 256)

    def down(c, t):
        i = c * steps + t
        slot = i % NBD
        d_load(i).wait()
        rows = pl.ds(pl.multiple_of(t * U * CAP, U * CAP), U * CAP)
        h4 = xall.at[block(t * U * 3, U * 3), :]
        for u in range(U):
            h = jnp.concatenate([h4[(u * 3 + n) * 256 : (u * 3 + n + 1) * 256, :] for n in range(3)], axis=1)
            v = jnp.dot(h, dbuf[slot, u], preferred_element_type=F32).astype(BF16)
            ybuf.at[:, rows, :][:, u * CAP : (u + 1) * CAP, :] = v.reshape(GROUP, CAP, CC)

        @pl.when(i + NBD < NC * steps)
        def _():
            d_load(i + NBD).start()

    def experts(k, first=False, last=False):
        wide = 1 if last else 2

        def body(tt, carry):
            i = k * steps + tt * wide
            for w in range(wide):
                for cp in w_load(i + w):
                    cp.wait()
            for w in range(wide):
                one_step(tt * wide + w, wbuf.at[(i + w) % NB])
            for w in range(wide):

                @pl.when(i + w + NB < NK * steps)
                def _():
                    for cp in w_load(i + w + NB):
                        cp.start()

            if last:
                down(0, tt)
            else:
                each = 4 if first else 2
                for w in range(each):
                    build_g((0 if first else 4 + k * 4) + tt * each + w, 0)

                if first:

                    @pl.when(tt == 0)
                    def _():
                        forward(k + 2)
                        own(k + 4)

                @pl.when(tt == 0)
                def _():
                    diagonal(k + 1)

            return carry

        def one_step(t, w4):
            lhs4 = gbuf.at[:, pl.ds(pl.multiple_of(t * U * CAP, U * CAP), U * CAP), :]
            h4 = xall.at[block(t * U * 3, U * 3), :]
            big4 = big.at[block(t * U * 12, U * 12), :]
            for u in range(U):
                lhs = lhs4[:, u * CAP : (u + 1) * CAP, :].reshape(GROUP * CAP, KC)
                for n in range(FF // 256):
                    vals = []
                    for j in range(2):
                        v = jnp.dot(lhs, w4[j, u, :, n * 256 : (n + 1) * 256], preferred_element_type=F32)
                        at = (u * 12 + j * 6 + n * 2) * 256
                        if not first:
                            v = v + jnp.concatenate([big4[at : at + 256, :], big4[at + 256 : at + 512, :]], axis=1)
                        if not last:
                            big4[at : at + 256, :] = v[:, :128]
                            big4[at + 256 : at + 512, :] = v[:, 128:]
                        vals.append(v)
                    if last:
                        h4[(u * 3 + n) * 256 : (u * 3 + n + 1) * 256, :] = (jax.nn.silu(vals[0]) * vals[1]).astype(BF16)

        lax.fori_loop(0, steps // wide, body, 0)

    gather_rows(0)
    experts(0, first=True)
    finish(1)

    def middle(k, carry):
        gather_rows(k)

        @pl.when(k + 2 < NK)
        def _():
            forward(k + 2)

        @pl.when(k + 4 < NK)
        def _():
            own(k + 4)

        experts(k)

        finish(k + 1)
        return carry

    lax.fori_loop(1, NK - 1, middle, 0)
    for k in range(6):
        for i in range(8):
            send(i, k).wait_send()
    gather_rows(NK - 1)
    experts(NK - 1, last=True)

    for dev in (partner, xn, yn):
        pl.semaphore_signal(ready, inc=1, device_id=dev, device_id_type=MESH)

    def part(core, d, to):
        dx, dy = d % 2, d // 2
        s = ((y + dy) % 2) * 4 + ((x + dx) % 2) * 2 + core
        ys = ybuf[s]
        v = jnp.dot(gmat[s], ys, preferred_element_type=F32)
        v = v[0:256] + (v[256:512] + v[512:768])
        into = big.at[block(to, 8), :]
        a, b = (dx * 2 + dy) * 256, (4 + dy * 2 + dx) * 256
        into[a : a + 256, :] = v[:, :128]
        into[b : b + 256, :] = v[:, 128:]

    def d2d(i, c):
        at = (2, 6, 0, 4)[i]
        return pltpu.make_async_remote_copy(
            src_ref=big.at[block(PBUF + (c % 2) * 8 + at, 2), :],
            dst_ref=big.at[block(DRECV + c * 8 + at, 2), :],
            send_sem=ds_sem.at[i, c], recv_sem=dr_sem.at[i, c],
            device_id=partner, device_id_type=MESH,
        )

    def pair_sum(i, c):
        at = (2, 6, 0, 4)[i]
        d2d(i, c).wait_recv()
        rows = block(OWN + c * 8 + at, 2)
        big[rows, :] = big[rows, :] + big[block(DRECV + c * 8 + at, 2), :]

    def ici(i, c):
        src, dst, n, dev = (
            (OWN + c * 8 + 2, RA1 + c * 2, 2, xn),
            (OWN + c * 8 + 6, RB1 + c * 2, 2, yn),
            (OWN + c * 8 + 1, RA2 + c, 1, yn),
            (OWN + c * 8 + 5, RB2 + c, 1, xn),
        )[i]
        return pltpu.make_async_remote_copy(
            src_ref=big.at[block(src, n), :], dst_ref=big.at[block(dst, n), :],
            send_sem=is_sem.at[i, c], recv_sem=ir_sem.at[i, c],
            device_id=dev, device_id_type=MESH,
        )

    def second_hop(c):
        ici(0, c).wait_recv()
        big[block(OWN + c * 8 + 1), :] = big[block(OWN + c * 8 + 1), :] + big[block(RA1 + c * 2 + 1), :]
        ici(2, c).start()
        ici(1, c).wait_recv()
        big[block(OWN + c * 8 + 5), :] = big[block(OWN + c * 8 + 5), :] + big[block(RB1 + c * 2 + 1), :]
        ici(3, c).start()

    def column_chunk(c, carry):
        @pl.when(c > 0)
        def _():
            def one(t, inner):
                down(c, t)
                return inner

            lax.fori_loop(0, steps, one, 0)

        @pl.when(c >= 2)
        def _():
            for i in range(4):
                d2d(i, c - 2).wait_send()

        for d in (3, 1, 2, 0):
            part(1 - q, d, PBUF + (c % 2) * 8)

        @pl.when(c == 0)
        def _():
            pl.semaphore_wait(ready, 3)

        for i in range(4):
            d2d(i, c).start()
        for d in (3, 1, 2, 0):
            part(q, d, OWN + c * 8)

        @pl.when(c >= LAG)
        def _():
            second_hop(c - LAG)

        pair_sum(0, c)
        ici(0, c).start()
        pair_sum(1, c)
        ici(1, c).start()
        pair_sum(2, c)
        pair_sum(3, c)
        return carry

    lax.fori_loop(0, NC, column_chunk, 0)

    def tail(c, carry):
        second_hop(c)
        return carry

    lax.fori_loop(NC - LAG, NC, tail, 0)

    def final(c, carry):
        ici(2, c).wait_recv()
        a = big[block(OWN + c * 8), :] + big[block(RA1 + c * 2), :] + big[block(RA2 + c), :]
        ici(3, c).wait_recv()
        b = big[block(OWN + c * 8 + 4), :] + big[block(RB1 + c * 2), :] + big[block(RB2 + c), :]
        out_ref[:, pl.ds(pl.multiple_of(c * CC, CC), 128)] = a.astype(BF16)
        out_ref[:, pl.ds(pl.multiple_of(c * CC + 128, 128), 128)] = b.astype(BF16)
        for i in range(4):
            ici(i, c).wait_send()
        return carry

    lax.fori_loop(0, NC, final, 0)

    for c in (NC - 2, NC - 1):
        for i in range(4):
            d2d(i, c).wait_send()
    for k in range(6, NK):
        for i in range(8):
            send(i, k).wait_send()
    for d in range(1, GROUP):
        for half in range(2):
            r_copy(d, half, g, (g + d) % GROUP).wait_send()


def solution(mesh):
    group_axes = ("node", "expert")
    group_size = mesh.shape["node"] * mesh.shape["expert"]
    tok_spec = P(("data", "node", "expert"), None)
    weight_spec = P(("node", "expert"), None, None)

    def local_layer(tokens, expert_ids, gate_weights, slot_ids, w_gate, w_up, w_down):
        rows, width = tokens.shape
        top_k = expert_ids.shape[1]
        local_experts = w_gate.shape[0]
        slot_count = capacity(rows, top_k, local_experts * group_size)
        assert (rows, width, local_experts, slot_count, group_size) == (ROWS, WIDTH, LOCAL, CAP, GROUP)
        vmem = pl.BlockSpec(memory_space=pltpu.VMEM)
        hbm = pl.BlockSpec(memory_space=pl.ANY)
        dma = pltpu.SemaphoreType.DMA
        return pl.pallas_call(
            layer_kernel,
            out_shape=pltpu.VMEM((rows, width), BF16),
            in_specs=[vmem, vmem, vmem, hbm, hbm, hbm, hbm],
            out_specs=vmem,
            scratch_shapes=[
                pltpu.VMEM((GROUP * 16, ROWS), F32),
                pltpu.VMEM((ROWS, GROUP * 16), F32),
                pltpu.VMEM((NK * GROUP * ROWS, KC), BF16),
                pltpu.VMEM((GROUP, SLOTS, ROWS), BF16),
                pltpu.VMEM((GROUP, 3 * ROWS, SLOTS), BF16),
                pltpu.VMEM((GROUP, SLOTS, KC), BF16),
                pltpu.VMEM((NBLK * 256, 128), F32),
                pltpu.VMEM((NB, 2, U, KC, FF), BF16),
                pltpu.VMEM((NBD, U, FF, CC), BF16),
                dma((NK,)),
                dma((2, GROUP - 1)),
                dma((2, GROUP - 1)),
                dma((8, NK)),
                dma((8, NK)),
                dma((NB, 2)),
                dma((NBD,)),
                dma((4, NC)),
                dma((4, NC)),
                dma((4, NC)),
                dma((4, NC)),
                pltpu.SemaphoreType.REGULAR,
            ],
            compiler_params=pltpu.CompilerParams(
                collective_id=0, has_side_effects=True, vmem_limit_bytes=65900000,
            ),
            cost_estimate=pl.CostEstimate(
                flops=6 * LOCAL * GROUP * CAP * WIDTH * FF,
                bytes_accessed=6 * LOCAL * WIDTH * FF,
                transcendentals=LOCAL * GROUP * CAP * FF,
            ),
            name="moe_layer",
        )(expert_ids.T, slot_ids.T, gate_weights.T, tokens, w_gate, w_up, w_down)

    return jax.shard_map(local_layer, mesh=mesh, in_specs=(tok_spec, tok_spec, tok_spec, tok_spec, weight_spec, weight_spec, weight_spec), out_specs=tok_spec, check_vma=False)
```
